128 devices in a mesh: band: 4 (over x_hi, core), grid: 32 (over z, x_lo, y).
Axes of the slice: x: 4 (x_hi: 2, x_lo: 2; x = x_hi * 2 + x_lo), y: 4, z: 4, core: 2. Of those that a mesh axis runs over, the one named last changes fastest.
Arguments:
- orbitals: float32 [8, 128, 128, 128], P('band', 'grid'), may hold values from -6 to 6
- occupation: float32 [8], P('band'), may hold values from 0.25 to 1
- g_list: int32 [524288], P('grid'), may hold values from 0 to 65535, as said below
- positions: float32 [3, 512], replicated, may hold values from 0 to 1
- species: int32 [512], replicated, may hold values from 0 to 3
- widths: float32 [4], replicated, may hold values from 0.3 to 2
Outputs:
- stress: float32 [3, 3], replicated
- atom_terms: float32 [512], replicated
The draws below stay inside these ranges and needn't reach their ends.
Inputs may be any that keep to these rules, and one draw needn't show every extreme that they name: `g_list`: within each aligned block of 16384 entries the values are distinct and increasing.
All inputs are finite; a program needn't handle non-finite values.
Results may differ from the reference program's by a relative error of at most 0.00013.
Values sent between devices are 32-bit elements; how exact they have to be, the bound alone decides.
A program may use at most 64 MiB of HBM per device.

```python
import math
import jax
import jax.numpy as jnp
from jax import lax

NX = 128
NY = 128
NZ = 128
GSEL_DEV = 16384
ATOMS = 512
SPECIES = 4
NBANDS = 8
SLAB_Y = 4
N_GRID = 32


def draw_orbitals(key, part):
    key_noise = jax.random.fold_in(key, 11)
    key_amplitude = jax.random.fold_in(key, 12)
    key_modes = jax.random.fold_in(key, 13)
    key_offset = jax.random.fold_in(key, 14)
    key_filter = jax.random.fold_in(key, 16)
    key_envelope = jax.random.fold_in(key, 17)
    shape = (NBANDS, NX, NY, NZ)
    noise_part = 0.3 * jnp.clip(jax.random.normal(key_noise, shape, jnp.float32), -4.0, 4.0)
    strength = jax.random.uniform(key_filter, (NBANDS,), jnp.float32, 0.04, 0.12)
    swing = jax.random.uniform(jax.random.fold_in(key_envelope, 1), (NBANDS,), jnp.float32, 0.1, 0.3)
    amp_low = 0.3
    amp_high = 0.55
    beside = jnp.roll(noise_part, 1, axis=1) + jnp.roll(noise_part, -1, axis=1)
    beside = beside + jnp.roll(noise_part, 1, axis=2) + jnp.roll(noise_part, -1, axis=2)
    beside = beside + jnp.roll(noise_part, 1, axis=3) + jnp.roll(noise_part, -1, axis=3)
    colored = noise_part + strength[:, None, None, None] * beside
    axis_x = jnp.arange(NX, dtype=jnp.float32)[None, :, None, None] / NX
    axis_y = jnp.arange(NY, dtype=jnp.float32)[None, None, :, None] / NY
    axis_z = jnp.arange(NZ, dtype=jnp.float32)[None, None, None, :] / NZ
    low_x = jax.random.randint(jax.random.fold_in(key_envelope, 2), (NBANDS,), -2, 3).astype(jnp.float32)
    low_y = jax.random.randint(jax.random.fold_in(key_envelope, 3), (NBANDS,), -2, 3).astype(jnp.float32)
    low_z = jax.random.randint(jax.random.fold_in(key_envelope, 4), (NBANDS,), -2, 3).astype(jnp.float32)
    low_phase = jax.random.uniform(jax.random.fold_in(key_envelope, 5), (NBANDS,), jnp.float32, -math.pi, math.pi)
    envelope_angle = 2.0 * math.pi * (low_x[:, None, None, None] * axis_x + low_y[:, None, None, None] * axis_y + low_z[:, None, None, None] * axis_z) + low_phase[:, None, None, None]
    envelope = 1.0 + swing[:, None, None, None] * jnp.cos(envelope_angle)
    start = (envelope * colored).astype(jnp.float32)

    def add_wave(wave, result):
        wave_key = jax.random.fold_in(key_modes, wave)
        mode_x = jax.random.randint(jax.random.fold_in(wave_key, 1), (NBANDS,), -(NX // 2), NX // 2).astype(jnp.float32)
        mode_y = jax.random.randint(jax.random.fold_in(wave_key, 2), (NBANDS,), -(NY // 2), NY // 2).astype(jnp.float32)
        mode_z = jax.random.randint(jax.random.fold_in(wave_key, 3), (NBANDS,), -(NZ // 2), NZ // 2).astype(jnp.float32)
        offset = jax.random.uniform(jax.random.fold_in(key_offset, wave), (NBANDS,), jnp.float32, -math.pi, math.pi)
        amplitude = jax.random.uniform(jax.random.fold_in(key_amplitude, wave), (NBANDS,), jnp.float32, amp_low, amp_high)
        angles = 2.0 * math.pi * (mode_x[:, None, None, None] * axis_x + mode_y[:, None, None, None] * axis_y + mode_z[:, None, None, None] * axis_z) + offset[:, None, None, None]
        return result + amplitude[:, None, None, None] * jnp.cos(angles)
    result = lax.fori_loop(0, 48, add_wave, start)
    return jnp.clip(result, -6.0, 6.0)


def draw_g_list(key, part):
    local_cells = NX * SLAB_Y * NZ
    slab_keys = jax.random.split(jax.random.fold_in(key, 21), N_GRID)

    def one_slab(slab_key):
        return jnp.sort(jax.random.permutation(slab_key, local_cells)[:GSEL_DEV])
    return jax.vmap(one_slab)(slab_keys).reshape(-1).astype(jnp.int32)


def touch_ends(values, stream_key, smallest, largest):
    longest = values.shape.index(max(values.shape))
    spots = []
    for shift in (0, 1):
        where = [jax.random.randint(jax.random.fold_in(stream_key, axis), (), 0, length) for axis, length in enumerate(values.shape)]
        where[longest] = (where[longest] + shift) % values.shape[longest]
        spots.append(tuple(where))
    return values.at[spots[0]].set(smallest).at[spots[1]].set(largest)


def shard_levels(key, extent, pieces, low, high):
    gain, own = 1.0, jax.random.fold_in(key, 6)
    for position, blocks in pieces:
        steps = jnp.exp(jax.random.uniform(jax.random.fold_in(own, position), (blocks,), jnp.float32, low / len(pieces), high / len(pieces)))
        gain = gain * jnp.repeat(steps, extent[position] // blocks).reshape([-1 if axis == position else 1 for axis in range(len(extent))])
    return gain


def setup_inputs(seed: int = 0) -> dict:
    splits = jax.random.split(jax.random.key(seed), 7)
    return {
        "orbitals": draw_orbitals(jax.random.fold_in(splits[6], 71), 0),
        "occupation": jnp.clip(0.25 + 0.75 * jax.random.uniform(splits[1], (NBANDS,), jnp.float32) ** shard_levels(splits[1], (NBANDS,), ((0, 4),), -0.2, 0.2), 0.25, 1.0),
        "g_list": draw_g_list(jax.random.fold_in(splits[6], 71), 0),
        "positions": jnp.clip(jax.random.uniform(splits[3], (3, ATOMS), jnp.float32, 0.0, 1.0), 0.0, 1.0),
        "species": touch_ends(jax.random.randint(splits[4], (ATOMS,), 0, SPECIES), jax.random.fold_in(splits[4], 1), 0, SPECIES - 1).astype(jnp.int32),
        "widths": jnp.clip(jnp.exp(jax.random.uniform(splits[5], (SPECIES,), jnp.float32, math.log(0.3), math.log(2.0))), 0.3, 2.0),
    }


HIGHEST = lax.Precision.HIGHEST


def folded_frequency(cell, length):
    folded = jnp.where(cell < length // 2, cell, cell - length)
    return folded.astype(jnp.float32)


def spectrum_sums(selected, freq_x, freq_y, freq_z, positions, species, widths, lengths, band_total):
    two_pi = 2.0 * math.pi
    wave_vector = jnp.stack([two_pi * freq_x / lengths[0], two_pi * freq_y / lengths[1], two_pi * freq_z / lengths[2]])
    wave_square = jnp.sum(wave_vector * wave_vector, axis=0)
    nonzero = (wave_square > 0).astype(jnp.float32)
    denominator = wave_square + 1.0 - nonzero
    weighted = selected * (4.0 * math.pi) * nonzero / denominator
    identity = jnp.eye(3, dtype=jnp.float32)[:, :, None]
    kernel = 2.0 * wave_vector[:, None, :] * wave_vector[None, :, :] / denominator - identity
    stress = jnp.sum(kernel * weighted[None, None, :], axis=2) / band_total
    form_factor = jnp.exp(-0.5 * wave_square[None, :] * (widths * widths)[:, None]) * weighted[None, :]
    kinds = widths.shape[0]
    one_hot = (species[:, None] == jnp.arange(kinds, dtype=jnp.int32)[None, :]).astype(jnp.float32)
    atom_count = species.shape[0]
    fractions = positions.reshape(3, atom_count // 32, 32).transpose(1, 0, 2)
    hot_rows = one_hot.reshape(atom_count // 32, 32, kinds)

    def atom_block(operands):
        fraction, hot_block = operands
        phases = two_pi * (fraction[0][:, None] * freq_x[None, :] + fraction[1][:, None] * freq_y[None, :] + fraction[2][:, None] * freq_z[None, :])
        projected = jnp.dot(jnp.cos(phases), form_factor.T, precision=HIGHEST)
        return jnp.sum(projected * hot_block, axis=1)

    atom_terms = lax.map(atom_block, (fractions, hot_rows)).reshape(atom_count) / band_total
    return stress, atom_terms


def reference(orbitals, occupation, g_list, positions, species, widths):
    cells = NX * NY * NZ

    def add_band(accumulated, operands):
        orbital_row, occupied = operands
        pair_rows = orbital_row[None] * orbitals
        spectra = jnp.fft.fftn(pair_rows, axes=(1, 2, 3)) / cells
        pair_power = jnp.real(spectra) ** 2 + jnp.imag(spectra) ** 2
        weights = occupied * occupation
        return accumulated + jnp.einsum("p,pxyz->xyz", weights, pair_power, precision=HIGHEST), None

    spectrum, ignored = lax.scan(add_band, jnp.zeros((NX, NY, NZ), jnp.float32), (orbitals, occupation))
    entries = jnp.arange(g_list.shape[0], dtype=jnp.int32)
    slab_index = entries // GSEL_DEV
    cell_x = g_list // (SLAB_Y * NZ)
    cell_y = slab_index * SLAB_Y + (g_list // NZ) % SLAB_Y
    cell_z = g_list % NZ
    selected = spectrum[cell_x, cell_y, cell_z]
    return spectrum_sums(selected, folded_frequency(cell_x, NX), folded_frequency(cell_y, NY), folded_frequency(cell_z, NZ), positions, species, widths, (NX, NY, NZ), NBANDS)
```

```python
import functools
import math

import jax
import jax.numpy as jnp
import numpy as np
from jax import lax
from jax.experimental import pallas as pl
from jax.experimental.pallas import tpu as pltpu
from jax.sharding import PartitionSpec as P

MESH = pl.DeviceIdType.MESH
N = 128
ATOMS = 512
BANDS = 8
TWO_PI = 2.0 * math.pi
F32 = jnp.float32
BF16 = jnp.bfloat16

WITHIN = ((0, 0), (1, 1), (2, 2), (3, 3), (0, 1), (2, 3), (0, 2), (1, 3), (0, 3), (1, 2))
CROSS = tuple((i, j) for i in range(4) for j in range(4, 8))
CHUNK_PLANES = (10, 8, 8, 10)
PLANES = 36


def table_parts():
    index = np.arange(N)
    angle = 2.0 * np.pi / N * ((index[:, None] * index[None, :]) % N)
    cos, sin = np.cos(angle), np.sin(angle)
    right = np.block([[cos, -sin], [sin, cos]])
    high = np.asarray(right, dtype=jnp.bfloat16)
    low = np.asarray(right - high.astype(np.float64), dtype=jnp.bfloat16)
    right_cat = np.concatenate([high, high, low], axis=0)
    left_cat = np.concatenate([high.T, high.T, low.T], axis=1)
    return right_cat, left_cat


def split(value):
    high = value.astype(BF16)
    low = (value - high.astype(F32)).astype(BF16)
    return high, low


def iota(shape, dim):
    return lax.broadcasted_iota(jnp.int32, shape, dim)


def fold(cell):
    return jnp.where(cell < N // 2, cell, cell - N)


def turns(value):
    return value - jnp.floor(value + 0.5)


def kernel(
    orbitals, occupation, g_list, positions, species, widths, right_table, left_table,
    out_atoms, out_stress,
    orb_v, list_v, neg_v, pos_v, spec_v, right_v, left_v,
    psi, y_buf, r_buf, z_re, z_im, zc_re, zc_im, x_re, x_im, col_x, col_z,
    red_src, red,
    load_sem, psi_send, psi_recv, neg_send, neg_recv, a2a_send, a2a_recv, red_send, red_recv,
):
    band = lax.axis_index("band")
    slab = lax.axis_index("grid")
    me = 4 * slab + band
    half = band // 2
    core = lax.rem(band, 2)
    pos_x = 2 * half + lax.rem(slab // 4, 2)
    pos_y = lax.rem(slab, 4)
    pos_z = slab // 8

    def target(step):
        mixed = lax.rem(step * 83, 128)
        to_core = lax.rem(core + mixed, 2)
        to_x = lax.rem(pos_x + mixed // 2, 4)
        to_y = lax.rem(pos_y + mixed // 8, 4)
        to_z = lax.rem(pos_z + mixed // 32, 4)
        to_band = 2 * (to_x // 2) + to_core
        to_slab = (2 * to_z + lax.rem(to_x, 2)) * 4 + to_y
        return to_band, to_slab

    barrier = pltpu.get_barrier_semaphore()

    def greet(step, carry):
        to_band, to_slab = target(step)
        pl.semaphore_signal(
            barrier, 1, device_id={"band": to_band, "grid": to_slab}, device_id_type=MESH
        )
        return carry

    loads = [
        pltpu.make_async_copy(src, dst, load_sem.at[k])
        for k, (src, dst) in enumerate(
            (
                (positions, pos_v),
                (species, spec_v),
                (orbitals, orb_v),
                (g_list, list_v),
                (right_table, right_v),
                (left_table, left_v),
            )
        )
    ]
    for load in loads:
        load.start()
    lax.fori_loop(1, N, greet, 0)

    loads[0].wait()
    loads[1].wait()
    kind = spec_v[...]
    width = jnp.zeros((1, ATOMS), F32)
    for s in range(4):
        width = jnp.where(kind == s, widths[s], width)
    spread = -0.5 * width * width
    low_row = iota((8, ATOMS), 0).astype(F32)
    high_row = iota((16, ATOMS), 0)
    high_row = jnp.where(high_row < 8, high_row, high_row - 16).astype(F32)
    for dim, re_ref, im_ref in ((0, x_re, x_im), (2, z_re, z_im)):
        where_at = pos_v[dim : dim + 1, :]
        low_turn = TWO_PI * turns(low_row * where_at)
        high_turn = TWO_PI * turns(high_row * turns(8.0 * where_at))
        low_cos, low_sin = jnp.cos(low_turn), jnp.sin(low_turn)
        high_cos, high_sin = jnp.cos(high_turn), jnp.sin(high_turn)
        for a in range(16):
            wave = (TWO_PI / N) * (low_row + float(8 * (a if a < 8 else a - 16)))
            form = jnp.exp(spread * (wave * wave))
            hc, hs = high_cos[a : a + 1, :], high_sin[a : a + 1, :]
            re_ref[8 * a : 8 * a + 8, :] = (hc * low_cos - hs * low_sin) * form
            im_ref[8 * a : 8 * a + 8, :] = (hc * low_sin + hs * low_cos) * form
    for table, cat in ((z_re, zc_re), (z_im, zc_im)):
        high, low = split(table[...])
        cat[0:N, :] = high
        cat[N : 2 * N, :] = high
        cat[2 * N : 3 * N, :] = low
    freq_y = fold(me)
    high_y = freq_y // 8
    low_y = freq_y - 8 * high_y
    at_y = pos_v[1:2, :]
    turn_y = TWO_PI * turns(
        low_y.astype(F32) * at_y + high_y.astype(F32) * turns(8.0 * at_y)
    )
    wave_y = (TWO_PI / N) * freq_y.astype(F32)
    form_y = jnp.exp(spread * (wave_y * wave_y))
    y_cos, y_sin = jnp.cos(turn_y) * form_y, jnp.sin(turn_y) * form_y

    loads[2].wait()
    for i in range(2):
        root = jnp.sqrt(jnp.full((N, N), occupation[i], F32))
        for plane in range(4):
            orb_v[i, plane] = orb_v[i, plane] * root
        psi[2 * band + i] = orb_v[i, band]

    pl.semaphore_wait(barrier, N - 1)

    mate = band + 1 - 2 * core
    trades = []
    for k, to_band in ((1, lax.rem(band + 2, 4)), (2, lax.rem(mate + 2, 4)), (0, mate)):
        trade = pltpu.make_async_remote_copy(
            orb_v.at[:, to_band],
            psi.at[pl.ds(2 * band, 2)],
            psi_send.at[k],
            psi_recv.at[k],
            device_id={"band": to_band, "grid": slab},
            device_id_type=MESH,
        )
        trade.start()
        trades.append(trade)
    loads[3].wait()
    neg_slab = jnp.where(band == 0, lax.rem(32 - slab, 32), 31 - slab)
    neg_copy = pltpu.make_async_remote_copy(
        list_v,
        neg_v,
        neg_send,
        neg_recv,
        device_id={"band": band, "grid": neg_slab},
        device_id_type=MESH,
    )

    @pl.when(neg_slab != slab)
    def _():
        neg_copy.start()

    @pl.when(neg_slab == slab)
    def _():
        neg_v[...] = list_v[...]

    loads[4].wait()
    loads[5].wait()

    def transform_yz(pairs, base, scales, first_plane, count):
        rows = []
        for q in range(count):
            parts = []
            for part in range(2):
                i, j = pairs[2 * q + part]
                rho = psi[base + i] * psi[base + j]
                scale = scales[2 * q + part]
                parts.append(rho if scale is None else rho * scale)
            rows.append(jnp.concatenate(parts, axis=1))
        high, low = split(jnp.concatenate(rows, axis=0))
        along_z = jnp.dot(
            jnp.concatenate([high, low, high], axis=1),
            right_v[...],
            preferred_element_type=F32,
        )
        columns = []
        for q in range(count):
            block = along_z[q * N : (q + 1) * N]
            columns.append(jnp.concatenate([block[:, :N], block[:, N:]], axis=0))
        high, low = split(jnp.concatenate(columns, axis=1))
        along_y = jnp.dot(
            left_v[...],
            jnp.concatenate([high, low, high], axis=0),
            preferred_element_type=F32,
        )
        for q in range(count):
            y_buf[first_plane + 2 * q] = along_y[:N, q * N : (q + 1) * N]
            y_buf[first_plane + 2 * q + 1] = along_y[N:, q * N : (q + 1) * N]

    def send(first_plane, planes, chunk):
        def one(step, carry):
            to_band, to_slab = target(step)
            pltpu.make_async_remote_copy(
                y_buf.at[pl.ds(first_plane, planes), 4 * to_slab + to_band, :],
                r_buf.at[pl.ds(first_plane, planes), me, :],
                a2a_send,
                a2a_recv.at[chunk],
                device_id={"band": to_band, "grid": to_slab},
                device_id_type=MESH,
            ).start()
            return carry

        lax.fori_loop(1, N, one, 0)

    root_two = math.sqrt(2.0)
    within_scale = [None if i == j else root_two for i, j in WITHIN]
    cross_scale = [root_two] * 8
    trades[2].wait_recv()
    transform_yz(WITHIN, 4 * half, within_scale, 26 * half, 5)
    send(26 * half, 10, 3 * half)
    trades[0].wait_recv()
    trades[1].wait_recv()
    transform_yz(CROSS[:8], 0, cross_scale, 10, 4)
    send(10, 8, 1)
    transform_yz(CROSS[8:], 0, cross_scale, 18, 4)
    send(18, 8, 2)
    transform_yz(WITHIN, 4 - 4 * half, within_scale, 26 - 26 * half, 5)
    send(26 - 26 * half, 10, 3 - 3 * half)

    for plane in range(PLANES):
        r_buf[plane, pl.ds(me, 1), :] = y_buf[plane, pl.ds(me, 1), :]

    @pl.when(neg_slab != slab)
    def _():
        neg_copy.wait_recv()

    def mask_of(list_ref, plane, negated):
        cells = list_ref[...]
        cell_x = lax.shift_right_logical(cells, 9)
        cell_z = cells & (N - 1)
        if negated:
            cell_x = (N - cell_x) & (N - 1)
            cell_z = (N - cell_z) & (N - 1)
        in_plane = (lax.shift_right_logical(cells, 7) & 3) == plane
        col_x[...] = jnp.where(in_plane, cell_x, -1)
        col_z[...] = cell_z
        row_index = iota((N, N), 0)

        def block(step, total):
            first = pl.multiple_of(step * 8, 8)
            block_x = col_x[pl.ds(first, 8), :]
            block_z = col_z[pl.ds(first, 8), :]
            hot_x = [(row_index == block_x[r : r + 1, :]).astype(F32).astype(BF16) for r in range(8)]
            hot_z = [(row_index == block_z[r : r + 1, :]).astype(F32).astype(BF16) for r in range(8)]
            return total + lax.dot_general(
                jnp.concatenate(hot_x, axis=1),
                jnp.concatenate(hot_z, axis=1),
                (((1,), (1,)), ((), ())),
                preferred_element_type=F32,
            )

        return lax.fori_loop(0, N // 8, block, jnp.zeros((N, N), F32))

    mask_here = mask_of(list_v, band, False)
    mask_neg = mask_of(neg_v, lax.rem(4 - band, 4), True)

    def power(first_plane, planes, chunk):
        arrived = r_buf.at[pl.ds(first_plane, planes), pl.ds(0, N - 1), :]
        pltpu.make_async_copy(arrived, arrived, a2a_recv.at[chunk]).wait()
        count = planes // 2
        columns = [
            jnp.concatenate(
                [r_buf[first_plane + 2 * q], r_buf[first_plane + 2 * q + 1]], axis=0
            )
            for q in range(count)
        ]
        high, low = split(jnp.concatenate(columns, axis=1))
        along_x = jnp.dot(
            left_v[...],
            jnp.concatenate([high, low, high], axis=0),
            preferred_element_type=F32,
        )
        total = None
        for q in range(count):
            real = along_x[:N, q * N : (q + 1) * N]
            imag = along_x[N:, q * N : (q + 1) * N]
            term = real * real + imag * imag
            total = term if total is None else total + term
        return total

    spectrum = power(10, 8, 1) + power(18, 8, 2)
    spectrum = spectrum + (power(0, 10, 0) + power(26, 10, 3))

    cell_x = iota((N, N), 0)
    cell_z = iota((N, N), 1)
    wave_x = (TWO_PI / N) * fold(cell_x).astype(F32)
    wave_z = (TWO_PI / N) * fold(cell_z).astype(F32)
    sign_x = jnp.where(cell_x == N // 2, -1.0, 1.0).astype(F32)
    sign_z = jnp.where(cell_z == N // 2, -1.0, 1.0).astype(F32)
    sign_y = jnp.where(me == N // 2, -1.0, 1.0).astype(F32)
    square = wave_x * wave_x + wave_y * wave_y + wave_z * wave_z
    nonzero = square > 0
    inverse = 1.0 / jnp.where(nonzero, square, 1.0)
    cells = float(N) ** 3
    scale = 0.5 * 4.0 * math.pi / (cells * cells * BANDS)
    weighted = jnp.where(nonzero, spectrum * scale * inverse, 0.0)
    here = weighted * mask_here
    there = weighted * mask_neg
    here_two = 2.0 * here * inverse
    there_two = 2.0 * there * inverse
    both_two = here_two + there_two
    total = here + there
    wave_xz = wave_x * wave_z
    terms = (
        both_two * (wave_x * wave_x) - total,
        wave_y * wave_x * (here_two + there_two * (sign_x * sign_y)),
        wave_xz * (here_two + there_two * (sign_x * sign_z)),
        both_two * (wave_y * wave_y) - total,
        wave_y * wave_z * (here_two + there_two * (sign_z * sign_y)),
        both_two * (wave_z * wave_z) - total,
    )
    lane = iota((1, N), 1)
    stress_row = jnp.zeros((1, N), F32)
    for term, lanes in zip(terms, ((0,), (1, 3), (2, 6), (4,), (5, 7), (8,))):
        value = jnp.sum(jnp.sum(term, axis=0, keepdims=True), axis=1, keepdims=True)
        for at in lanes:
            stress_row = jnp.where(lane == at, value, stress_row)

    def projected(rows, table):
        high, low = split(rows)
        return jnp.dot(
            jnp.concatenate([high, low, high], axis=1),
            table[...],
            preferred_element_type=F32,
        )

    proj_re = projected(jnp.concatenate([here, there], axis=0), zc_re)
    proj_im = projected(jnp.concatenate([here, there * sign_z], axis=0), zc_im)
    ex_re, ex_im = x_re[...], x_im[...]
    flip_im = jnp.where(iota((N, ATOMS), 0) == N // 2, -ex_im, ex_im)

    def along(re_part, im_part, table_im, sine):
        real = jnp.sum(ex_re * re_part - table_im * im_part, axis=0, keepdims=True)
        imag = jnp.sum(ex_re * im_part + table_im * re_part, axis=0, keepdims=True)
        return real * y_cos - imag * sine

    atoms = along(proj_re[:N], proj_im[:N], ex_im, y_sin)
    atoms = atoms + along(proj_re[N:], proj_im[N:], flip_im, y_sin * sign_y)
    for r in range(4):
        red_src[r : r + 1, :] = atoms[:, r * N : (r + 1) * N]
    red_src[4:5, :] = stress_row

    def share(step, carry):
        to_band, to_slab = target(step)
        pltpu.make_async_remote_copy(
            red_src.at[pl.ds(0, 5)],
            red.at[me, pl.ds(0, 5)],
            red_send,
            red_recv,
            device_id={"band": to_band, "grid": to_slab},
            device_id_type=MESH,
        ).start()
        return carry

    lax.fori_loop(1, N, share, 0)
    red[me, 0:5, :] = red_src[0:5, :]
    shared = red.at[pl.ds(0, N - 1), pl.ds(0, 5)]
    pltpu.make_async_copy(shared, shared, red_recv).wait()
    sums = jnp.sum(red[:, 0:5, :], axis=0)
    out_atoms[...] = sums[0:4]
    for r in range(3):
        row = sums[4:5, :]
        out_stress[r : r + 1, :] = (row if r == 0 else pltpu.roll(row, N - 3 * r, 1))[:, :3]

    for trade in trades:
        trade.wait_send()

    @pl.when(neg_slab != slab)
    def _():
        neg_copy.wait_send()

    sent = r_buf.at[:, pl.ds(0, N - 1), :]
    pltpu.make_async_copy(sent, sent, a2a_send).wait()
    pltpu.make_async_copy(shared, shared, red_send).wait()


def per_device(orbitals, occupation, g_list, positions, species, widths):
    right_table, left_table = table_parts()
    anywhere = pl.BlockSpec(memory_space=pl.ANY)
    scalars = pl.BlockSpec(memory_space=pltpu.SMEM)
    vector = pl.BlockSpec(memory_space=pltpu.VMEM)
    dma = pltpu.SemaphoreType.DMA
    atoms, stress = pl.pallas_call(
        kernel,
        out_shape=(
            jax.ShapeDtypeStruct((4, N), F32),
            jax.ShapeDtypeStruct((3, 3), F32),
        ),
        in_specs=[anywhere, scalars, anywhere, anywhere, anywhere, scalars, anywhere, anywhere],
        out_specs=(vector, vector),
        scratch_shapes=[
            pltpu.VMEM((2, 4, N, N), F32),
            pltpu.VMEM((N, N), jnp.int32),
            pltpu.VMEM((N, N), jnp.int32),
            pltpu.VMEM((3, ATOMS), F32),
            pltpu.VMEM((1, ATOMS), jnp.int32),
            pltpu.VMEM((6 * N, 2 * N), BF16),
            pltpu.VMEM((2 * N, 6 * N), BF16),
            pltpu.VMEM((BANDS, N, N), F32),
            pltpu.VMEM((PLANES, N, N), F32),
            pltpu.VMEM((PLANES, N, N), F32),
            pltpu.VMEM((N, ATOMS), F32),
            pltpu.VMEM((N, ATOMS), F32),
            pltpu.VMEM((3 * N, ATOMS), BF16),
            pltpu.VMEM((3 * N, ATOMS), BF16),
            pltpu.VMEM((N, ATOMS), F32),
            pltpu.VMEM((N, ATOMS), F32),
            pltpu.VMEM((N, N), jnp.int32),
            pltpu.VMEM((N, N), jnp.int32),
            pltpu.VMEM((8, N), F32),
            pltpu.VMEM((N, 8, N), F32),
            dma((6,)),
            dma((3,)),
            dma((3,)),
            dma,
            dma,
            dma,
            dma((4,)),
            dma,
            dma,
        ],
        compiler_params=pltpu.CompilerParams(
            collective_id=0, has_side_effects=True, vmem_limit_bytes=48 << 20
        ),
    )(
        orbitals,
        occupation,
        g_list.reshape(N, N),
        positions,
        species.reshape(1, ATOMS),
        widths,
        jnp.asarray(right_table),
        jnp.asarray(left_table),
    )
    return stress, atoms.reshape(ATOMS)


def solution(mesh):
    return jax.shard_map(
        per_device,
        mesh=mesh,
        in_specs=(P("band", "grid", None, None), P("band"), P("grid"), P(), P(), P()),
        out_specs=(P(), P()),
        check_vma=False,
    )
```

```python
import functools
import math

import jax
import jax.numpy as jnp
import numpy as np
from jax import lax
from jax.experimental import pallas as pl
from jax.experimental.pallas import tpu as pltpu
from jax.sharding import PartitionSpec as P

MESH = pl.DeviceIdType.MESH
N = 128
ATOMS = 512
BANDS = 8
TWO_PI = 2.0 * math.pi
F32 = jnp.float32
BF16 = jnp.bfloat16

WITHIN = ((0, 0), (1, 1), (2, 2), (3, 3), (0, 1), (2, 3), (0, 2), (1, 3), (0, 3), (1, 2))
CROSS = tuple((i, j) for i in range(4) for j in range(4, 8))
CHUNK_PLANES = (10, 8, 8, 10)
PLANES = 36


def far_first():
    steps = np.random.RandomState(1).permutation(np.arange(1, N))
    moves = [(int(o) // 2 % 4, int(o) // 8 % 4, int(o) // 32, int(o) % 2) for o in steps]
    return sorted(moves, key=lambda m: -sum(min(v, 4 - v) for v in m[:3]))


MOVES = far_first()


def table_parts():
    index = np.arange(N)
    angle = 2.0 * np.pi / N * ((index[:, None] * index[None, :]) % N)
    cos, sin = np.cos(angle), np.sin(angle)
    right = np.block([[cos, -sin], [sin, cos]])
    high = np.asarray(right, dtype=jnp.bfloat16)
    low = np.asarray(right - high.astype(np.float64), dtype=jnp.bfloat16)
    right_cat = np.concatenate([high, high, low], axis=0)
    left_cat = np.concatenate([high.T, high.T, low.T], axis=1)
    return right_cat, left_cat


def split(value):
    high = value.astype(BF16)
    low = (value - high.astype(F32)).astype(BF16)
    return high, low


def iota(shape, dim):
    return lax.broadcasted_iota(jnp.int32, shape, dim)


def fold(cell):
    return jnp.where(cell < N // 2, cell, cell - N)


def turns(value):
    return value - jnp.floor(value + 0.5)


def kernel(
    orbitals, occupation, g_list, positions, species, widths, right_table, left_table,
    out_atoms, out_stress,
    orb_v, list_v, neg_v, pos_v, spec_v, right_v, left_v,
    psi, y_buf, r_buf, z_re, z_im, zc_re, zc_im, x_re, x_im, col_x, col_z,
    mask_v, red_src, red,
    load_sem, psi_send, psi_recv, neg_send, neg_recv, a2a_send, a2a_recv, red_send, red_recv,
):
    band = lax.axis_index("band")
    slab = lax.axis_index("grid")
    me = 4 * slab + band
    half = band // 2
    core = lax.rem(band, 2)
    pos_x = 2 * half + lax.rem(slab // 4, 2)
    pos_y = lax.rem(slab, 4)
    pos_z = slab // 8

    at_x = [lax.rem(pos_x + move, 4) for move in range(4)]
    at_z = [8 * lax.rem(pos_z + move, 4) for move in range(4)]
    at_y = [lax.rem(pos_y + move, 4) for move in range(4)]
    at_core = [core, 1 - core]
    bands = [[2 * (x // 2) + c for c in at_core] for x in at_x]
    slabs = [[4 * lax.rem(x, 2) + y for y in at_y] for x in at_x]

    def others():
        for dx, dy, dz, dc in MOVES:
            yield bands[dx][dc], slabs[dx][dy] + at_z[dz]

    barrier = pltpu.get_barrier_semaphore()

    loads = [
        pltpu.make_async_copy(src, dst, load_sem.at[k])
        for k, (src, dst) in enumerate(
            (
                (positions, pos_v),
                (species, spec_v),
                (orbitals, orb_v),
                (g_list, list_v),
                (right_table, right_v),
                (left_table, left_v),
            )
        )
    ]
    for load in loads:
        load.start()
    for to_band, to_slab in others():
        pl.semaphore_signal(
            barrier, 1, device_id={"band": to_band, "grid": to_slab}, device_id_type=MESH
        )

    loads[0].wait()
    loads[1].wait()
    kind = spec_v[...]
    width = jnp.zeros((1, ATOMS), F32)
    for s in range(4):
        width = jnp.where(kind == s, widths[s], width)
    spread = -0.5 * width * width
    low_row = iota((8, ATOMS), 0).astype(F32)
    high_row = iota((16, ATOMS), 0)
    high_row = jnp.where(high_row < 8, high_row, high_row - 16).astype(F32)
    for dim, re_ref, im_ref in ((0, x_re, x_im), (2, z_re, z_im)):
        where_at = pos_v[dim : dim + 1, :]
        low_turn = TWO_PI * turns(low_row * where_at)
        high_turn = TWO_PI * turns(high_row * turns(8.0 * where_at))
        low_cos, low_sin = jnp.cos(low_turn), jnp.sin(low_turn)
        high_cos, high_sin = jnp.cos(high_turn), jnp.sin(high_turn)
        for a in range(16):
            wave = (TWO_PI / N) * (low_row + float(8 * (a if a < 8 else a - 16)))
            form = jnp.exp(spread * (wave * wave))
            hc, hs = high_cos[a : a + 1, :], high_sin[a : a + 1, :]
            re_ref[8 * a : 8 * a + 8, :] = (hc * low_cos - hs * low_sin) * form
            im_ref[8 * a : 8 * a + 8, :] = (hc * low_sin + hs * low_cos) * form
    for table, cat in ((z_re, zc_re), (z_im, zc_im)):
        high, low = split(table[...])
        cat[0:N, :] = high
        cat[N : 2 * N, :] = high
        cat[2 * N : 3 * N, :] = low
    freq_y = fold(me)
    high_y = freq_y // 8
    low_y = freq_y - 8 * high_y
    at_y = pos_v[1:2, :]
    turn_y = TWO_PI * turns(
        low_y.astype(F32) * at_y + high_y.astype(F32) * turns(8.0 * at_y)
    )
    wave_y = (TWO_PI / N) * freq_y.astype(F32)
    form_y = jnp.exp(spread * (wave_y * wave_y))
    y_cos, y_sin = jnp.cos(turn_y) * form_y, jnp.sin(turn_y) * form_y

    loads[2].wait()
    for i in range(2):
        root = jnp.sqrt(jnp.full((N, N), occupation[i], F32))
        for plane in range(4):
            orb_v[i, plane] = orb_v[i, plane] * root
        psi[2 * band + i] = orb_v[i, band]

    def mask_of(list_ref, plane, negated):
        cells = list_ref[...]
        cell_x = lax.shift_right_logical(cells, 9)
        cell_z = cells & (N - 1)
        if negated:
            cell_x = (N - cell_x) & (N - 1)
            cell_z = (N - cell_z) & (N - 1)
        in_plane = (lax.shift_right_logical(cells, 7) & 3) == plane
        col_x[...] = jnp.where(in_plane, cell_x, -1)
        col_z[...] = cell_z
        row_index = iota((N, N), 0)

        def block(step, total):
            first = pl.multiple_of(step * 8, 8)
            block_x = col_x[pl.ds(first, 8), :]
            block_z = col_z[pl.ds(first, 8), :]
            hot_x = [(row_index == block_x[r : r + 1, :]).astype(F32).astype(BF16) for r in range(8)]
            hot_z = [(row_index == block_z[r : r + 1, :]).astype(F32).astype(BF16) for r in range(8)]
            return total + lax.dot_general(
                jnp.concatenate(hot_x, axis=1),
                jnp.concatenate(hot_z, axis=1),
                (((1,), (1,)), ((), ())),
                preferred_element_type=F32,
            )

        return lax.fori_loop(0, N // 8, block, jnp.zeros((N, N), F32))

    loads[3].wait()
    mask_v[...] = mask_of(list_v, band, False)

    pl.semaphore_wait(barrier, N - 1)

    mate = band + 1 - 2 * core
    trades = []
    for k, to_band in ((1, lax.rem(band + 2, 4)), (2, lax.rem(mate + 2, 4)), (0, mate)):
        trade = pltpu.make_async_remote_copy(
            orb_v.at[:, to_band],
            psi.at[pl.ds(2 * band, 2)],
            psi_send.at[k],
            psi_recv.at[k],
            device_id={"band": to_band, "grid": slab},
            device_id_type=MESH,
        )
        trade.start()
        trades.append(trade)
    neg_slab = jnp.where(band == 0, lax.rem(32 - slab, 32), 31 - slab)
    neg_copy = pltpu.make_async_remote_copy(
        list_v,
        neg_v,
        neg_send,
        neg_recv,
        device_id={"band": band, "grid": neg_slab},
        device_id_type=MESH,
    )

    @pl.when(neg_slab != slab)
    def _():
        neg_copy.start()

    @pl.when(neg_slab == slab)
    def _():
        neg_v[...] = list_v[...]

    loads[4].wait()
    loads[5].wait()

    def transform_yz(pairs, base, scales, first_plane, count):
        rows = []
        for q in range(count):
            parts = []
            for part in range(2):
                i, j = pairs[2 * q + part]
                rho = psi[base + i] * psi[base + j]
                scale = scales[2 * q + part]
                parts.append(rho if scale is None else rho * scale)
            rows.append(jnp.concatenate(parts, axis=1))
        high, low = split(jnp.concatenate(rows, axis=0))
        along_z = jnp.dot(
            jnp.concatenate([high, low, high], axis=1),
            right_v[...],
            preferred_element_type=F32,
        )
        columns = []
        for q in range(count):
            block = along_z[q * N : (q + 1) * N]
            columns.append(jnp.concatenate([block[:, :N], block[:, N:]], axis=0))
        high, low = split(jnp.concatenate(columns, axis=1))
        along_y = jnp.dot(
            left_v[...],
            jnp.concatenate([high, low, high], axis=0),
            preferred_element_type=F32,
        )
        for q in range(count):
            y_buf[first_plane + 2 * q] = along_y[:N, q * N : (q + 1) * N]
            y_buf[first_plane + 2 * q + 1] = along_y[N:, q * N : (q + 1) * N]

    def send(first_plane, planes, chunk):
        for to_band, to_slab in others():
            pltpu.make_async_remote_copy(
                y_buf.at[pl.ds(first_plane, planes), 4 * to_slab + to_band, :],
                r_buf.at[pl.ds(first_plane, planes), me, :],
                a2a_send,
                a2a_recv.at[chunk],
                device_id={"band": to_band, "grid": to_slab},
                device_id_type=MESH,
            ).start()

    root_two = math.sqrt(2.0)
    within_scale = [None if i == j else root_two for i, j in WITHIN]
    cross_scale = [root_two] * 8
    trades[2].wait_recv()
    transform_yz(WITHIN, 4 * half, within_scale, 26 * half, 5)
    send(26 * half, 10, 3 * half)
    trades[0].wait_recv()
    trades[1].wait_recv()
    transform_yz(WITHIN, 4 - 4 * half, within_scale, 26 - 26 * half, 5)
    send(26 - 26 * half, 10, 3 - 3 * half)
    transform_yz(CROSS[:8], 0, cross_scale, 10, 4)
    send(10, 8, 1)
    transform_yz(CROSS[8:], 0, cross_scale, 18, 4)
    send(18, 8, 2)

    for plane in range(PLANES):
        r_buf[plane, pl.ds(me, 1), :] = y_buf[plane, pl.ds(me, 1), :]

    @pl.when(neg_slab != slab)
    def _():
        neg_copy.wait_recv()

    mask_neg = mask_of(neg_v, lax.rem(4 - band, 4), True)

    def power(first_plane, planes, chunk):
        arrived = r_buf.at[pl.ds(first_plane, planes), pl.ds(0, N - 1), :]
        pltpu.make_async_copy(arrived, arrived, a2a_recv.at[chunk]).wait()
        count = planes // 2
        columns = [
            jnp.concatenate(
                [r_buf[first_plane + 2 * q], r_buf[first_plane + 2 * q + 1]], axis=0
            )
            for q in range(count)
        ]
        high, low = split(jnp.concatenate(columns, axis=1))
        along_x = jnp.dot(
            left_v[...],
            jnp.concatenate([high, low, high], axis=0),
            preferred_element_type=F32,
        )
        total = None
        for q in range(count):
            real = along_x[:N, q * N : (q + 1) * N]
            imag = along_x[N:, q * N : (q + 1) * N]
            term = real * real + imag * imag
            total = term if total is None else total + term
        return total

    spectrum = power(0, 10, 0) + power(26, 10, 3)
    spectrum = spectrum + power(10, 8, 1)
    spectrum = spectrum + power(18, 8, 2)

    cell_x = iota((N, N), 0)
    cell_z = iota((N, N), 1)
    wave_x = (TWO_PI / N) * fold(cell_x).astype(F32)
    wave_z = (TWO_PI / N) * fold(cell_z).astype(F32)
    sign_x = jnp.where(cell_x == N // 2, -1.0, 1.0).astype(F32)
    sign_z = jnp.where(cell_z == N // 2, -1.0, 1.0).astype(F32)
    sign_y = jnp.where(me == N // 2, -1.0, 1.0).astype(F32)
    square = wave_x * wave_x + wave_y * wave_y + wave_z * wave_z
    nonzero = square > 0
    inverse = 1.0 / jnp.where(nonzero, square, 1.0)
    cells = float(N) ** 3
    scale = 0.5 * 4.0 * math.pi / (cells * cells * BANDS)
    weighted = jnp.where(nonzero, spectrum * scale * inverse, 0.0)
    here = weighted * mask_v[...]
    there = weighted * mask_neg
    here_two = 2.0 * here * inverse
    there_two = 2.0 * there * inverse
    both_two = here_two + there_two
    total = here + there
    wave_xz = wave_x * wave_z
    terms = (
        both_two * (wave_x * wave_x) - total,
        wave_y * wave_x * (here_two + there_two * (sign_x * sign_y)),
        wave_xz * (here_two + there_two * (sign_x * sign_z)),
        both_two * (wave_y * wave_y) - total,
        wave_y * wave_z * (here_two + there_two * (sign_z * sign_y)),
        both_two * (wave_z * wave_z) - total,
    )
    lane = iota((1, N), 1)
    stress_row = jnp.zeros((1, N), F32)
    for term, lanes in zip(terms, ((0,), (1, 3), (2, 6), (4,), (5, 7), (8,))):
        value = jnp.sum(jnp.sum(term, axis=0, keepdims=True), axis=1, keepdims=True)
        for at in lanes:
            stress_row = jnp.where(lane == at, value, stress_row)

    def projected(rows, table):
        high, low = split(rows)
        return jnp.dot(
            jnp.concatenate([high, low, high], axis=1),
            table[...],
            preferred_element_type=F32,
        )

    proj_re = projected(jnp.concatenate([here, there], axis=0), zc_re)
    proj_im = projected(jnp.concatenate([here, there * sign_z], axis=0), zc_im)
    ex_re, ex_im = x_re[...], x_im[...]
    flip_im = jnp.where(iota((N, ATOMS), 0) == N // 2, -ex_im, ex_im)

    def along(re_part, im_part, table_im, sine):
        real = jnp.sum(ex_re * re_part - table_im * im_part, axis=0, keepdims=True)
        imag = jnp.sum(ex_re * im_part + table_im * re_part, axis=0, keepdims=True)
        return real * y_cos - imag * sine

    atoms = along(proj_re[:N], proj_im[:N], ex_im, y_sin)
    atoms = atoms + along(proj_re[N:], proj_im[N:], flip_im, y_sin * sign_y)
    for r in range(4):
        red_src[r : r + 1, :] = atoms[:, r * N : (r + 1) * N]
    red_src[4:5, :] = stress_row

    for to_band, to_slab in others():
        pltpu.make_async_remote_copy(
            red_src.at[pl.ds(0, 5)],
            red.at[me, pl.ds(0, 5)],
            red_send,
            red_recv,
            device_id={"band": to_band, "grid": to_slab},
            device_id_type=MESH,
        ).start()
    red[me, 0:5, :] = red_src[0:5, :]
    shared = red.at[pl.ds(0, N - 1), pl.ds(0, 5)]
    pltpu.make_async_copy(shared, shared, red_recv).wait()
    sums = jnp.sum(red[:, 0:5, :], axis=0)
    out_atoms[...] = sums[0:4]
    for r in range(3):
        row = sums[4:5, :]
        out_stress[r : r + 1, :] = (row if r == 0 else pltpu.roll(row, N - 3 * r, 1))[:, :3]

    for trade in trades:
        trade.wait_send()

    @pl.when(neg_slab != slab)
    def _():
        neg_copy.wait_send()

    sent = r_buf.at[:, pl.ds(0, N - 1), :]
    pltpu.make_async_copy(sent, sent, a2a_send).wait()
    pltpu.make_async_copy(shared, shared, red_send).wait()


def per_device(orbitals, occupation, g_list, positions, species, widths):
    right_table, left_table = table_parts()
    anywhere = pl.BlockSpec(memory_space=pltpu.HBM)
    scalars = pl.BlockSpec(memory_space=pltpu.SMEM)
    vector = pl.BlockSpec(memory_space=pltpu.VMEM)
    dma = pltpu.SemaphoreType.DMA
    atoms, stress = pl.pallas_call(
        kernel,
        out_shape=(
            jax.ShapeDtypeStruct((4, N), F32),
            jax.ShapeDtypeStruct((3, 3), F32),
        ),
        in_specs=[anywhere, scalars, anywhere, anywhere, anywhere, scalars, anywhere, anywhere],
        out_specs=(vector, vector),
        scratch_shapes=[
            pltpu.VMEM((2, 4, N, N), F32),
            pltpu.VMEM((N, N), jnp.int32),
            pltpu.VMEM((N, N), jnp.int32),
            pltpu.VMEM((3, ATOMS), F32),
            pltpu.VMEM((1, ATOMS), jnp.int32),
            pltpu.VMEM((6 * N, 2 * N), BF16),
            pltpu.VMEM((2 * N, 6 * N), BF16),
            pltpu.VMEM((BANDS, N, N), F32),
            pltpu.VMEM((PLANES, N, N), F32),
            pltpu.VMEM((PLANES, N, N), F32),
            pltpu.VMEM((N, ATOMS), F32),
            pltpu.VMEM((N, ATOMS), F32),
            pltpu.VMEM((3 * N, ATOMS), BF16),
            pltpu.VMEM((3 * N, ATOMS), BF16),
            pltpu.VMEM((N, ATOMS), F32),
            pltpu.VMEM((N, ATOMS), F32),
            pltpu.VMEM((N, N), jnp.int32),
            pltpu.VMEM((N, N), jnp.int32),
            pltpu.VMEM((N, N), F32),
            pltpu.VMEM((8, N), F32),
            pltpu.VMEM((N, 8, N), F32),
            dma((6,)),
            dma((3,)),
            dma((3,)),
            dma,
            dma,
            dma,
            dma((4,)),
            dma,
            dma,
        ],
        compiler_params=pltpu.CompilerParams(
            collective_id=0, has_side_effects=True
        ),
    )(
        orbitals,
        occupation,
        g_list.reshape(N, N),
        positions,
        species.reshape(1, ATOMS),
        widths,
        jnp.asarray(right_table),
        jnp.asarray(left_table),
    )
    return stress, atoms.reshape(ATOMS)


def solution(mesh):
    return jax.shard_map(
        per_device,
        mesh=mesh,
        in_specs=(P("band", "grid", None, None), P("band"), P("grid"), P(), P(), P()),
        out_specs=(P(), P()),
        check_vma=False,
    )
```

```python
import functools
import math

import jax
import jax.numpy as jnp
import numpy as np
from jax import lax
from jax.experimental import pallas as pl
from jax.experimental.pallas import tpu as pltpu
from jax.sharding import PartitionSpec as P

MESH = pl.DeviceIdType.MESH
N = 128
ATOMS = 512
BANDS = 8
TWO_PI = 2.0 * math.pi
F32 = jnp.float32
BF16 = jnp.bfloat16

WITHIN = ((0, 0), (1, 1), (2, 2), (3, 3), (0, 1), (2, 3), (0, 2), (1, 3), (0, 3), (1, 2))
WITHIN_PARTS = 10
PARTS = 18


def far_first(moves):
    order = np.random.RandomState(1).permutation(len(moves))
    return sorted((moves[o] for o in order), key=lambda m: -sum(min(v, 4 - v) for v in m[:3]))


MOVES = far_first(
    [(x, y, z, c) for x in range(2) for y in range(4) for z in range(4) for c in range(2) if x + y + z + c]
)
GREETED = far_first(
    [
        (x, y, z, c)
        for x in range(4)
        for y in range(4)
        for z in range(4)
        for c in range(2)
        if x + y + z + c and (x != 2 or y + z == 0)
    ]
)


def table_parts():
    index = np.arange(N)
    angle = 2.0 * np.pi / N * ((index[:, None] * index[None, :]) % N)
    cos, sin = np.cos(angle), np.sin(angle)
    right = np.block([[cos, -sin], [sin, cos]])
    high = np.asarray(right, dtype=jnp.bfloat16)
    low = np.asarray(right - high.astype(np.float64), dtype=jnp.bfloat16)
    right_cat = np.concatenate([high, high, low], axis=0)
    left_cat = np.concatenate([high.T, high.T, low.T], axis=1)
    order = np.concatenate([index[0::2], index[1::2]])
    order = np.concatenate([order, N + order])
    high_x, low_x = high.T[:, order], low.T[:, order]
    cross_cat = np.concatenate([high_x, high_x, low_x], axis=1)
    return right_cat, left_cat, cross_cat


def split(value):
    high = value.astype(BF16)
    low = (value - high.astype(F32)).astype(BF16)
    return high, low


def iota(shape, dim):
    return lax.broadcasted_iota(jnp.int32, shape, dim)


def fold(cell):
    return jnp.where(cell < N // 2, cell, cell - N)


def turns(value):
    return value - jnp.floor(value + 0.5)


def kernel(
    orbitals, occupation, g_list, positions, species, widths, right_table, left_table, x_table,
    out_atoms, out_stress,
    orb_v, list_v, neg_v, pos_v, spec_v, right_v, left_v, tx_v,
    psi, y_buf, r_buf, z_re, z_im, zc_re, zc_im, x_re, x_im, col_x, col_z, masks,
    red_src, red_x, red_mid, red_yz,
    load_sem, mate_sem, cross_send, cross_recv, neg_sem, pass_sem, a2a_send, a2a_recv, red_sem,
):
    band = lax.axis_index("band")
    slab = lax.axis_index("grid")
    half = band // 2
    core = lax.rem(band, 2)
    low = lax.rem(slab // 4, 2)
    pos_x = 2 * half + low
    pos_y = lax.rem(slab, 4)
    pos_z = slab // 8
    owner = 2 * slab + core
    mate = band + 1 - 2 * core

    def device(to_band, to_slab):
        return dict(device_id={"band": to_band, "grid": to_slab}, device_id_type=MESH)

    at_x = [lax.rem(pos_x + move, 4) for move in range(4)]
    at_y = [lax.rem(pos_y + move, 4) for move in range(4)]
    at_z = [8 * lax.rem(pos_z + move, 4) for move in range(4)]
    at_core = [core, 1 - core]
    at_half = [half, 1 - half]
    lows = [[4 * at + y for y in at_y] for at in (low, 1 - low)]

    barrier = pltpu.get_barrier_semaphore()
    loads = [
        pltpu.make_async_copy(src, dst, load_sem.at[k])
        for k, (src, dst) in enumerate(
            (
                (positions, pos_v),
                (species, spec_v),
                (orbitals, orb_v),
                (g_list, list_v),
                (right_table, right_v),
                (left_table, left_v),
                (x_table, tx_v),
            )
        )
    ]
    for load in loads:
        load.start()
    greet_bands = [[2 * (x // 2) + c for c in at_core] for x in at_x]
    greet_slabs = [[4 * lax.rem(x, 2) + y for y in at_y] for x in at_x]
    for dx, dy, dz, dc in GREETED:
        pl.semaphore_signal(
            barrier, 1, **device(greet_bands[dx][dc], greet_slabs[dx][dy] + at_z[dz])
        )

    loads[0].wait()
    loads[1].wait()
    kind = spec_v[...]
    width = jnp.zeros((1, ATOMS), F32)
    for s in range(4):
        width = jnp.where(kind == s, widths[s], width)
    spread = -0.5 * width * width
    low_row = iota((8, ATOMS), 0).astype(F32)
    high_row = iota((16, ATOMS), 0)
    high_row = jnp.where(high_row < 8, high_row, high_row - 16).astype(F32)
    for dim, re_ref, im_ref in ((0, x_re, x_im), (2, z_re, z_im)):
        where_at = pos_v[dim : dim + 1, :]
        low_turn = TWO_PI * turns(low_row * where_at)
        high_turn = TWO_PI * turns(high_row * turns(8.0 * where_at))
        low_cos, low_sin = jnp.cos(low_turn), jnp.sin(low_turn)
        high_cos, high_sin = jnp.cos(high_turn), jnp.sin(high_turn)
        for a in range(16):
            wave = (TWO_PI / N) * (low_row + float(8 * (a if a < 8 else a - 16)))
            form = jnp.exp(spread * (wave * wave))
            hc, hs = high_cos[a : a + 1, :], high_sin[a : a + 1, :]
            re_ref[8 * a : 8 * a + 8, :] = (hc * low_cos - hs * low_sin) * form
            im_ref[8 * a : 8 * a + 8, :] = (hc * low_sin + hs * low_cos) * form
    for table, cat in ((z_re, zc_re), (z_im, zc_im)):
        high_part, low_part = split(table[...])
        cat[0:N, :] = high_part
        cat[N : 2 * N, :] = high_part
        cat[2 * N : 3 * N, :] = low_part
    y_waves = []
    at_turn = pos_v[1:2, :]
    for k in range(2):
        freq_y = fold(2 * owner + k)
        high_y = freq_y // 8
        low_y = freq_y - 8 * high_y
        turn_y = TWO_PI * turns(
            low_y.astype(F32) * at_turn + high_y.astype(F32) * turns(8.0 * at_turn)
        )
        wave_y = (TWO_PI / N) * freq_y.astype(F32)
        form_y = jnp.exp(spread * (wave_y * wave_y))
        y_waves.append((wave_y, jnp.cos(turn_y) * form_y, jnp.sin(turn_y) * form_y))

    loads[2].wait()
    for i in range(2):
        root = jnp.sqrt(jnp.full((N, N), occupation[i], F32))
        for plane in range(4):
            orb_v[i, plane] = orb_v[i, plane] * root
        for plane in range(2):
            psi[2 * band + i, plane] = orb_v[i, 2 * core + plane]

    pl.semaphore_wait(barrier, len(GREETED))

    loads[3].wait()
    neg_slab = jnp.where(core == 0, lax.rem(32 - slab, 32), 31 - slab)
    neg_copy = pltpu.make_async_remote_copy(
        list_v, neg_v.at[core], neg_sem.at[0], neg_sem.at[1], **device(band, neg_slab)
    )
    neg_pass = pltpu.make_async_remote_copy(
        neg_v.at[1], neg_v.at[1], pass_sem.at[0], pass_sem.at[1], **device(mate, slab)
    )

    @pl.when(neg_slab != slab)
    def _():
        neg_copy.start()

    @pl.when(neg_slab == slab)
    def _():
        neg_v[core] = list_v[...]

    def trade(to_band, to_core, send_sem, recv_sem):
        return pltpu.make_async_remote_copy(
            orb_v.at[:, pl.ds(2 * to_core, 2)],
            psi.at[pl.ds(2 * band, 2)],
            send_sem,
            recv_sem,
            **device(to_band, slab),
        )

    gives = jnp.logical_or(half == 0, core == low)
    gifts = [
        trade(2 * (1 - half) + to_core, to_core, cross_send.at[to_core], cross_recv.at[core])
        for to_core in range(2)
    ]

    @pl.when(gives)
    def _():
        for gift in gifts:
            gift.start()

    mate_trade = trade(mate, 1 - core, mate_sem.at[0], mate_sem.at[1])
    mate_trade.start()
    loads[4].wait()
    loads[5].wait()

    def transform_yz(pairs, base_i, base_j, scales, first_part, planes):
        blocks = [(q, plane) for plane in planes for q in range(len(pairs) // 2)]
        rows = []
        for q, plane in blocks:
            parts = []
            for part in range(2):
                i, j = pairs[2 * q + part]
                rho = psi[base_i + i, plane] * psi[base_j + j, plane]
                scale = scales[2 * q + part]
                parts.append(rho if scale is None else rho * scale)
            rows.append(jnp.concatenate(parts, axis=1))
        high_part, low_part = split(jnp.concatenate(rows, axis=0))
        along_z = jnp.dot(
            jnp.concatenate([high_part, low_part, high_part], axis=1),
            right_v[...],
            preferred_element_type=F32,
        )
        columns = []
        for n in range(len(blocks)):
            block = along_z[n * N : (n + 1) * N]
            columns.append(jnp.concatenate([block[:, :N], block[:, N:]], axis=0))
        high_part, low_part = split(jnp.concatenate(columns, axis=1))
        along_y = jnp.dot(
            left_v[...],
            jnp.concatenate([high_part, low_part, high_part], axis=0),
            preferred_element_type=F32,
        )
        for n, (q, plane) in enumerate(blocks):
            y_buf[first_part + 2 * q, plane] = along_y[:N, n * N : (n + 1) * N]
            y_buf[first_part + 2 * q + 1, plane] = along_y[N:, n * N : (n + 1) * N]

    def send(first_part, parts, first_plane, planes, chunk, halves):
        for dx, dy, dz, dc in MOVES:
            to_slab = lows[dx][dy] + at_z[dz]
            to_core = at_core[dc]
            to_row = pl.multiple_of(4 * to_slab + 2 * to_core, 2)
            my_row = pl.multiple_of(2 * owner, 2)
            where = (pl.ds(first_part, parts), pl.ds(first_plane, planes))
            pltpu.make_async_remote_copy(
                y_buf.at[(*where, pl.ds(to_row, 2))],
                r_buf.at[(*where, pl.ds(my_row, 2))],
                a2a_send,
                a2a_recv.at[chunk],
                **device(2 * halves[dx] + to_core, to_slab),
            ).start()

    root_two = math.sqrt(2.0)
    within_scale = [None if i == j else root_two for i, j in WITHIN]
    mate_trade.wait_recv()
    for plane in range(2):
        transform_yz(WITHIN, 4 * half, 4 * half, within_scale, 0, (plane,))
        send(0, WITHIN_PARTS, plane, 1, plane, [half, half])

    def mask_of(cells, chosen, columns, negated):
        cell_x = lax.shift_right_logical(cells, 9)
        cell_z = cells & (columns - 1)
        if negated:
            cell_x = (N - cell_x) & (N - 1)
            cell_z = (N - cell_z) & (N - 1)
        col_x[...] = jnp.where(chosen, cell_x, -1)
        col_z[...] = cell_z
        x_index = iota((N, N), 0)
        z_index = iota((columns, N), 0)

        def block(step, total):
            first = pl.multiple_of(step * 8, 8)
            block_x = col_x[pl.ds(first, 8), :]
            block_z = col_z[pl.ds(first, 8), :]
            hot_x = [(x_index == block_x[r : r + 1, :]).astype(F32).astype(BF16) for r in range(8)]
            hot_z = [(z_index == block_z[r : r + 1, :]).astype(F32).astype(BF16) for r in range(8)]
            return total + lax.dot_general(
                jnp.concatenate(hot_x, axis=1),
                jnp.concatenate(hot_z, axis=1),
                (((1,), (1,)), ((), ())),
                preferred_element_type=F32,
            )

        return lax.fori_loop(0, N // 8, block, jnp.zeros((N, columns), F32))

    own_cells = list_v[...]
    own_pair = (lax.shift_right_logical(own_cells, 8) & 1) == core
    own_masks = mask_of(own_cells, own_pair, 2 * N, False)
    masks[0] = own_masks[:, :N]
    masks[1] = own_masks[:, N:]

    cross_bytes = [trade(0, 0, cross_send.at[0], cross_recv.at[k]) for k in range(2)]

    @pl.when(jnp.logical_or(half == 1, low == 0))
    def _():
        cross_bytes[0].wait_recv()

    @pl.when(jnp.logical_or(half == 1, low == 1))
    def _():
        cross_bytes[1].wait_recv()

    cross_scale = [root_two] * 4
    kind_set = half + low - 2 * half * low
    for pair in range(2):
        pairs = [(2 * pair + i, j) for i in range(2) for j in range(2)]
        first_part = WITHIN_PARTS + 4 * pair
        transform_yz(pairs, 0, 4 + 2 * kind_set, cross_scale, first_part, (0, 1))
        send(first_part, 4, 0, 2, 2 + pair, at_half)

    @pl.when(neg_slab != slab)
    def _():
        neg_copy.wait_recv()

    @pl.when(core == 1)
    def _():
        neg_pass.start()

    own_row = pl.ds(pl.multiple_of(2 * owner, 2), 2)
    for part in range(PARTS):
        for plane in range(2):
            r_buf[part, plane, own_row, :] = y_buf[part, plane, own_row, :]

    neg_cells = neg_v[core]
    neg_plane = lax.shift_right_logical(neg_cells, 7) & 3
    masks[2] = mask_of(neg_cells, neg_plane == 2 * core, N, True)

    @pl.when(core == 0)
    def _():
        neg_pass.wait_recv()

    neg_cells = neg_v[1]
    neg_plane = lax.shift_right_logical(neg_cells, 7) & 3
    masks[3] = mask_of(neg_cells, neg_plane == 3 - 2 * core, N, True)
    loads[6].wait()

    def arrived(first_part, parts, first_plane, planes, chunk):
        there = r_buf.at[pl.ds(first_part, parts), pl.ds(first_plane, planes), pl.ds(0, N - 2)]
        pltpu.make_async_copy(there, there, a2a_recv.at[chunk]).wait()

    def power(first_part, count, totals):
        blocks = [(q, k) for q in range(count) for k in range(2)]
        columns = [
            jnp.concatenate(
                [
                    r_buf[first_part + 2 * q + part, plane, pl.ds(k, N // 2, stride=2), :]
                    for part in range(2)
                    for plane in range(2)
                ],
                axis=0,
            )
            for q, k in blocks
        ]
        high_part, low_part = split(jnp.concatenate(columns, axis=1))
        along_x = jnp.dot(
            tx_v[...],
            jnp.concatenate([high_part, low_part, high_part], axis=0),
            preferred_element_type=F32,
        )
        for n, (q, k) in enumerate(blocks):
            real = along_x[:N, n * N : (n + 1) * N]
            imag = along_x[N:, n * N : (n + 1) * N]
            term = real * real + imag * imag
            totals[k] = term if totals[k] is None else totals[k] + term
        return totals

    arrived(0, WITHIN_PARTS, 0, 1, 0)
    arrived(0, WITHIN_PARTS, 1, 1, 1)
    spectrum = power(0, 5, [None, None])
    arrived(WITHIN_PARTS, 4, 0, 2, 2)
    spectrum = power(WITHIN_PARTS, 2, spectrum)
    arrived(WITHIN_PARTS + 4, 4, 0, 2, 3)
    spectrum = power(WITHIN_PARTS + 4, 2, spectrum)

    cell_x = iota((N, N), 0)
    cell_z = iota((N, N), 1)
    wave_x = (TWO_PI / N) * fold(cell_x).astype(F32)
    wave_z = (TWO_PI / N) * fold(cell_z).astype(F32)
    sign_x = jnp.where(cell_x == N // 2, -1.0, 1.0).astype(F32)
    sign_z = jnp.where(cell_z == N // 2, -1.0, 1.0).astype(F32)
    cells = float(N) ** 3
    scale = 0.5 * 4.0 * math.pi / (cells * cells * BANDS)
    wave_xz = wave_x * wave_z
    stress_terms = None
    rows_re, rows_im = [], []
    signs_y = []
    for k in range(2):
        wave_y = y_waves[k][0]
        sign_y = jnp.where(2 * owner + k == N // 2, -1.0, 1.0).astype(F32)
        signs_y.append(sign_y)
        square = wave_x * wave_x + wave_y * wave_y + wave_z * wave_z
        nonzero = square > 0
        inverse = 1.0 / jnp.where(nonzero, square, 1.0)
        weighted = jnp.where(nonzero, spectrum[k] * scale * inverse, 0.0)
        here = weighted * masks[k]
        there = weighted * masks[2 + k]
        here_two = 2.0 * here * inverse
        there_two = 2.0 * there * inverse
        both_two = here_two + there_two
        total = here + there
        terms = (
            both_two * (wave_x * wave_x) - total,
            wave_y * wave_x * (here_two + there_two * (sign_x * sign_y)),
            wave_xz * (here_two + there_two * (sign_x * sign_z)),
            both_two * (wave_y * wave_y) - total,
            wave_y * wave_z * (here_two + there_two * (sign_z * sign_y)),
            both_two * (wave_z * wave_z) - total,
        )
        if stress_terms is None:
            stress_terms = terms
        else:
            stress_terms = [a + b for a, b in zip(stress_terms, terms)]
        rows_re += [here, there]
        rows_im += [here, there * sign_z]
    lane = iota((1, N), 1)
    stress_row = jnp.zeros((1, N), F32)
    for term, lanes in zip(stress_terms, ((0,), (1, 3), (2, 6), (4,), (5, 7), (8,))):
        value = jnp.sum(jnp.sum(term, axis=0, keepdims=True), axis=1, keepdims=True)
        for at in lanes:
            stress_row = jnp.where(lane == at, value, stress_row)

    def projected(rows, table):
        high_part, low_part = split(jnp.concatenate(rows, axis=0))
        return jnp.dot(
            jnp.concatenate([high_part, low_part, high_part], axis=1),
            table[...],
            preferred_element_type=F32,
        )

    proj_re = projected(rows_re, zc_re)
    proj_im = projected(rows_im, zc_im)
    ex_re, ex_im = x_re[...], x_im[...]
    flip_im = jnp.where(iota((N, ATOMS), 0) == N // 2, -ex_im, ex_im)
    atoms = jnp.zeros((1, ATOMS), F32)
    for n in range(4):
        re_part = proj_re[n * N : (n + 1) * N]
        im_part = proj_im[n * N : (n + 1) * N]
        k = n // 2
        table_im = flip_im if n % 2 else ex_im
        sine = y_waves[k][2] * signs_y[k] if n % 2 else y_waves[k][2]
        real = jnp.sum(ex_re * re_part - table_im * im_part, axis=0, keepdims=True)
        imag = jnp.sum(ex_re * im_part + table_im * re_part, axis=0, keepdims=True)
        atoms = atoms + (real * y_waves[k][1] - imag * sine)
    for r in range(4):
        red_src[r : r + 1, :] = atoms[:, r * N : (r + 1) * N]
    red_src[4:5, :] = stress_row

    def summed(source, parts, moves, slot, stage):
        used = source.at[pl.ds(0, 5)]
        for to_band, to_slab in moves:
            pltpu.make_async_remote_copy(
                used,
                parts.at[slot, pl.ds(0, 5)],
                red_sem.at[2 * stage],
                red_sem.at[2 * stage + 1],
                **device(to_band, to_slab),
            ).start()
        parts[slot, 0:5, :] = source[0:5, :]
        count = len(moves)
        shared = parts.at[pl.ds(0, count), pl.ds(0, 5)]
        pltpu.make_async_copy(shared, shared, red_sem.at[2 * stage + 1]).wait()
        return jnp.sum(parts[:, 0:5, :], axis=0), shared

    moves_x = [
        (greet_bands[dx][dc], greet_slabs[dx][0] + at_z[0])
        for dx in (2, 1, 3, 0)
        for dc in (1, 0)
        if dx + dc
    ]
    moves_yz = [
        (band, lows[0][dy] + at_z[dz])
        for dy, dz in sorted(
            ((dy, dz) for dy in range(4) for dz in range(4) if dy + dz),
            key=lambda m: -sum(min(v, 4 - v) for v in m),
        )
    ]
    middle, sent_x = summed(red_src, red_x, moves_x, 2 * pos_x + core, 0)
    red_mid[0:5, :] = middle
    sums, sent_yz = summed(red_mid, red_yz, moves_yz, 4 * pos_z + pos_y, 1)
    out_atoms[...] = sums[0:4]
    for r in range(3):
        row = sums[4:5, :]
        out_stress[r : r + 1, :] = (row if r == 0 else pltpu.roll(row, N - 3 * r, 1))[:, :3]

    mate_trade.wait_send()

    @pl.when(gives)
    def _():
        for gift in gifts:
            gift.wait_send()

    @pl.when(neg_slab != slab)
    def _():
        neg_copy.wait_send()

    @pl.when(core == 1)
    def _():
        neg_pass.wait_send()

    sent = r_buf.at[:, :, pl.ds(0, N - 2)]
    pltpu.make_async_copy(sent, sent, a2a_send).wait()
    pltpu.make_async_copy(sent_x, sent_x, red_sem.at[0]).wait()
    pltpu.make_async_copy(sent_yz, sent_yz, red_sem.at[2]).wait()


def per_device(orbitals, occupation, g_list, positions, species, widths):
    right_table, left_table, x_table = table_parts()
    anywhere = pl.BlockSpec(memory_space=pltpu.HBM)
    scalars = pl.BlockSpec(memory_space=pltpu.SMEM)
    vector = pl.BlockSpec(memory_space=pltpu.VMEM)
    dma = pltpu.SemaphoreType.DMA
    atoms, stress = pl.pallas_call(
        kernel,
        out_shape=(
            jax.ShapeDtypeStruct((4, N), F32),
            jax.ShapeDtypeStruct((3, 3), F32),
        ),
        in_specs=[anywhere, scalars, anywhere, anywhere, anywhere, scalars]
        + [anywhere] * 3,
        out_specs=(vector, vector),
        scratch_shapes=[
            pltpu.VMEM((2, 4, N, N), F32),
            pltpu.VMEM((N, N), jnp.int32),
            pltpu.VMEM((2, N, N), jnp.int32),
            pltpu.VMEM((3, ATOMS), F32),
            pltpu.VMEM((1, ATOMS), jnp.int32),
            pltpu.VMEM((6 * N, 2 * N), BF16),
            pltpu.VMEM((2 * N, 6 * N), BF16),
            pltpu.VMEM((2 * N, 6 * N), BF16),
            pltpu.VMEM((BANDS, 2, N, N), F32),
            pltpu.VMEM((PARTS, 2, N, N), F32),
            pltpu.VMEM((PARTS, 2, N, N), F32),
            pltpu.VMEM((N, ATOMS), F32),
            pltpu.VMEM((N, ATOMS), F32),
            pltpu.VMEM((3 * N, ATOMS), BF16),
            pltpu.VMEM((3 * N, ATOMS), BF16),
            pltpu.VMEM((N, ATOMS), F32),
            pltpu.VMEM((N, ATOMS), F32),
            pltpu.VMEM((N, N), jnp.int32),
            pltpu.VMEM((N, N), jnp.int32),
            pltpu.VMEM((4, N, N), F32),
            pltpu.VMEM((8, N), F32),
            pltpu.VMEM((8, 8, N), F32),
            pltpu.VMEM((8, N), F32),
            pltpu.VMEM((16, 8, N), F32),
            dma((7,)),
            dma((2,)),
            dma((2,)),
            dma((2,)),
            dma((2,)),
            dma((2,)),
            dma,
            dma((4,)),
            dma((4,)),
        ],
        compiler_params=pltpu.CompilerParams(collective_id=0, has_side_effects=True),
    )(
        orbitals,
        occupation,
        g_list.reshape(N, N),
        positions,
        species.reshape(1, ATOMS),
        widths,
        jnp.asarray(right_table),
        jnp.asarray(left_table),
        jnp.asarray(x_table),
    )
    return stress, atoms.reshape(ATOMS)


def solution(mesh):
    return jax.shard_map(
        per_device,
        mesh=mesh,
        in_specs=(P("band", "grid", None, None), P("band"), P("grid"), P(), P(), P()),
        out_specs=(P(), P()),
        check_vma=False,
    )
```

```python
import functools
import math

import jax
import jax.numpy as jnp
import numpy as np
from jax import lax
from jax.experimental import pallas as pl
from jax.experimental.pallas import tpu as pltpu
from jax.sharding import PartitionSpec as P

MESH = pl.DeviceIdType.MESH
N = 128
ATOMS = 512
BANDS = 8
TWO_PI = 2.0 * math.pi
F32 = jnp.float32
BF16 = jnp.bfloat16

MIXED = (((0, 1), (2, 3)), ((0, 2), (1, 3)), ((0, 3), (1, 2)))
WITHIN_PARTS = 10
PARTS = 18


def far_first(moves):
    order = np.random.RandomState(1).permutation(len(moves))
    return sorted((moves[o] for o in order), key=lambda m: -sum(min(v, 4 - v) for v in m[:3]))


MOVES = far_first(
    [(x, y, z, c) for x in range(2) for y in range(4) for z in range(4) for c in range(2) if x + y + z + c]
)
GREETED = far_first(
    [
        (x, y, z, c)
        for x in range(4)
        for y in range(4)
        for z in range(4)
        for c in range(2)
        if x + y + z + c and (x != 2 or y + z == 0)
    ]
)


def table_parts():
    index = np.arange(N)
    angle = 2.0 * np.pi / N * ((index[:, None] * index[None, :]) % N)
    cos, sin = np.cos(angle), np.sin(angle)
    right = np.block([[cos, -sin], [sin, cos]])
    high = np.asarray(right, dtype=jnp.bfloat16)
    low = np.asarray(right - high.astype(np.float64), dtype=jnp.bfloat16)
    right_cat = np.concatenate([high, high, low], axis=0)
    left_cat = np.concatenate([high.T, high.T, low.T], axis=1)
    order = np.concatenate([index[0::2], index[1::2]])
    order = np.concatenate([order, N + order])
    high_x, low_x = high.T[:, order], low.T[:, order]
    cross_cat = np.concatenate([high_x, high_x, low_x], axis=1)
    return right_cat, left_cat, cross_cat


def split(value):
    high = value.astype(BF16)
    low = (value - high.astype(F32)).astype(BF16)
    return high, low


def iota(shape, dim):
    return lax.broadcasted_iota(jnp.int32, shape, dim)


def fold(cell):
    return jnp.where(cell < N // 2, cell, cell - N)


def turns(value):
    return value - jnp.floor(value + 0.5)


def kernel(
    orbitals, occupation_at, g_list, positions, species, widths_at, right_table, left_table, x_table,
    out_atoms, out_stress,
    occupation, widths, orb_v, list_v, neg_v, pos_v, spec_v, right_v, left_v, tx_v,
    psi, y_buf, r_buf, z_re, z_im, zc_re, zc_im, x_re, x_im, col_x, col_z, masks,
    red_src, red_x, red_mid, red_yz,
    load_sem, mate_sem, cross_send, cross_recv, neg_sem, pass_sem, a2a_send, a2a_recv, red_sem,
):
    band = lax.axis_index("band")
    slab = lax.axis_index("grid")
    half = band // 2
    core = lax.rem(band, 2)
    low = lax.rem(slab // 4, 2)
    pos_x = 2 * half + low
    pos_y = lax.rem(slab, 4)
    pos_z = slab // 8
    owner = 2 * slab + core
    mate = band + 1 - 2 * core

    def device(to_band, to_slab):
        return dict(device_id={"band": to_band, "grid": to_slab}, device_id_type=MESH)

    at_x = [lax.rem(pos_x + move, 4) for move in range(4)]
    at_y = [lax.rem(pos_y + move, 4) for move in range(4)]
    at_z = [8 * lax.rem(pos_z + move, 4) for move in range(4)]
    at_core = [core, 1 - core]
    at_half = [half, 1 - half]
    lows = [[4 * at + y for y in at_y] for at in (low, 1 - low)]

    barrier = pltpu.get_barrier_semaphore()
    loads = [
        pltpu.make_async_copy(src, dst, load_sem.at[k])
        for k, (src, dst) in enumerate(
            (
                (positions, pos_v),
                (species, spec_v),
                (orbitals, orb_v),
                (g_list, list_v),
                (right_table, right_v),
                (left_table, left_v),
                (x_table, tx_v),
                (occupation_at, occupation),
                (widths_at, widths),
            )
        )
    ]
    for k in (7, 2, 4, 5, 3, 0, 1, 8, 6):
        loads[k].start()
    greet_bands = [[2 * (x // 2) + c for c in at_core] for x in at_x]
    greet_slabs = [[4 * lax.rem(x, 2) + y for y in at_y] for x in at_x]
    for dx, dy, dz, dc in GREETED:
        pl.semaphore_signal(
            barrier, 1, **device(greet_bands[dx][dc], greet_slabs[dx][dy] + at_z[dz])
        )

    loads[7].wait()
    loads[2].wait()
    for i in range(2):
        root = jnp.sqrt(jnp.full((N, N), occupation[i], F32))
        for plane in range(4):
            orb_v[i, plane] = orb_v[i, plane] * root
        for plane in range(2):
            psi[2 * band + i, plane] = orb_v[i, 2 * core + plane]

    def transform_yz(transforms, planes):
        blocks = [(transform, plane) for plane in planes for transform in transforms]
        rows = []
        for (_, *pairs), plane in blocks:
            parts = []
            for i, j, scale in pairs:
                rho = psi[i, plane] * psi[j, plane]
                parts.append(rho if scale is None else rho * scale)
            rows.append(jnp.concatenate(parts, axis=1))
        high_part, low_part = split(jnp.concatenate(rows, axis=0))
        along_z = jnp.dot(
            jnp.concatenate([high_part, low_part, high_part], axis=1),
            right_v[...],
            preferred_element_type=F32,
        )
        columns = []
        for n in range(len(blocks)):
            block = along_z[n * N : (n + 1) * N]
            columns.append(jnp.concatenate([block[:, :N], block[:, N:]], axis=0))
        high_part, low_part = split(jnp.concatenate(columns, axis=1))
        along_y = jnp.dot(
            left_v[...],
            jnp.concatenate([high_part, low_part, high_part], axis=0),
            preferred_element_type=F32,
        )
        for n, ((part, *_), plane) in enumerate(blocks):
            y_buf[part, plane] = along_y[:N, n * N : (n + 1) * N]
            y_buf[part + 1, plane] = along_y[N:, n * N : (n + 1) * N]

    def send(first_part, parts, first_plane, planes, chunk, halves, columns):
        for dx, dy, dz, dc in MOVES:
            if dx not in columns:
                continue
            to_slab = lows[dx][dy] + at_z[dz]
            to_core = at_core[dc]
            to_row = pl.multiple_of(4 * to_slab + 2 * to_core, 2)
            my_row = pl.multiple_of(2 * owner, 2)
            where = (pl.ds(first_part, parts), pl.ds(first_plane, planes))
            pltpu.make_async_remote_copy(
                y_buf.at[(*where, pl.ds(to_row, 2))],
                r_buf.at[(*where, pl.ds(my_row, 2))],
                a2a_send,
                a2a_recv.at[chunk],
                **device(2 * halves[dx] + to_core, to_slab),
            ).start()

    loads[4].wait()
    loads[5].wait()
    root_two = math.sqrt(2.0)
    first = 4 * half
    same_half = [half, half]

    def within(part, band_at):
        return (part, (band_at, band_at, None), (band_at + 1, band_at + 1, None))

    transform_yz([within(8 * core, 2 * band)], (0, 1))

    pl.semaphore_wait(barrier, len(GREETED))

    loads[3].wait()
    neg_slab = jnp.where(core == 0, lax.rem(32 - slab, 32), 31 - slab)
    neg_copy = pltpu.make_async_remote_copy(
        list_v, neg_v.at[core], neg_sem.at[0], neg_sem.at[1], **device(band, neg_slab)
    )
    neg_pass = pltpu.make_async_remote_copy(
        neg_v.at[1], neg_v.at[1], pass_sem.at[0], pass_sem.at[1], **device(mate, slab)
    )

    @pl.when(neg_slab != slab)
    def _():
        neg_copy.start()

    @pl.when(neg_slab == slab)
    def _():
        neg_v[core] = list_v[...]

    def trade(to_band, to_core, send_sem, recv_sem):
        return pltpu.make_async_remote_copy(
            orb_v.at[:, pl.ds(2 * to_core, 2)],
            psi.at[pl.ds(2 * band, 2)],
            send_sem,
            recv_sem,
            **device(to_band, slab),
        )

    gives = jnp.logical_or(half == 0, core == low)
    gives_late = jnp.logical_and(half == 0, core == 1)
    gifts = [
        trade(2 * (1 - half) + to_core, to_core, cross_send.at[to_core], cross_recv.at[core])
        for to_core in range(2)
    ]

    @pl.when(jnp.logical_and(gives, jnp.logical_not(gives_late)))
    def _():
        for gift in gifts:
            gift.start()

    mate_trade = trade(mate, 1 - core, mate_sem.at[0], mate_sem.at[1])
    mate_trade.start()
    send(8 * core, 2, 0, 2, 0, same_half, (0, 1))

    mate_trade.wait_recv()
    rest = [within(8 - 8 * core, 2 * mate)]
    for n, ((i, j), (k, m)) in enumerate(MIXED):
        rest.append(
            (2 + 2 * n, (first + i, first + j, root_two), (first + k, first + m, root_two))
        )
    for plane in range(2):
        transform_yz(rest, (plane,))
        send(2 - 2 * core, 8, plane, 1, 0, same_half, (0,))

    @pl.when(gives_late)
    def _():
        for gift in gifts:
            gift.start()

    for plane in range(2):
        send(2 - 2 * core, 8, plane, 1, 0, same_half, (1,))

    loads[0].wait()
    loads[1].wait()
    loads[8].wait()
    kind = spec_v[...]
    width = jnp.zeros((1, ATOMS), F32)
    for s in range(4):
        width = jnp.where(kind == s, widths[s], width)
    spread = -0.5 * width * width
    low_row = iota((8, ATOMS), 0).astype(F32)
    high_row = iota((16, ATOMS), 0)
    high_row = jnp.where(high_row < 8, high_row, high_row - 16).astype(F32)
    for dim, re_ref, im_ref in ((0, x_re, x_im), (2, z_re, z_im)):
        where_at = pos_v[dim : dim + 1, :]
        low_turn = TWO_PI * turns(low_row * where_at)
        high_turn = TWO_PI * turns(high_row * turns(8.0 * where_at))
        low_cos, low_sin = jnp.cos(low_turn), jnp.sin(low_turn)
        high_cos, high_sin = jnp.cos(high_turn), jnp.sin(high_turn)
        for a in range(16):
            wave = (TWO_PI / N) * (low_row + float(8 * (a if a < 8 else a - 16)))
            form = jnp.exp(spread * (wave * wave))
            hc, hs = high_cos[a : a + 1, :], high_sin[a : a + 1, :]
            re_ref[8 * a : 8 * a + 8, :] = (hc * low_cos - hs * low_sin) * form
            im_ref[8 * a : 8 * a + 8, :] = (hc * low_sin + hs * low_cos) * form
    for table, cat in ((z_re, zc_re), (z_im, zc_im)):
        high_part, low_part = split(table[...])
        cat[0:N, :] = high_part
        cat[N : 2 * N, :] = high_part
        cat[2 * N : 3 * N, :] = low_part
    y_waves = []
    at_turn = pos_v[1:2, :]
    for k in range(2):
        freq_y = fold(2 * owner + k)
        high_y = freq_y // 8
        low_y = freq_y - 8 * high_y
        turn_y = TWO_PI * turns(
            low_y.astype(F32) * at_turn + high_y.astype(F32) * turns(8.0 * at_turn)
        )
        wave_y = (TWO_PI / N) * freq_y.astype(F32)
        form_y = jnp.exp(spread * (wave_y * wave_y))
        y_waves.append((wave_y, jnp.cos(turn_y) * form_y, jnp.sin(turn_y) * form_y))

    def mask_of(cells, chosen, columns, negated):
        cell_x = lax.shift_right_logical(cells, 9)
        cell_z = cells & (columns - 1)
        if negated:
            cell_x = (N - cell_x) & (N - 1)
            cell_z = (N - cell_z) & (N - 1)
        col_x[...] = jnp.where(chosen, cell_x, -1).astype(F32)
        col_z[...] = cell_z.astype(F32)
        x_index = iota((N, N), 0).astype(F32).astype(BF16)
        z_index = iota((columns, N), 0).astype(F32).astype(BF16)
        one, zero = jnp.ones((), BF16), jnp.zeros((), BF16)

        def hot(index, block):
            found = []
            for r in range(8):
                row = jnp.broadcast_to(block[r : r + 1, :], (16, N)).astype(BF16)
                rows = jnp.concatenate([row] * (index.shape[0] // 16), axis=0)
                found.append(jnp.where(index == rows, one, zero))
            return found

        def block(step, total):
            first = pl.multiple_of(step * 8, 8)
            hot_x = hot(x_index, col_x[pl.ds(first, 8), :])
            hot_z = hot(z_index, col_z[pl.ds(first, 8), :])
            return total + lax.dot_general(
                jnp.concatenate(hot_x, axis=1),
                jnp.concatenate(hot_z, axis=1),
                (((1,), (1,)), ((), ())),
                preferred_element_type=F32,
            )

        return lax.fori_loop(0, N // 8, block, jnp.zeros((N, columns), F32))

    own_cells = list_v[...]
    own_pair = (lax.shift_right_logical(own_cells, 8) & 1) == core
    own_masks = mask_of(own_cells, own_pair, 2 * N, False)
    masks[0] = own_masks[:, :N]
    masks[1] = own_masks[:, N:]

    cross_bytes = [trade(0, 0, cross_send.at[0], cross_recv.at[k]) for k in range(2)]

    kind_set = half + low - 2 * half * low
    other = 4 + 2 * kind_set
    for pair in range(2):
        for sender in range(2):
            from_both = jnp.logical_and(half == 1, sender == pair)
            from_one = jnp.logical_and(half == 0, low == sender)

            @pl.when(jnp.logical_or(from_both, from_one) if pair == 0 else from_both)
            def _():
                cross_bytes[sender].wait_recv()

        first_part = WITHIN_PARTS + 4 * pair
        transform_yz(
            [
                (first_part + 2 * n, (i, other, root_two), (i, other + 1, root_two))
                for n, i in enumerate((2 * pair, 2 * pair + 1))
            ],
            (0, 1),
        )
        send(first_part, 4, 0, 2, 1 + pair, at_half, (0, 1))

    @pl.when(neg_slab != slab)
    def _():
        neg_copy.wait_recv()

    @pl.when(core == 1)
    def _():
        neg_pass.start()

    own_row = pl.ds(pl.multiple_of(2 * owner, 2), 2)
    for part in range(PARTS):
        for plane in range(2):
            r_buf[part, plane, own_row, :] = y_buf[part, plane, own_row, :]

    neg_cells = neg_v[core]
    neg_plane = lax.shift_right_logical(neg_cells, 7) & 3
    masks[2] = mask_of(neg_cells, neg_plane == 2 * core, N, True)

    @pl.when(core == 0)
    def _():
        neg_pass.wait_recv()

    neg_cells = neg_v[1]
    neg_plane = lax.shift_right_logical(neg_cells, 7) & 3
    masks[3] = mask_of(neg_cells, neg_plane == 3 - 2 * core, N, True)
    loads[6].wait()

    def arrived(first_part, parts, chunk):
        there = r_buf.at[pl.ds(first_part, parts), :, pl.ds(0, N - 2)]
        pltpu.make_async_copy(there, there, a2a_recv.at[chunk]).wait()

    def power(first_part, count, totals):
        blocks = [(q, k) for q in range(count) for k in range(2)]
        columns = [
            jnp.concatenate(
                [
                    r_buf[first_part + 2 * q + part, plane, pl.ds(k, N // 2, stride=2), :]
                    for part in range(2)
                    for plane in range(2)
                ],
                axis=0,
            )
            for q, k in blocks
        ]
        high_part, low_part = split(jnp.concatenate(columns, axis=1))
        along_x = jnp.dot(
            tx_v[...],
            jnp.concatenate([high_part, low_part, high_part], axis=0),
            preferred_element_type=F32,
        )
        for n, (q, k) in enumerate(blocks):
            real = along_x[:N, n * N : (n + 1) * N]
            imag = along_x[N:, n * N : (n + 1) * N]
            term = real * real + imag * imag
            totals[k] = term if totals[k] is None else totals[k] + term
        return totals

    arrived(0, WITHIN_PARTS, 0)
    spectrum = power(0, 5, [None, None])
    arrived(WITHIN_PARTS, 4, 1)
    spectrum = power(WITHIN_PARTS, 2, spectrum)
    arrived(WITHIN_PARTS + 4, 4, 2)
    spectrum = power(WITHIN_PARTS + 4, 2, spectrum)

    cell_x = iota((N, N), 0)
    cell_z = iota((N, N), 1)
    wave_x = (TWO_PI / N) * fold(cell_x).astype(F32)
    wave_z = (TWO_PI / N) * fold(cell_z).astype(F32)
    sign_x = jnp.where(cell_x == N // 2, -1.0, 1.0).astype(F32)
    sign_z = jnp.where(cell_z == N // 2, -1.0, 1.0).astype(F32)
    cells = float(N) ** 3
    scale = 0.5 * 4.0 * math.pi / (cells * cells * BANDS)
    wave_xz = wave_x * wave_z
    stress_terms = None
    rows_re, rows_im = [], []
    signs_y = []
    for k in range(2):
        wave_y = y_waves[k][0]
        sign_y = jnp.where(2 * owner + k == N // 2, -1.0, 1.0).astype(F32)
        signs_y.append(sign_y)
        square = wave_x * wave_x + wave_y * wave_y + wave_z * wave_z
        nonzero = square > 0
        inverse = 1.0 / jnp.where(nonzero, square, 1.0)
        weighted = jnp.where(nonzero, spectrum[k] * scale * inverse, 0.0)
        here = weighted * masks[k]
        there = weighted * masks[2 + k]
        here_two = 2.0 * here * inverse
        there_two = 2.0 * there * inverse
        both_two = here_two + there_two
        total = here + there
        terms = (
            both_two * (wave_x * wave_x) - total,
            wave_y * wave_x * (here_two + there_two * (sign_x * sign_y)),
            wave_xz * (here_two + there_two * (sign_x * sign_z)),
            both_two * (wave_y * wave_y) - total,
            wave_y * wave_z * (here_two + there_two * (sign_z * sign_y)),
            both_two * (wave_z * wave_z) - total,
        )
        if stress_terms is None:
            stress_terms = terms
        else:
            stress_terms = [a + b for a, b in zip(stress_terms, terms)]
        rows_re += [here, there]
        rows_im += [here, there * sign_z]
    lane = iota((1, N), 1)
    stress_row = jnp.zeros((1, N), F32)
    for term, lanes in zip(stress_terms, ((0,), (1, 3), (2, 6), (4,), (5, 7), (8,))):
        value = jnp.sum(jnp.sum(term, axis=0, keepdims=True), axis=1, keepdims=True)
        for at in lanes:
            stress_row = jnp.where(lane == at, value, stress_row)

    def projected(rows, table):
        high_part, low_part = split(jnp.concatenate(rows, axis=0))
        return jnp.dot(
            jnp.concatenate([high_part, low_part, high_part], axis=1),
            table[...],
            preferred_element_type=F32,
        )

    proj_re = projected(rows_re, zc_re)
    proj_im = projected(rows_im, zc_im)
    ex_re, ex_im = x_re[...], x_im[...]
    flip_im = jnp.where(iota((N, ATOMS), 0) == N // 2, -ex_im, ex_im)
    atoms = jnp.zeros((1, ATOMS), F32)
    for n in range(4):
        re_part = proj_re[n * N : (n + 1) * N]
        im_part = proj_im[n * N : (n + 1) * N]
        k = n // 2
        table_im = flip_im if n % 2 else ex_im
        sine = y_waves[k][2] * signs_y[k] if n % 2 else y_waves[k][2]
        real = jnp.sum(ex_re * re_part - table_im * im_part, axis=0, keepdims=True)
        imag = jnp.sum(ex_re * im_part + table_im * re_part, axis=0, keepdims=True)
        atoms = atoms + (real * y_waves[k][1] - imag * sine)
    for r in range(4):
        red_src[r : r + 1, :] = atoms[:, r * N : (r + 1) * N]
    red_src[4:5, :] = stress_row

    def summed(source, parts, moves, slot, stage):
        used = source.at[pl.ds(0, 5)]
        for to_band, to_slab in moves:
            pltpu.make_async_remote_copy(
                used,
                parts.at[slot, pl.ds(0, 5)],
                red_sem.at[2 * stage],
                red_sem.at[2 * stage + 1],
                **device(to_band, to_slab),
            ).start()
        parts[slot, 0:5, :] = source[0:5, :]
        count = len(moves)
        shared = parts.at[pl.ds(0, count), pl.ds(0, 5)]
        pltpu.make_async_copy(shared, shared, red_sem.at[2 * stage + 1]).wait()
        return jnp.sum(parts[:, 0:5, :], axis=0), shared

    moves_x = [
        (greet_bands[dx][dc], greet_slabs[dx][0] + at_z[0])
        for dx in (2, 1, 3, 0)
        for dc in (1, 0)
        if dx + dc
    ]
    moves_yz = [
        (band, lows[0][dy] + at_z[dz])
        for dy, dz in sorted(
            ((dy, dz) for dy in range(4) for dz in range(4) if dy + dz),
            key=lambda m: -sum(min(v, 4 - v) for v in m),
        )
    ]
    middle, sent_x = summed(red_src, red_x, moves_x, 2 * pos_x + core, 0)
    red_mid[0:5, :] = middle
    sums, sent_yz = summed(red_mid, red_yz, moves_yz, 4 * pos_z + pos_y, 1)
    out_atoms[...] = sums[0:4]
    for r in range(3):
        row = sums[4:5, :]
        out_stress[r : r + 1, :] = (row if r == 0 else pltpu.roll(row, N - 3 * r, 1))[:, :3]

    mate_trade.wait_send()

    @pl.when(gives)
    def _():
        for gift in gifts:
            gift.wait_send()

    @pl.when(neg_slab != slab)
    def _():
        neg_copy.wait_send()

    @pl.when(core == 1)
    def _():
        neg_pass.wait_send()

    sent = r_buf.at[:, :, pl.ds(0, N - 2)]
    pltpu.make_async_copy(sent, sent, a2a_send).wait()
    pltpu.make_async_copy(sent_x, sent_x, red_sem.at[0]).wait()
    pltpu.make_async_copy(sent_yz, sent_yz, red_sem.at[2]).wait()


def per_device(orbitals, occupation, g_list, positions, species, widths):
    right_table, left_table, x_table = table_parts()
    anywhere = pl.BlockSpec(memory_space=pltpu.HBM)
    vector = pl.BlockSpec(memory_space=pltpu.VMEM)
    dma = pltpu.SemaphoreType.DMA
    atoms, stress = pl.pallas_call(
        kernel,
        out_shape=(
            jax.ShapeDtypeStruct((4, N), F32),
            jax.ShapeDtypeStruct((3, 3), F32),
        ),
        in_specs=[anywhere] * 9,
        out_specs=(vector, vector),
        scratch_shapes=[
            pltpu.SMEM((2,), F32),
            pltpu.SMEM((4,), F32),
            pltpu.VMEM((2, 4, N, N), F32),
            pltpu.VMEM((N, N), jnp.int32),
            pltpu.VMEM((2, N, N), jnp.int32),
            pltpu.VMEM((3, ATOMS), F32),
            pltpu.VMEM((1, ATOMS), jnp.int32),
            pltpu.VMEM((6 * N, 2 * N), BF16),
            pltpu.VMEM((2 * N, 6 * N), BF16),
            pltpu.VMEM((2 * N, 6 * N), BF16),
            pltpu.VMEM((BANDS, 2, N, N), F32),
            pltpu.VMEM((PARTS, 2, N, N), F32),
            pltpu.VMEM((PARTS, 2, N, N), F32),
            pltpu.VMEM((N, ATOMS), F32),
            pltpu.VMEM((N, ATOMS), F32),
            pltpu.VMEM((3 * N, ATOMS), BF16),
            pltpu.VMEM((3 * N, ATOMS), BF16),
            pltpu.VMEM((N, ATOMS), F32),
            pltpu.VMEM((N, ATOMS), F32),
            pltpu.VMEM((N, N), F32),
            pltpu.VMEM((N, N), F32),
            pltpu.VMEM((4, N, N), F32),
            pltpu.VMEM((8, N), F32),
            pltpu.VMEM((8, 8, N), F32),
            pltpu.VMEM((8, N), F32),
            pltpu.VMEM((16, 8, N), F32),
            dma((9,)),
            dma((2,)),
            dma((2,)),
            dma((2,)),
            dma((2,)),
            dma((2,)),
            dma,
            dma((3,)),
            dma((4,)),
        ],
        compiler_params=pltpu.CompilerParams(
            collective_id=0, has_side_effects=True, vmem_limit_bytes=56538000
        ),
    )(
        orbitals,
        occupation,
        g_list.reshape(N, N),
        positions,
        species.reshape(1, ATOMS),
        widths,
        jnp.asarray(right_table),
        jnp.asarray(left_table),
        jnp.asarray(x_table),
    )
    return stress, atoms.reshape(ATOMS)


def solution(mesh):
    return jax.shard_map(
        per_device,
        mesh=mesh,
        in_specs=(P("band", "grid", None, None), P("band"), P("grid"), P(), P(), P()),
        out_specs=(P(), P()),
        check_vma=False,
    )
```

```python
import functools
import math

import jax
import jax.numpy as jnp
import numpy as np
from jax import lax
from jax.experimental import pallas as pl
from jax.experimental.pallas import tpu as pltpu
from jax.sharding import PartitionSpec as P

MESH = pl.DeviceIdType.MESH
N = 128
ATOMS = 512
BANDS = 8
TWO_PI = 2.0 * math.pi
F32 = jnp.float32
BF16 = jnp.bfloat16

MIXED = (((0, 1), (2, 3)), ((0, 2), (1, 3)), ((0, 3), (1, 2)))
WITHIN_PARTS = 10
PARTS = 18


def far_first(moves):
    order = np.random.RandomState(1).permutation(len(moves))
    return sorted((moves[o] for o in order), key=lambda m: -sum(min(v, 4 - v) for v in m[:3]))


MOVES = far_first(
    [(x, y, z, c) for x in range(2) for y in range(4) for z in range(4) for c in range(2) if x + y + z + c]
)
GREETED = far_first(
    [
        (x, y, z, c)
        for x in range(4)
        for y in range(4)
        for z in range(4)
        for c in range(2)
        if x + y + z + c and (x != 2 or y + z == 0)
    ]
)


def table_parts():
    index = np.arange(N)
    angle = 2.0 * np.pi / N * ((index[:, None] * index[None, :]) % N)
    cos, sin = np.cos(angle), np.sin(angle)
    right = np.block([[cos, -sin], [sin, cos]])
    high = np.asarray(right, dtype=jnp.bfloat16)
    low = np.asarray(right - high.astype(np.float64), dtype=jnp.bfloat16)
    right_cat = np.concatenate([high, high, low], axis=0)
    left_cat = np.concatenate([high.T, high.T, low.T], axis=1)
    order = np.concatenate([index[0::2], index[1::2]])
    order = np.concatenate([order, N + order])
    high_x, low_x = high.T[:, order], low.T[:, order]
    cross_cat = np.concatenate([high_x, high_x, low_x], axis=1)
    return right_cat, left_cat, cross_cat


def split(value):
    high = value.astype(BF16)
    low = (value - high.astype(F32)).astype(BF16)
    return high, low


def iota(shape, dim):
    return lax.broadcasted_iota(jnp.int32, shape, dim)


def fold(cell):
    return jnp.where(cell < N // 2, cell, cell - N)


def turns(value):
    return value - jnp.floor(value + 0.5)


def kernel(
    orbitals, occupation_at, g_list, positions, species, widths_at, right_table, left_table, x_table,
    out_atoms, out_stress,
    occupation, widths, orb_v, list_v, neg_v, pos_v, spec_v, right_v, left_v, tx_v,
    psi, y_buf, r_buf, z_re, z_im, zc_re, zc_im, x_re, x_im, col_x, col_z, masks, coefs,
    red_src, red_x, red_mid, red_yz,
    load_sem, mate_sem, cross_send, cross_recv, neg_sem, pass_sem, a2a_send, a2a_recv, red_sem,
):
    band = lax.axis_index("band")
    slab = lax.axis_index("grid")
    half = band // 2
    core = lax.rem(band, 2)
    low = lax.rem(slab // 4, 2)
    pos_x = 2 * half + low
    pos_y = lax.rem(slab, 4)
    pos_z = slab // 8
    owner = 2 * slab + core
    mate = band + 1 - 2 * core

    def device(to_band, to_slab):
        return dict(device_id={"band": to_band, "grid": to_slab}, device_id_type=MESH)

    at_x = [lax.rem(pos_x + move, 4) for move in range(4)]
    at_y = [lax.rem(pos_y + move, 4) for move in range(4)]
    at_z = [8 * lax.rem(pos_z + move, 4) for move in range(4)]
    at_core = [core, 1 - core]
    at_half = [half, 1 - half]
    lows = [[4 * at + y for y in at_y] for at in (low, 1 - low)]

    barrier = pltpu.get_barrier_semaphore()
    loads = [
        pltpu.make_async_copy(src, dst, load_sem.at[k])
        for k, (src, dst) in enumerate(
            (
                (positions, pos_v),
                (species, spec_v),
                (orbitals, orb_v),
                (g_list, list_v),
                (right_table, right_v),
                (left_table, left_v),
                (x_table, tx_v),
                (occupation_at, occupation),
                (widths_at, widths),
            )
        )
    ]
    for k in (7, 2, 4, 5, 3, 0, 1, 8, 6):
        loads[k].start()
    greet_bands = [[2 * (x // 2) + c for c in at_core] for x in at_x]
    greet_slabs = [[4 * lax.rem(x, 2) + y for y in at_y] for x in at_x]
    for dx, dy, dz, dc in GREETED:
        pl.semaphore_signal(
            barrier, 1, **device(greet_bands[dx][dc], greet_slabs[dx][dy] + at_z[dz])
        )

    loads[7].wait()
    loads[2].wait()
    for i in range(2):
        root = jnp.sqrt(jnp.full((N, N), occupation[i], F32))
        for plane in range(4):
            orb_v[i, plane] = orb_v[i, plane] * root
        for plane in range(2):
            psi[2 * band + i, plane] = orb_v[i, 2 * core + plane]

    def transform_yz(transforms, planes):
        blocks = [(transform, plane) for plane in planes for transform in transforms]
        rows = []
        for (_, *pairs), plane in blocks:
            parts = []
            for i, j, scale in pairs:
                rho = psi[i, plane] * psi[j, plane]
                parts.append(rho if scale is None else rho * scale)
            rows.append(jnp.concatenate(parts, axis=1))
        high_part, low_part = split(jnp.concatenate(rows, axis=0))
        along_z = jnp.dot(
            jnp.concatenate([high_part, low_part, high_part], axis=1),
            right_v[...],
            preferred_element_type=F32,
        )
        columns = []
        for n in range(len(blocks)):
            block = along_z[n * N : (n + 1) * N]
            columns.append(jnp.concatenate([block[:, :N], block[:, N:]], axis=0))
        high_part, low_part = split(jnp.concatenate(columns, axis=1))
        along_y = jnp.dot(
            left_v[...],
            jnp.concatenate([high_part, low_part, high_part], axis=0),
            preferred_element_type=F32,
        )
        for n, ((part, *_), plane) in enumerate(blocks):
            y_buf[part, plane] = along_y[:N, n * N : (n + 1) * N]
            y_buf[part + 1, plane] = along_y[N:, n * N : (n + 1) * N]

    def send(first_part, parts, first_plane, planes, chunk, halves, columns):
        for dx, dy, dz, dc in MOVES:
            if dx not in columns:
                continue
            to_slab = lows[dx][dy] + at_z[dz]
            to_core = at_core[dc]
            to_row = pl.multiple_of(4 * to_slab + 2 * to_core, 2)
            my_row = pl.multiple_of(2 * owner, 2)
            where = (pl.ds(first_part, parts), pl.ds(first_plane, planes))
            pltpu.make_async_remote_copy(
                y_buf.at[(*where, pl.ds(to_row, 2))],
                r_buf.at[(*where, pl.ds(my_row, 2))],
                a2a_send,
                a2a_recv.at[chunk],
                **device(2 * halves[dx] + to_core, to_slab),
            ).start()

    loads[4].wait()
    loads[5].wait()
    root_two = math.sqrt(2.0)
    first = 4 * half
    same_half = [half, half]

    def within(part, band_at):
        return (part, (band_at, band_at, None), (band_at + 1, band_at + 1, None))

    transform_yz([within(8 * core, 2 * band)], (0, 1))

    pl.semaphore_wait(barrier, len(GREETED))

    loads[3].wait()
    neg_slab = jnp.where(core == 0, lax.rem(32 - slab, 32), 31 - slab)
    neg_copy = pltpu.make_async_remote_copy(
        list_v, neg_v.at[core], neg_sem.at[0], neg_sem.at[1], **device(band, neg_slab)
    )
    neg_pass = pltpu.make_async_remote_copy(
        neg_v.at[1], neg_v.at[1], pass_sem.at[0], pass_sem.at[1], **device(mate, slab)
    )

    @pl.when(neg_slab != slab)
    def _():
        neg_copy.start()

    @pl.when(neg_slab == slab)
    def _():
        neg_v[core] = list_v[...]

    def trade(to_band, to_core, send_sem, recv_sem):
        return pltpu.make_async_remote_copy(
            orb_v.at[:, pl.ds(2 * to_core, 2)],
            psi.at[pl.ds(2 * band, 2)],
            send_sem,
            recv_sem,
            **device(to_band, slab),
        )

    gives = jnp.logical_or(half == 0, core == low)
    gives_late = jnp.logical_and(half == 0, core == 1)
    gifts = [
        trade(2 * (1 - half) + to_core, to_core, cross_send.at[to_core], cross_recv.at[core])
        for to_core in range(2)
    ]

    @pl.when(jnp.logical_and(gives, jnp.logical_not(gives_late)))
    def _():
        for gift in gifts:
            gift.start()

    mate_trade = trade(mate, 1 - core, mate_sem.at[0], mate_sem.at[1])
    mate_trade.start()
    send(8 * core, 2, 0, 2, 0, same_half, (0, 1))

    mate_trade.wait_recv()
    rest = [within(8 - 8 * core, 2 * mate)]
    for n, ((i, j), (k, m)) in enumerate(MIXED):
        rest.append(
            (2 + 2 * n, (first + i, first + j, root_two), (first + k, first + m, root_two))
        )
    for plane in range(2):
        transform_yz(rest, (plane,))
        send(2 - 2 * core, 8, plane, 1, 0, same_half, (0,))

    @pl.when(gives_late)
    def _():
        for gift in gifts:
            gift.start()

    for plane in range(2):
        send(2 - 2 * core, 8, plane, 1, 0, same_half, (1,))

    loads[0].wait()
    loads[1].wait()
    loads[8].wait()
    kind = spec_v[...]
    width = jnp.zeros((1, ATOMS), F32)
    for s in range(4):
        width = jnp.where(kind == s, widths[s], width)
    spread = -0.5 * width * width
    low_row = iota((8, ATOMS), 0).astype(F32)
    high_row = iota((16, ATOMS), 0)
    high_row = jnp.where(high_row < 8, high_row, high_row - 16).astype(F32)
    for dim, re_ref, im_ref in ((0, x_re, x_im), (2, z_re, z_im)):
        where_at = pos_v[dim : dim + 1, :]
        low_turn = TWO_PI * turns(low_row * where_at)
        high_turn = TWO_PI * turns(high_row * turns(8.0 * where_at))
        low_cos, low_sin = jnp.cos(low_turn), jnp.sin(low_turn)
        high_cos, high_sin = jnp.cos(high_turn), jnp.sin(high_turn)
        for a in range(16):
            wave = (TWO_PI / N) * (low_row + float(8 * (a if a < 8 else a - 16)))
            form = jnp.exp(spread * (wave * wave))
            hc, hs = high_cos[a : a + 1, :], high_sin[a : a + 1, :]
            re_ref[8 * a : 8 * a + 8, :] = (hc * low_cos - hs * low_sin) * form
            im_ref[8 * a : 8 * a + 8, :] = (hc * low_sin + hs * low_cos) * form
    for table, cat in ((z_re, zc_re), (z_im, zc_im)):
        high_part, low_part = split(table[...])
        cat[0:N, :] = high_part
        cat[N : 2 * N, :] = high_part
        cat[2 * N : 3 * N, :] = low_part
    y_waves = []
    at_turn = pos_v[1:2, :]
    for k in range(2):
        freq_y = fold(2 * owner + k)
        high_y = freq_y // 8
        low_y = freq_y - 8 * high_y
        turn_y = TWO_PI * turns(
            low_y.astype(F32) * at_turn + high_y.astype(F32) * turns(8.0 * at_turn)
        )
        wave_y = (TWO_PI / N) * freq_y.astype(F32)
        form_y = jnp.exp(spread * (wave_y * wave_y))
        y_waves.append((wave_y, jnp.cos(turn_y) * form_y, jnp.sin(turn_y) * form_y))

    def mask_of(cells, chosen, columns, negated):
        cell_x = lax.shift_right_logical(cells, 9)
        cell_z = cells & (columns - 1)
        if negated:
            cell_x = (N - cell_x) & (N - 1)
            cell_z = (N - cell_z) & (N - 1)
        col_x[...] = jnp.where(chosen, cell_x, -1).astype(F32)
        col_z[...] = cell_z.astype(F32)
        x_index = iota((N, N), 0).astype(F32).astype(BF16)
        z_index = iota((columns, N), 0).astype(F32).astype(BF16)
        one, zero = jnp.ones((), BF16), jnp.zeros((), BF16)

        def hot(index, block):
            found = []
            for r in range(8):
                row = jnp.broadcast_to(block[r : r + 1, :], (16, N)).astype(BF16)
                rows = jnp.concatenate([row] * (index.shape[0] // 16), axis=0)
                found.append(jnp.where(index == rows, one, zero))
            return found

        def block(step, total):
            first = pl.multiple_of(step * 8, 8)
            hot_x = hot(x_index, col_x[pl.ds(first, 8), :])
            hot_z = hot(z_index, col_z[pl.ds(first, 8), :])
            return total + lax.dot_general(
                jnp.concatenate(hot_x, axis=1),
                jnp.concatenate(hot_z, axis=1),
                (((1,), (1,)), ((), ())),
                preferred_element_type=F32,
            )

        return lax.fori_loop(0, N // 8, block, jnp.zeros((N, columns), F32))

    def own_mask():
        own_cells = list_v[...]
        own_pair = (lax.shift_right_logical(own_cells, 8) & 1) == core
        own_masks = mask_of(own_cells, own_pair, 2 * N, False)
        masks[0] = own_masks[:, :N]
        masks[1] = own_masks[:, N:]

    @pl.when(half == 1)
    def _():
        own_mask()

    cross_bytes = [trade(0, 0, cross_send.at[0], cross_recv.at[k]) for k in range(2)]

    kind_set = half + low - 2 * half * low
    other = 4 + 2 * kind_set
    for pair in range(2):
        for sender in range(2):
            from_both = jnp.logical_and(half == 1, sender == pair)
            from_one = jnp.logical_and(half == 0, low == sender)

            @pl.when(jnp.logical_or(from_both, from_one) if pair == 0 else from_both)
            def _():
                cross_bytes[sender].wait_recv()

        first_part = WITHIN_PARTS + 4 * pair
        transform_yz(
            [
                (first_part + 2 * n, (i, other, root_two), (i, other + 1, root_two))
                for n, i in enumerate((2 * pair, 2 * pair + 1))
            ],
            (0, 1),
        )
        send(first_part, 4, 0, 2, 1 + pair, at_half, (0, 1))

    @pl.when(neg_slab != slab)
    def _():
        neg_copy.wait_recv()

    @pl.when(core == 1)
    def _():
        neg_pass.start()

    @pl.when(half == 0)
    def _():
        own_mask()

    own_row = pl.ds(pl.multiple_of(2 * owner, 2), 2)
    for part in range(PARTS):
        for plane in range(2):
            r_buf[part, plane, own_row, :] = y_buf[part, plane, own_row, :]

    neg_cells = neg_v[core]
    neg_plane = lax.shift_right_logical(neg_cells, 7) & 3
    masks[2] = mask_of(neg_cells, neg_plane == 2 * core, N, True)

    @pl.when(core == 0)
    def _():
        neg_pass.wait_recv()

    neg_cells = neg_v[1]
    neg_plane = lax.shift_right_logical(neg_cells, 7) & 3
    masks[3] = mask_of(neg_cells, neg_plane == 3 - 2 * core, N, True)
    loads[6].wait()

    def arrived(first_part, parts, chunk):
        there = r_buf.at[pl.ds(first_part, parts), :, pl.ds(0, N - 2)]
        pltpu.make_async_copy(there, there, a2a_recv.at[chunk]).wait()

    def power(first_part, count, totals):
        blocks = [(q, k) for q in range(count) for k in range(2)]
        columns = [
            jnp.concatenate(
                [
                    r_buf[first_part + 2 * q + part, plane, pl.ds(k, N // 2, stride=2), :]
                    for part in range(2)
                    for plane in range(2)
                ],
                axis=0,
            )
            for q, k in blocks
        ]
        high_part, low_part = split(jnp.concatenate(columns, axis=1))
        along_x = jnp.dot(
            tx_v[...],
            jnp.concatenate([high_part, low_part, high_part], axis=0),
            preferred_element_type=F32,
        )
        for n, (q, k) in enumerate(blocks):
            real = along_x[:N, n * N : (n + 1) * N]
            imag = along_x[N:, n * N : (n + 1) * N]
            term = real * real + imag * imag
            totals[k] = term if totals[k] is None else totals[k] + term
        return totals

    cell_x = iota((N, N), 0)
    cell_z = iota((N, N), 1)
    wave_x = (TWO_PI / N) * fold(cell_x).astype(F32)
    wave_z = (TWO_PI / N) * fold(cell_z).astype(F32)
    sign_x = jnp.where(cell_x == N // 2, -1.0, 1.0).astype(F32)
    sign_z = jnp.where(cell_z == N // 2, -1.0, 1.0).astype(F32)
    cells = float(N) ** 3
    scale = 0.5 * 4.0 * math.pi / (cells * cells * BANDS)
    wave_xz = wave_x * wave_z
    signs_y = []
    for k in range(2):
        wave_y = y_waves[k][0]
        sign_y = jnp.where(2 * owner + k == N // 2, -1.0, 1.0).astype(F32)
        signs_y.append(sign_y)
        square = wave_x * wave_x + wave_y * wave_y + wave_z * wave_z
        nonzero = square > 0
        inverse = 1.0 / jnp.where(nonzero, square, 1.0)
        weight = jnp.where(nonzero, scale * inverse, 0.0)
        here = weight * masks[k]
        there = weight * masks[2 + k]
        here_two = 2.0 * here * inverse
        there_two = 2.0 * there * inverse
        both_two = here_two + there_two
        total = here + there
        coefs[k, 0] = here
        coefs[k, 1] = there
        coefs[k, 2] = both_two * (wave_x * wave_x) - total
        coefs[k, 3] = wave_y * wave_x * (here_two + there_two * (sign_x * sign_y))
        coefs[k, 4] = wave_xz * (here_two + there_two * (sign_x * sign_z))
        coefs[k, 5] = both_two * (wave_y * wave_y) - total
        coefs[k, 6] = wave_y * wave_z * (here_two + there_two * (sign_z * sign_y))
        coefs[k, 7] = both_two * (wave_z * wave_z) - total

    arrived(0, WITHIN_PARTS, 0)
    spectrum = power(0, 5, [None, None])
    arrived(WITHIN_PARTS, 4, 1)
    spectrum = power(WITHIN_PARTS, 2, spectrum)
    arrived(WITHIN_PARTS + 4, 4, 2)
    spectrum = power(WITHIN_PARTS + 4, 2, spectrum)

    rows_re, rows_im = [], []
    for k in range(2):
        here = spectrum[k] * coefs[k, 0]
        there = spectrum[k] * coefs[k, 1]
        rows_re += [here, there]
        rows_im += [here, there * sign_z]
    stress_terms = [
        spectrum[0] * coefs[0, 2 + n] + spectrum[1] * coefs[1, 2 + n] for n in range(6)
    ]
    lane = iota((1, N), 1)
    stress_row = jnp.zeros((1, N), F32)
    for term, lanes in zip(stress_terms, ((0,), (1, 3), (2, 6), (4,), (5, 7), (8,))):
        value = jnp.sum(jnp.sum(term, axis=0, keepdims=True), axis=1, keepdims=True)
        for at in lanes:
            stress_row = jnp.where(lane == at, value, stress_row)

    def projected(rows, table):
        high_part, low_part = split(jnp.concatenate(rows, axis=0))
        return jnp.dot(
            jnp.concatenate([high_part, low_part, high_part], axis=1),
            table[...],
            preferred_element_type=F32,
        )

    proj_re = projected(rows_re, zc_re)
    proj_im = projected(rows_im, zc_im)
    ex_re, ex_im = x_re[...], x_im[...]
    flip_im = jnp.where(iota((N, ATOMS), 0) == N // 2, -ex_im, ex_im)
    atoms = jnp.zeros((1, ATOMS), F32)
    for n in range(4):
        re_part = proj_re[n * N : (n + 1) * N]
        im_part = proj_im[n * N : (n + 1) * N]
        k = n // 2
        table_im = flip_im if n % 2 else ex_im
        sine = y_waves[k][2] * signs_y[k] if n % 2 else y_waves[k][2]
        real = jnp.sum(ex_re * re_part - table_im * im_part, axis=0, keepdims=True)
        imag = jnp.sum(ex_re * im_part + table_im * re_part, axis=0, keepdims=True)
        atoms = atoms + (real * y_waves[k][1] - imag * sine)
    for r in range(4):
        red_src[r : r + 1, :] = atoms[:, r * N : (r + 1) * N]
    red_src[4:5, :] = stress_row

    def summed(source, parts, moves, slot, stage):
        used = source.at[pl.ds(0, 5)]
        for to_band, to_slab in moves:
            pltpu.make_async_remote_copy(
                used,
                parts.at[slot, pl.ds(0, 5)],
                red_sem.at[2 * stage],
                red_sem.at[2 * stage + 1],
                **device(to_band, to_slab),
            ).start()
        parts[slot, 0:5, :] = source[0:5, :]
        count = len(moves)
        shared = parts.at[pl.ds(0, count), pl.ds(0, 5)]
        pltpu.make_async_copy(shared, shared, red_sem.at[2 * stage + 1]).wait()
        return jnp.sum(parts[:, 0:5, :], axis=0), shared

    moves_x = [
        (greet_bands[dx][dc], greet_slabs[dx][0] + at_z[0])
        for dx in (2, 1, 3, 0)
        for dc in (1, 0)
        if dx + dc
    ]
    moves_yz = [
        (band, lows[0][dy] + at_z[dz])
        for dy, dz in sorted(
            ((dy, dz) for dy in range(4) for dz in range(4) if dy + dz),
            key=lambda m: -sum(min(v, 4 - v) for v in m),
        )
    ]
    middle, sent_x = summed(red_src, red_x, moves_x, 2 * pos_x + core, 0)
    red_mid[0:5, :] = middle
    sums, sent_yz = summed(red_mid, red_yz, moves_yz, 4 * pos_z + pos_y, 1)
    out_atoms[...] = sums[0:4]
    for r in range(3):
        row = sums[4:5, :]
        out_stress[r : r + 1, :] = (row if r == 0 else pltpu.roll(row, N - 3 * r, 1))[:, :3]

    mate_trade.wait_send()

    @pl.when(gives)
    def _():
        for gift in gifts:
            gift.wait_send()

    @pl.when(neg_slab != slab)
    def _():
        neg_copy.wait_send()

    @pl.when(core == 1)
    def _():
        neg_pass.wait_send()

    sent = r_buf.at[:, :, pl.ds(0, N - 2)]
    pltpu.make_async_copy(sent, sent, a2a_send).wait()
    pltpu.make_async_copy(sent_x, sent_x, red_sem.at[0]).wait()
    pltpu.make_async_copy(sent_yz, sent_yz, red_sem.at[2]).wait()


def per_device(orbitals, occupation, g_list, positions, species, widths):
    right_table, left_table, x_table = table_parts()
    anywhere = pl.BlockSpec(memory_space=pltpu.HBM)
    vector = pl.BlockSpec(memory_space=pltpu.VMEM)
    dma = pltpu.SemaphoreType.DMA
    atoms, stress = pl.pallas_call(
        kernel,
        out_shape=(
            jax.ShapeDtypeStruct((4, N), F32),
            jax.ShapeDtypeStruct((3, 3), F32),
        ),
        in_specs=[anywhere] * 9,
        out_specs=(vector, vector),
        scratch_shapes=[
            pltpu.SMEM((2,), F32),
            pltpu.SMEM((4,), F32),
            pltpu.VMEM((2, 4, N, N), F32),
            pltpu.VMEM((N, N), jnp.int32),
            pltpu.VMEM((2, N, N), jnp.int32),
            pltpu.VMEM((3, ATOMS), F32),
            pltpu.VMEM((1, ATOMS), jnp.int32),
            pltpu.VMEM((6 * N, 2 * N), BF16),
            pltpu.VMEM((2 * N, 6 * N), BF16),
            pltpu.VMEM((2 * N, 6 * N), BF16),
            pltpu.VMEM((BANDS, 2, N, N), F32),
            pltpu.VMEM((PARTS, 2, N, N), F32),
            pltpu.VMEM((PARTS, 2, N, N), F32),
            pltpu.VMEM((N, ATOMS), F32),
            pltpu.VMEM((N, ATOMS), F32),
            pltpu.VMEM((3 * N, ATOMS), BF16),
            pltpu.VMEM((3 * N, ATOMS), BF16),
            pltpu.VMEM((N, ATOMS), F32),
            pltpu.VMEM((N, ATOMS), F32),
            pltpu.VMEM((N, N), F32),
            pltpu.VMEM((N, N), F32),
            pltpu.VMEM((4, N, N), F32),
            pltpu.VMEM((2, 8, N, N), F32),
            pltpu.VMEM((8, N), F32),
            pltpu.VMEM((8, 8, N), F32),
            pltpu.VMEM((8, N), F32),
            pltpu.VMEM((16, 8, N), F32),
            dma((9,)),
            dma((2,)),
            dma((2,)),
            dma((2,)),
            dma((2,)),
            dma((2,)),
            dma,
            dma((3,)),
            dma((4,)),
        ],
        compiler_params=pltpu.CompilerParams(
            collective_id=0, has_side_effects=True, vmem_limit_bytes=56538000
        ),
    )(
        orbitals,
        occupation,
        g_list.reshape(N, N),
        positions,
        species.reshape(1, ATOMS),
        widths,
        jnp.asarray(right_table),
        jnp.asarray(left_table),
        jnp.asarray(x_table),
    )
    return stress, atoms.reshape(ATOMS)


def solution(mesh):
    return jax.shard_map(
        per_device,
        mesh=mesh,
        in_specs=(P("band", "grid", None, None), P("band"), P("grid"), P(), P(), P()),
        out_specs=(P(), P()),
        check_vma=False,
    )
```

```python
import functools
import math

import jax
import jax.numpy as jnp
import numpy as np
from jax import lax
from jax.experimental import pallas as pl
from jax.experimental.pallas import tpu as pltpu
from jax.sharding import PartitionSpec as P

MESH = pl.DeviceIdType.MESH
N = 128
ATOMS = 512
BANDS = 8
TWO_PI = 2.0 * math.pi
F32 = jnp.float32
BF16 = jnp.bfloat16

MIXED = (((0, 1), (2, 3)), ((0, 2), (1, 3)), ((0, 3), (1, 2)))
WITHIN_PARTS = 10
PARTS = 18


def far_first(moves):
    order = np.random.RandomState(1).permutation(len(moves))
    return sorted((moves[o] for o in order), key=lambda m: -sum(min(v, 4 - v) for v in m[:3]))


MOVES = far_first(
    [(x, y, z, c) for x in range(2) for y in range(4) for z in range(4) for c in range(2) if x + y + z + c]
)
GREETED = far_first(
    [
        (x, y, z, c)
        for x in range(4)
        for y in range(4)
        for z in range(4)
        for c in range(2)
        if x + y + z + c and (x != 2 or y + z == 0)
    ]
)


def table_parts():
    index = np.arange(N)
    angle = 2.0 * np.pi / N * ((index[:, None] * index[None, :]) % N)
    cos, sin = np.cos(angle), np.sin(angle)
    right = np.block([[cos, -sin], [sin, cos]])
    high = np.asarray(right, dtype=jnp.bfloat16)
    low = np.asarray(right - high.astype(np.float64), dtype=jnp.bfloat16)
    right_cat = np.concatenate([high, high, low], axis=0)
    left_cat = np.concatenate([high.T, high.T, low.T], axis=1)
    order = np.concatenate([index[0::2], index[1::2]])
    order = np.concatenate([order, N + order])
    high_x, low_x = high.T[:, order], low.T[:, order]
    cross_cat = np.concatenate([high_x, high_x, low_x], axis=1)
    return right_cat, left_cat, cross_cat


def split(value):
    high = value.astype(BF16)
    low = (value - high.astype(F32)).astype(BF16)
    return high, low


def iota(shape, dim):
    return lax.broadcasted_iota(jnp.int32, shape, dim)


def fold(cell):
    return jnp.where(cell < N // 2, cell, cell - N)


def turns(value):
    return value - jnp.floor(value + 0.5)


def kernel(
    orbitals, occupation_at, g_list, positions, species, widths_at, right_table, left_table, x_table,
    out_atoms, out_stress,
    occupation, widths, orb_v, list_v, neg_v, pos_v, spec_v, right_v, left_v, tx_v,
    psi, y_buf, r_buf, z_re, z_im, zc_re, zc_im, x_re, x_im, col_x, col_z, masks, coefs,
    red_src, red_x, red_mid, red_yz,
    load_sem, mate_sem, cross_send, cross_recv, neg_sem, pass_sem, a2a_send, a2a_recv, red_sem,
):
    band = lax.axis_index("band")
    slab = lax.axis_index("grid")
    half = band // 2
    core = lax.rem(band, 2)
    low = lax.rem(slab // 4, 2)
    pos_x = 2 * half + low
    pos_y = lax.rem(slab, 4)
    pos_z = slab // 8
    owner = 2 * slab + core
    mate = band + 1 - 2 * core

    def device(to_band, to_slab):
        return dict(device_id={"band": to_band, "grid": to_slab}, device_id_type=MESH)

    at_x = [lax.rem(pos_x + move, 4) for move in range(4)]
    at_y = [lax.rem(pos_y + move, 4) for move in range(4)]
    at_z = [8 * lax.rem(pos_z + move, 4) for move in range(4)]
    at_core = [core, 1 - core]
    at_half = [half, 1 - half]
    lows = [[4 * at + y for y in at_y] for at in (low, 1 - low)]

    barrier = pltpu.get_barrier_semaphore()
    loads = [
        pltpu.make_async_copy(src, dst, load_sem.at[k])
        for k, (src, dst) in enumerate(
            (
                (positions, pos_v),
                (species, spec_v),
                (orbitals, orb_v),
                (g_list, list_v),
                (right_table, right_v),
                (left_table, left_v),
                (x_table, tx_v),
                (occupation_at, occupation),
                (widths_at, widths),
            )
        )
    ]
    for k in (7, 2, 4, 5, 3, 0, 1, 8, 6):
        loads[k].start()
    greet_bands = [[2 * (x // 2) + c for c in at_core] for x in at_x]
    greet_slabs = [[4 * lax.rem(x, 2) + y for y in at_y] for x in at_x]
    for dx, dy, dz, dc in GREETED:
        pl.semaphore_signal(
            barrier, 1, **device(greet_bands[dx][dc], greet_slabs[dx][dy] + at_z[dz])
        )

    loads[7].wait()
    loads[2].wait()
    for i in range(2):
        root = jnp.sqrt(jnp.full((N, N), occupation[i], F32))
        for plane in range(4):
            orb_v[i, plane] = orb_v[i, plane] * root
        for plane in range(2):
            psi[2 * band + i, plane] = orb_v[i, 2 * core + plane]

    def transform_yz(transforms, planes):
        blocks = [(transform, plane) for plane in planes for transform in transforms]
        rows = []
        for (_, *pairs), plane in blocks:
            parts = []
            for i, j, scale in pairs:
                rho = psi[i, plane] * psi[j, plane]
                parts.append(rho if scale is None else rho * scale)
            rows.append(jnp.concatenate(parts, axis=1))
        high_part, low_part = split(jnp.concatenate(rows, axis=0))
        along_z = jnp.dot(
            jnp.concatenate([high_part, low_part, high_part], axis=1),
            right_v[...],
            preferred_element_type=F32,
        )
        columns = []
        for n in range(len(blocks)):
            block = along_z[n * N : (n + 1) * N]
            columns.append(jnp.concatenate([block[:, :N], block[:, N:]], axis=0))
        high_part, low_part = split(jnp.concatenate(columns, axis=1))
        along_y = jnp.dot(
            left_v[...],
            jnp.concatenate([high_part, low_part, high_part], axis=0),
            preferred_element_type=F32,
        )
        for n, ((part, *_), plane) in enumerate(blocks):
            y_buf[part, plane] = along_y[:N, n * N : (n + 1) * N]
            y_buf[part + 1, plane] = along_y[N:, n * N : (n + 1) * N]

    def send(first_part, parts, first_plane, planes, chunk, halves, columns):
        for dx, dy, dz, dc in MOVES:
            if dx not in columns:
                continue
            to_slab = lows[dx][dy] + at_z[dz]
            to_core = at_core[dc]
            to_row = pl.multiple_of(4 * to_slab + 2 * to_core, 2)
            my_row = pl.multiple_of(2 * owner, 2)
            where = (pl.ds(first_part, parts), pl.ds(first_plane, planes))
            pltpu.make_async_remote_copy(
                y_buf.at[(*where, pl.ds(to_row, 2))],
                r_buf.at[(*where, pl.ds(my_row, 2))],
                a2a_send,
                a2a_recv.at[chunk],
                **device(2 * halves[dx] + to_core, to_slab),
            ).start()

    loads[4].wait()
    loads[5].wait()
    root_two = math.sqrt(2.0)
    first = 4 * half
    same_half = [half, half]

    def within(part, band_at):
        return (part, (band_at, band_at, None), (band_at + 1, band_at + 1, None))

    transform_yz([within(8 * core, 2 * band)], (0, 1))

    pl.semaphore_wait(barrier, len(GREETED))

    loads[3].wait()
    neg_slab = jnp.where(core == 0, lax.rem(32 - slab, 32), 31 - slab)
    neg_copy = pltpu.make_async_remote_copy(
        list_v, neg_v.at[core], neg_sem.at[0], neg_sem.at[1], **device(band, neg_slab)
    )
    neg_pass = pltpu.make_async_remote_copy(
        neg_v.at[1], neg_v.at[1], pass_sem.at[0], pass_sem.at[1], **device(mate, slab)
    )

    @pl.when(neg_slab != slab)
    def _():
        neg_copy.start()

    @pl.when(neg_slab == slab)
    def _():
        neg_v[core] = list_v[...]

    def trade(to_band, to_core, send_sem, recv_sem):
        return pltpu.make_async_remote_copy(
            orb_v.at[:, pl.ds(2 * to_core, 2)],
            psi.at[pl.ds(2 * band, 2)],
            send_sem,
            recv_sem,
            **device(to_band, slab),
        )

    gives = jnp.logical_or(half == 0, core == low)
    gives_late = jnp.logical_and(half == 0, core == 1)
    gifts = [
        trade(2 * (1 - half) + to_core, to_core, cross_send.at[to_core], cross_recv.at[core])
        for to_core in range(2)
    ]

    @pl.when(jnp.logical_and(gives, jnp.logical_not(gives_late)))
    def _():
        for gift in gifts:
            gift.start()

    mate_trade = trade(mate, 1 - core, mate_sem.at[0], mate_sem.at[1])
    mate_trade.start()
    send(8 * core, 2, 0, 2, 0, same_half, (0,))

    mate_trade.wait_recv()
    rest = [within(8 - 8 * core, 2 * mate)]
    for n, ((i, j), (k, m)) in enumerate(MIXED):
        rest.append(
            (2 + 2 * n, (first + i, first + j, root_two), (first + k, first + m, root_two))
        )
    for plane in range(2):
        transform_yz(rest, (plane,))
        send(2 - 2 * core, 8, plane, 1, 0, same_half, (0,))

    @pl.when(gives_late)
    def _():
        for gift in gifts:
            gift.start()

    send(8 * core, 2, 0, 2, 0, same_half, (1,))
    for plane in range(2):
        send(2 - 2 * core, 8, plane, 1, 0, same_half, (1,))

    loads[0].wait()
    loads[1].wait()
    loads[8].wait()
    kind = spec_v[...]
    width = jnp.zeros((1, ATOMS), F32)
    for s in range(4):
        width = jnp.where(kind == s, widths[s], width)
    spread = -0.5 * width * width
    low_row = iota((8, ATOMS), 0).astype(F32)
    high_row = iota((16, ATOMS), 0)
    high_row = jnp.where(high_row < 8, high_row, high_row - 16).astype(F32)
    for dim, re_ref, im_ref in ((0, x_re, x_im), (2, z_re, z_im)):
        where_at = pos_v[dim : dim + 1, :]
        low_turn = TWO_PI * turns(low_row * where_at)
        high_turn = TWO_PI * turns(high_row * turns(8.0 * where_at))
        low_cos, low_sin = jnp.cos(low_turn), jnp.sin(low_turn)
        high_cos, high_sin = jnp.cos(high_turn), jnp.sin(high_turn)
        for a in range(16):
            wave = (TWO_PI / N) * (low_row + float(8 * (a if a < 8 else a - 16)))
            form = jnp.exp(spread * (wave * wave))
            hc, hs = high_cos[a : a + 1, :], high_sin[a : a + 1, :]
            re_ref[8 * a : 8 * a + 8, :] = (hc * low_cos - hs * low_sin) * form
            im_ref[8 * a : 8 * a + 8, :] = (hc * low_sin + hs * low_cos) * form
    for table, cat in ((z_re, zc_re), (z_im, zc_im)):
        high_part, low_part = split(table[...])
        cat[0:N, :] = high_part
        cat[N : 2 * N, :] = high_part
        cat[2 * N : 3 * N, :] = low_part
    y_waves = []
    at_turn = pos_v[1:2, :]
    for k in range(2):
        freq_y = fold(2 * owner + k)
        high_y = freq_y // 8
        low_y = freq_y - 8 * high_y
        turn_y = TWO_PI * turns(
            low_y.astype(F32) * at_turn + high_y.astype(F32) * turns(8.0 * at_turn)
        )
        wave_y = (TWO_PI / N) * freq_y.astype(F32)
        form_y = jnp.exp(spread * (wave_y * wave_y))
        y_waves.append((wave_y, jnp.cos(turn_y) * form_y, jnp.sin(turn_y) * form_y))

    def mask_of(cells, chosen, columns, negated):
        cell_x = lax.shift_right_logical(cells, 9)
        cell_z = cells & (columns - 1)
        if negated:
            cell_x = (N - cell_x) & (N - 1)
            cell_z = (N - cell_z) & (N - 1)
        col_x[...] = jnp.where(chosen, cell_x, -1).astype(F32)
        col_z[...] = cell_z.astype(F32)
        x_index = iota((N, N), 0).astype(F32).astype(BF16)
        z_index = iota((columns, N), 0).astype(F32).astype(BF16)
        one, zero = jnp.ones((), BF16), jnp.zeros((), BF16)

        def hot(index, block):
            found = []
            for r in range(8):
                row = jnp.broadcast_to(block[r : r + 1, :], (16, N)).astype(BF16)
                rows = jnp.concatenate([row] * (index.shape[0] // 16), axis=0)
                found.append(jnp.where(index == rows, one, zero))
            return found

        def block(step, total):
            first = pl.multiple_of(step * 8, 8)
            hot_x = hot(x_index, col_x[pl.ds(first, 8), :])
            hot_z = hot(z_index, col_z[pl.ds(first, 8), :])
            return total + lax.dot_general(
                jnp.concatenate(hot_x, axis=1),
                jnp.concatenate(hot_z, axis=1),
                (((1,), (1,)), ((), ())),
                preferred_element_type=F32,
            )

        return lax.fori_loop(0, N // 8, block, jnp.zeros((N, columns), F32))

    def own_mask():
        own_cells = list_v[...]
        own_pair = (lax.shift_right_logical(own_cells, 8) & 1) == core
        own_masks = mask_of(own_cells, own_pair, 2 * N, False)
        masks[0] = own_masks[:, :N]
        masks[1] = own_masks[:, N:]

    def pass_list():
        @pl.when(neg_slab != slab)
        def _():
            neg_copy.wait_recv()

        @pl.when(core == 1)
        def _():
            neg_pass.start()

    def neg_mask(slot, plane, at):
        cells = neg_v[slot]
        masks[at] = mask_of(cells, (lax.shift_right_logical(cells, 7) & 3) == plane, N, True)

    @pl.when(half == 1)
    def _():
        own_mask()

    cross_bytes = [trade(0, 0, cross_send.at[0], cross_recv.at[k]) for k in range(2)]

    kind_set = half + low - 2 * half * low
    other = 4 + 2 * kind_set
    for pair in range(2):
        for sender in range(2):
            from_both = jnp.logical_and(half == 1, sender == pair)
            from_one = jnp.logical_and(half == 0, low == sender)

            @pl.when(jnp.logical_or(from_both, from_one) if pair == 0 else from_both)
            def _():
                cross_bytes[sender].wait_recv()

        first_part = WITHIN_PARTS + 4 * pair
        transform_yz(
            [
                (first_part + 2 * n, (i, other, root_two), (i, other + 1, root_two))
                for n, i in enumerate((2 * pair, 2 * pair + 1))
            ],
            (0, 1),
        )
        send(first_part, 4, 0, 2, 1 + pair, at_half, (0, 1))
        if pair == 0:

            @pl.when(half == 1)
            def _():
                pass_list()
                neg_mask(core, 2 * core, 2)

    @pl.when(half == 0)
    def _():
        pass_list()
        own_mask()
        neg_mask(core, 2 * core, 2)

    own_row = pl.ds(pl.multiple_of(2 * owner, 2), 2)
    for part in range(PARTS):
        for plane in range(2):
            r_buf[part, plane, own_row, :] = y_buf[part, plane, own_row, :]

    @pl.when(core == 0)
    def _():
        neg_pass.wait_recv()

    neg_mask(1, 3 - 2 * core, 3)
    loads[6].wait()

    def arrived(first_part, parts, chunk):
        there = r_buf.at[pl.ds(first_part, parts), :, pl.ds(0, N - 2)]
        pltpu.make_async_copy(there, there, a2a_recv.at[chunk]).wait()

    def power(first_part, count, totals):
        blocks = [(q, k) for q in range(count) for k in range(2)]
        columns = [
            jnp.concatenate(
                [
                    r_buf[first_part + 2 * q + part, plane, pl.ds(k, N // 2, stride=2), :]
                    for part in range(2)
                    for plane in range(2)
                ],
                axis=0,
            )
            for q, k in blocks
        ]
        high_part, low_part = split(jnp.concatenate(columns, axis=1))
        along_x = jnp.dot(
            tx_v[...],
            jnp.concatenate([high_part, low_part, high_part], axis=0),
            preferred_element_type=F32,
        )
        for n, (q, k) in enumerate(blocks):
            real = along_x[:N, n * N : (n + 1) * N]
            imag = along_x[N:, n * N : (n + 1) * N]
            term = real * real + imag * imag
            totals[k] = term if totals[k] is None else totals[k] + term
        return totals

    cell_x = iota((N, N), 0)
    cell_z = iota((N, N), 1)
    wave_x = (TWO_PI / N) * fold(cell_x).astype(F32)
    wave_z = (TWO_PI / N) * fold(cell_z).astype(F32)
    sign_x = jnp.where(cell_x == N // 2, -1.0, 1.0).astype(F32)
    sign_z = jnp.where(cell_z == N // 2, -1.0, 1.0).astype(F32)
    cells = float(N) ** 3
    scale = 0.5 * 4.0 * math.pi / (cells * cells * BANDS)
    wave_xz = wave_x * wave_z
    signs_y = []
    for k in range(2):
        wave_y = y_waves[k][0]
        sign_y = jnp.where(2 * owner + k == N // 2, -1.0, 1.0).astype(F32)
        signs_y.append(sign_y)
        square = wave_x * wave_x + wave_y * wave_y + wave_z * wave_z
        nonzero = square > 0
        inverse = 1.0 / jnp.where(nonzero, square, 1.0)
        weight = jnp.where(nonzero, scale * inverse, 0.0)
        here = weight * masks[k]
        there = weight * masks[2 + k]
        here_two = 2.0 * here * inverse
        there_two = 2.0 * there * inverse
        both_two = here_two + there_two
        total = here + there
        coefs[k, 0] = here
        coefs[k, 1] = there
        coefs[k, 2] = both_two * (wave_x * wave_x) - total
        coefs[k, 3] = wave_y * wave_x * (here_two + there_two * (sign_x * sign_y))
        coefs[k, 4] = wave_xz * (here_two + there_two * (sign_x * sign_z))
        coefs[k, 5] = both_two * (wave_y * wave_y) - total
        coefs[k, 6] = wave_y * wave_z * (here_two + there_two * (sign_z * sign_y))
        coefs[k, 7] = both_two * (wave_z * wave_z) - total

    arrived(0, WITHIN_PARTS, 0)
    spectrum = power(0, 5, [None, None])
    arrived(WITHIN_PARTS, 4, 1)
    spectrum = power(WITHIN_PARTS, 2, spectrum)
    arrived(WITHIN_PARTS + 4, 4, 2)
    spectrum = power(WITHIN_PARTS + 4, 2, spectrum)

    rows_re, rows_im = [], []
    for k in range(2):
        here = spectrum[k] * coefs[k, 0]
        there = spectrum[k] * coefs[k, 1]
        rows_re += [here, there]
        rows_im += [here, there * sign_z]
    stress_terms = [
        spectrum[0] * coefs[0, 2 + n] + spectrum[1] * coefs[1, 2 + n] for n in range(6)
    ]
    lane = iota((1, N), 1)
    stress_row = jnp.zeros((1, N), F32)
    for term, lanes in zip(stress_terms, ((0,), (1, 3), (2, 6), (4,), (5, 7), (8,))):
        value = jnp.sum(jnp.sum(term, axis=0, keepdims=True), axis=1, keepdims=True)
        for at in lanes:
            stress_row = jnp.where(lane == at, value, stress_row)

    def projected(rows, table):
        high_part, low_part = split(jnp.concatenate(rows, axis=0))
        return jnp.dot(
            jnp.concatenate([high_part, low_part, high_part], axis=1),
            table[...],
            preferred_element_type=F32,
        )

    proj_re = projected(rows_re, zc_re)
    proj_im = projected(rows_im, zc_im)
    ex_re, ex_im = x_re[...], x_im[...]
    flip_im = jnp.where(iota((N, ATOMS), 0) == N // 2, -ex_im, ex_im)
    atoms = jnp.zeros((1, ATOMS), F32)
    for n in range(4):
        re_part = proj_re[n * N : (n + 1) * N]
        im_part = proj_im[n * N : (n + 1) * N]
        k = n // 2
        table_im = flip_im if n % 2 else ex_im
        sine = y_waves[k][2] * signs_y[k] if n % 2 else y_waves[k][2]
        real = jnp.sum(ex_re * re_part - table_im * im_part, axis=0, keepdims=True)
        imag = jnp.sum(ex_re * im_part + table_im * re_part, axis=0, keepdims=True)
        atoms = atoms + (real * y_waves[k][1] - imag * sine)
    for r in range(4):
        red_src[r : r + 1, :] = atoms[:, r * N : (r + 1) * N]
    red_src[4:5, :] = stress_row

    def summed(source, parts, moves, slot, stage):
        used = source.at[pl.ds(0, 5)]
        for to_band, to_slab in moves:
            pltpu.make_async_remote_copy(
                used,
                parts.at[slot, pl.ds(0, 5)],
                red_sem.at[2 * stage],
                red_sem.at[2 * stage + 1],
                **device(to_band, to_slab),
            ).start()
        parts[slot, 0:5, :] = source[0:5, :]
        count = len(moves)
        shared = parts.at[pl.ds(0, count), pl.ds(0, 5)]
        pltpu.make_async_copy(shared, shared, red_sem.at[2 * stage + 1]).wait()
        return jnp.sum(parts[:, 0:5, :], axis=0), shared

    moves_x = [
        (greet_bands[dx][dc], greet_slabs[dx][0] + at_z[0])
        for dx in (2, 1, 3, 0)
        for dc in (1, 0)
        if dx + dc
    ]
    moves_yz = [
        (band, lows[0][dy] + at_z[dz])
        for dy, dz in sorted(
            ((dy, dz) for dy in range(4) for dz in range(4) if dy + dz),
            key=lambda m: -sum(min(v, 4 - v) for v in m),
        )
    ]
    middle, sent_x = summed(red_src, red_x, moves_x, 2 * pos_x + core, 0)
    red_mid[0:5, :] = middle
    sums, sent_yz = summed(red_mid, red_yz, moves_yz, 4 * pos_z + pos_y, 1)
    out_atoms[...] = sums[0:4]
    for r in range(3):
        row = sums[4:5, :]
        out_stress[r : r + 1, :] = (row if r == 0 else pltpu.roll(row, N - 3 * r, 1))[:, :3]

    mate_trade.wait_send()

    @pl.when(gives)
    def _():
        for gift in gifts:
            gift.wait_send()

    @pl.when(neg_slab != slab)
    def _():
        neg_copy.wait_send()

    @pl.when(core == 1)
    def _():
        neg_pass.wait_send()

    sent = r_buf.at[:, :, pl.ds(0, N - 2)]
    pltpu.make_async_copy(sent, sent, a2a_send).wait()
    pltpu.make_async_copy(sent_x, sent_x, red_sem.at[0]).wait()
    pltpu.make_async_copy(sent_yz, sent_yz, red_sem.at[2]).wait()


def per_device(orbitals, occupation, g_list, positions, species, widths):
    right_table, left_table, x_table = table_parts()
    anywhere = pl.BlockSpec(memory_space=pltpu.HBM)
    vector = pl.BlockSpec(memory_space=pltpu.VMEM)
    dma = pltpu.SemaphoreType.DMA
    atoms, stress = pl.pallas_call(
        kernel,
        out_shape=(
            jax.ShapeDtypeStruct((4, N), F32),
            jax.ShapeDtypeStruct((3, 3), F32),
        ),
        in_specs=[anywhere] * 9,
        out_specs=(vector, vector),
        scratch_shapes=[
            pltpu.SMEM((2,), F32),
            pltpu.SMEM((4,), F32),
            pltpu.VMEM((2, 4, N, N), F32),
            pltpu.VMEM((N, N), jnp.int32),
            pltpu.VMEM((2, N, N), jnp.int32),
            pltpu.VMEM((3, ATOMS), F32),
            pltpu.VMEM((1, ATOMS), jnp.int32),
            pltpu.VMEM((6 * N, 2 * N), BF16),
            pltpu.VMEM((2 * N, 6 * N), BF16),
            pltpu.VMEM((2 * N, 6 * N), BF16),
            pltpu.VMEM((BANDS, 2, N, N), F32),
            pltpu.VMEM((PARTS, 2, N, N), F32),
            pltpu.VMEM((PARTS, 2, N, N), F32),
            pltpu.VMEM((N, ATOMS), F32),
            pltpu.VMEM((N, ATOMS), F32),
            pltpu.VMEM((3 * N, ATOMS), BF16),
            pltpu.VMEM((3 * N, ATOMS), BF16),
            pltpu.VMEM((N, ATOMS), F32),
            pltpu.VMEM((N, ATOMS), F32),
            pltpu.VMEM((N, N), F32),
            pltpu.VMEM((N, N), F32),
            pltpu.VMEM((4, N, N), F32),
            pltpu.VMEM((2, 8, N, N), F32),
            pltpu.VMEM((8, N), F32),
            pltpu.VMEM((8, 8, N), F32),
            pltpu.VMEM((8, N), F32),
            pltpu.VMEM((16, 8, N), F32),
            dma((9,)),
            dma((2,)),
            dma((2,)),
            dma((2,)),
            dma((2,)),
            dma((2,)),
            dma,
            dma((3,)),
            dma((4,)),
        ],
        compiler_params=pltpu.CompilerParams(
            collective_id=0, has_side_effects=True, vmem_limit_bytes=56538000
        ),
    )(
        orbitals,
        occupation,
        g_list.reshape(N, N),
        positions,
        species.reshape(1, ATOMS),
        widths,
        jnp.asarray(right_table),
        jnp.asarray(left_table),
        jnp.asarray(x_table),
    )
    return stress, atoms.reshape(ATOMS)


def solution(mesh):
    return jax.shard_map(
        per_device,
        mesh=mesh,
        in_specs=(P("band", "grid", None, None), P("band"), P("grid"), P(), P(), P()),
        out_specs=(P(), P()),
        check_vma=False,
    )
```

```python
import functools
import math

import jax
import jax.numpy as jnp
import numpy as np
from jax import lax
from jax.experimental import pallas as pl
from jax.experimental.pallas import tpu as pltpu
from jax.sharding import PartitionSpec as P

MESH = pl.DeviceIdType.MESH
N = 128
ATOMS = 512
BANDS = 8
TWO_PI = 2.0 * math.pi
F32 = jnp.float32
BF16 = jnp.bfloat16

MIXED = (((0, 1), (2, 3)), ((0, 2), (1, 3)), ((0, 3), (1, 2)))
WITHIN_PARTS = 10
PARTS = 18


def far_first(moves):
    order = np.random.RandomState(1).permutation(len(moves))
    return sorted((moves[o] for o in order), key=lambda m: -sum(min(v, 4 - v) for v in m[:3]))


MOVES = far_first(
    [(x, y, z, c) for x in range(2) for y in range(4) for z in range(4) for c in range(2) if x + y + z + c]
)
GREETED = far_first(
    [
        (x, y, z, c)
        for x in range(4)
        for y in range(4)
        for z in range(4)
        for c in range(2)
        if x + y + z + c and (x != 2 or y + z == 0)
    ]
)


def table_parts():
    index = np.arange(N)
    angle = 2.0 * np.pi / N * ((index[:, None] * index[None, :]) % N)
    cos, sin = np.cos(angle), np.sin(angle)
    right = np.block([[cos, -sin], [sin, cos]])
    high = np.asarray(right, dtype=jnp.bfloat16)
    low = np.asarray(right - high.astype(np.float64), dtype=jnp.bfloat16)
    right_cat = np.concatenate([high, high, low], axis=0)
    left_cat = np.concatenate([high.T, high.T, low.T], axis=1)
    order = np.concatenate([index[0::2], index[1::2]])
    order = np.concatenate([order, N + order])
    high_x, low_x = high.T[:, order], low.T[:, order]
    cross_cat = np.concatenate([high_x, high_x, low_x], axis=1)
    return right_cat, left_cat, cross_cat


def split(value):
    high = value.astype(BF16)
    low = (value - high.astype(F32)).astype(BF16)
    return high, low


def iota(shape, dim):
    return lax.broadcasted_iota(jnp.int32, shape, dim)


def fold(cell):
    return jnp.where(cell < N // 2, cell, cell - N)


def turns(value):
    return value - jnp.floor(value + 0.5)


def kernel(
    orbitals, occupation_at, g_list, positions, species, widths_at, right_table, left_table, x_table,
    out_atoms, out_stress,
    occupation, widths, orb_v, list_v, neg_v, pos_v, spec_v, right_v, left_v, tx_v,
    psi, y_buf, r_buf, z_re, z_im, zc_re, zc_im, x_re, x_im, col_x, col_z, masks, coefs,
    red_src, red_x, red_mid, red_yz,
    load_sem, mate_sem, cross_send, cross_recv, neg_sem, pass_sem, a2a_send, a2a_recv, red_sem,
):
    band = lax.axis_index("band")
    slab = lax.axis_index("grid")
    half = band // 2
    core = lax.rem(band, 2)
    low = lax.rem(slab // 4, 2)
    pos_x = 2 * half + low
    pos_y = lax.rem(slab, 4)
    pos_z = slab // 8
    owner = 2 * slab + core
    mate = band + 1 - 2 * core

    def device(to_band, to_slab):
        return dict(device_id={"band": to_band, "grid": to_slab}, device_id_type=MESH)

    at_x = [lax.rem(pos_x + move, 4) for move in range(4)]
    at_y = [lax.rem(pos_y + move, 4) for move in range(4)]
    at_z = [8 * lax.rem(pos_z + move, 4) for move in range(4)]
    at_core = [core, 1 - core]
    at_half = [half, 1 - half]
    lows = [[4 * at + y for y in at_y] for at in (low, 1 - low)]

    barrier = pltpu.get_barrier_semaphore()
    loads = [
        pltpu.make_async_copy(src, dst, load_sem.at[k])
        for k, (src, dst) in enumerate(
            (
                (positions, pos_v),
                (species, spec_v),
                (orbitals, orb_v),
                (g_list, list_v),
                (right_table, right_v),
                (left_table, left_v),
                (x_table, tx_v),
                (occupation_at, occupation),
                (widths_at, widths),
            )
        )
    ]
    for k in (7, 2, 4, 5):
        loads[k].start()
    greet_bands = [[2 * (x // 2) + c for c in at_core] for x in at_x]
    greet_slabs = [[4 * lax.rem(x, 2) + y for y in at_y] for x in at_x]
    for dx, dy, dz, dc in GREETED:
        pl.semaphore_signal(
            barrier, 1, **device(greet_bands[dx][dc], greet_slabs[dx][dy] + at_z[dz])
        )

    for k in (3, 0, 1, 8, 6):
        loads[k].start()

    loads[7].wait()
    loads[2].wait()
    for i in range(2):
        root = jnp.sqrt(jnp.full((N, N), occupation[i], F32))
        for plane in range(4):
            orb_v[i, plane] = orb_v[i, plane] * root
        for plane in range(2):
            psi[2 * band + i, plane] = orb_v[i, 2 * core + plane]

    def transform_yz(transforms, planes):
        blocks = [(transform, plane) for plane in planes for transform in transforms]
        rows = []
        for (_, *pairs), plane in blocks:
            parts = []
            for i, j, scale in pairs:
                rho = psi[i, plane] * psi[j, plane]
                parts.append(rho if scale is None else rho * scale)
            rows.append(jnp.concatenate(parts, axis=1))
        high_part, low_part = split(jnp.concatenate(rows, axis=0))
        along_z = jnp.dot(
            jnp.concatenate([high_part, low_part, high_part], axis=1),
            right_v[...],
            preferred_element_type=F32,
        )
        columns = []
        for n in range(len(blocks)):
            block = along_z[n * N : (n + 1) * N]
            columns.append(jnp.concatenate([block[:, :N], block[:, N:]], axis=0))
        high_part, low_part = split(jnp.concatenate(columns, axis=1))
        along_y = jnp.dot(
            left_v[...],
            jnp.concatenate([high_part, low_part, high_part], axis=0),
            preferred_element_type=F32,
        )
        for n, ((part, *_), plane) in enumerate(blocks):
            y_buf[part, plane] = along_y[:N, n * N : (n + 1) * N]
            y_buf[part + 1, plane] = along_y[N:, n * N : (n + 1) * N]

    def send(first_part, parts, first_plane, planes, chunk, halves, columns):
        for dx, dy, dz, dc in MOVES:
            if dx not in columns:
                continue
            to_slab = lows[dx][dy] + at_z[dz]
            to_core = at_core[dc]
            to_row = pl.multiple_of(4 * to_slab + 2 * to_core, 2)
            my_row = pl.multiple_of(2 * owner, 2)
            where = (pl.ds(first_part, parts), pl.ds(first_plane, planes))
            pltpu.make_async_remote_copy(
                y_buf.at[(*where, pl.ds(to_row, 2))],
                r_buf.at[(*where, pl.ds(my_row, 2))],
                a2a_send,
                a2a_recv.at[chunk],
                **device(2 * halves[dx] + to_core, to_slab),
            ).start()

    loads[4].wait()
    loads[5].wait()
    root_two = math.sqrt(2.0)
    first = 4 * half
    same_half = [half, half]

    def within(part, band_at):
        return (part, (band_at, band_at, None), (band_at + 1, band_at + 1, None))

    transform_yz([within(8 * core, 2 * band)], (0, 1))

    pl.semaphore_wait(barrier, len(GREETED))

    loads[3].wait()
    neg_slab = jnp.where(core == 0, lax.rem(32 - slab, 32), 31 - slab)
    neg_copy = pltpu.make_async_remote_copy(
        list_v, neg_v.at[core], neg_sem.at[0], neg_sem.at[1], **device(band, neg_slab)
    )
    neg_pass = pltpu.make_async_remote_copy(
        neg_v.at[1], neg_v.at[1], pass_sem.at[0], pass_sem.at[1], **device(mate, slab)
    )

    @pl.when(neg_slab != slab)
    def _():
        neg_copy.start()

    @pl.when(neg_slab == slab)
    def _():
        neg_v[core] = list_v[...]

    def trade(to_band, to_core, send_sem, recv_sem):
        return pltpu.make_async_remote_copy(
            orb_v.at[:, pl.ds(2 * to_core, 2)],
            psi.at[pl.ds(2 * band, 2)],
            send_sem,
            recv_sem,
            **device(to_band, slab),
        )

    gives = jnp.logical_or(half == 0, core == low)
    gives_late = jnp.logical_and(half == 0, core == 1)
    gifts = [
        trade(2 * (1 - half) + to_core, to_core, cross_send.at[to_core], cross_recv.at[core])
        for to_core in range(2)
    ]

    @pl.when(jnp.logical_and(gives, jnp.logical_not(gives_late)))
    def _():
        for gift in gifts:
            gift.start()

    mate_trade = trade(mate, 1 - core, mate_sem.at[0], mate_sem.at[1])
    mate_trade.start()
    send(8 * core, 2, 0, 2, 0, same_half, (0,))

    mate_trade.wait_recv()
    rest = [within(8 - 8 * core, 2 * mate)]
    for n, ((i, j), (k, m)) in enumerate(MIXED):
        rest.append(
            (2 + 2 * n, (first + i, first + j, root_two), (first + k, first + m, root_two))
        )
    for plane in range(2):
        transform_yz(rest, (plane,))
        send(2 - 2 * core, 8, plane, 1, 0, same_half, (0,))

    @pl.when(gives_late)
    def _():
        for gift in gifts:
            gift.start()

    send(8 * core, 2, 0, 2, 0, same_half, (1,))
    for plane in range(2):
        send(2 - 2 * core, 8, plane, 1, 0, same_half, (1,))

    loads[0].wait()
    loads[1].wait()
    loads[8].wait()
    kind = spec_v[...]
    width = jnp.zeros((1, ATOMS), F32)
    for s in range(4):
        width = jnp.where(kind == s, widths[s], width)
    spread = -0.5 * width * width
    low_row = iota((8, ATOMS), 0).astype(F32)
    high_row = iota((16, ATOMS), 0)
    high_row = jnp.where(high_row < 8, high_row, high_row - 16).astype(F32)
    for dim, re_ref, im_ref in ((0, x_re, x_im), (2, z_re, z_im)):
        where_at = pos_v[dim : dim + 1, :]
        low_turn = TWO_PI * turns(low_row * where_at)
        high_turn = TWO_PI * turns(high_row * turns(8.0 * where_at))
        low_cos, low_sin = jnp.cos(low_turn), jnp.sin(low_turn)
        high_cos, high_sin = jnp.cos(high_turn), jnp.sin(high_turn)
        for a in range(16):
            wave = (TWO_PI / N) * (low_row + float(8 * (a if a < 8 else a - 16)))
            form = jnp.exp(spread * (wave * wave))
            hc, hs = high_cos[a : a + 1, :], high_sin[a : a + 1, :]
            re_ref[8 * a : 8 * a + 8, :] = (hc * low_cos - hs * low_sin) * form
            im_ref[8 * a : 8 * a + 8, :] = (hc * low_sin + hs * low_cos) * form
    for table, cat in ((z_re, zc_re), (z_im, zc_im)):
        high_part, low_part = split(table[...])
        cat[0:N, :] = high_part
        cat[N : 2 * N, :] = high_part
        cat[2 * N : 3 * N, :] = low_part
    y_waves = []
    at_turn = pos_v[1:2, :]
    for k in range(2):
        freq_y = fold(2 * owner + k)
        high_y = freq_y // 8
        low_y = freq_y - 8 * high_y
        turn_y = TWO_PI * turns(
            low_y.astype(F32) * at_turn + high_y.astype(F32) * turns(8.0 * at_turn)
        )
        wave_y = (TWO_PI / N) * freq_y.astype(F32)
        form_y = jnp.exp(spread * (wave_y * wave_y))
        y_waves.append((wave_y, jnp.cos(turn_y) * form_y, jnp.sin(turn_y) * form_y))

    def mask_of(cells, chosen, columns, negated):
        cell_x = lax.shift_right_logical(cells, 9)
        cell_z = cells & (columns - 1)
        if negated:
            cell_x = (N - cell_x) & (N - 1)
            cell_z = (N - cell_z) & (N - 1)
        col_x[...] = jnp.where(chosen, cell_x, -1).astype(F32)
        col_z[...] = cell_z.astype(F32)
        x_index = iota((N, N), 0).astype(F32).astype(BF16)
        z_index = iota((columns, N), 0).astype(F32).astype(BF16)
        one, zero = jnp.ones((), BF16), jnp.zeros((), BF16)

        def hot(index, block):
            found = []
            for r in range(8):
                row = jnp.broadcast_to(block[r : r + 1, :], (16, N)).astype(BF16)
                rows = jnp.concatenate([row] * (index.shape[0] // 16), axis=0)
                found.append(jnp.where(index == rows, one, zero))
            return found

        def block(step, total):
            first = pl.multiple_of(step * 8, 8)
            hot_x = hot(x_index, col_x[pl.ds(first, 8), :])
            hot_z = hot(z_index, col_z[pl.ds(first, 8), :])
            return total + lax.dot_general(
                jnp.concatenate(hot_x, axis=1),
                jnp.concatenate(hot_z, axis=1),
                (((1,), (1,)), ((), ())),
                preferred_element_type=F32,
            )

        return lax.fori_loop(0, N // 8, block, jnp.zeros((N, columns), F32))

    def own_mask():
        own_cells = list_v[...]
        own_pair = (lax.shift_right_logical(own_cells, 8) & 1) == core
        own_masks = mask_of(own_cells, own_pair, 2 * N, False)
        masks[0] = own_masks[:, :N]
        masks[1] = own_masks[:, N:]

    def pass_list():
        @pl.when(neg_slab != slab)
        def _():
            neg_copy.wait_recv()

        @pl.when(core == 1)
        def _():
            neg_pass.start()

    def neg_mask(slot, plane, at):
        cells = neg_v[slot]
        masks[at] = mask_of(cells, (lax.shift_right_logical(cells, 7) & 3) == plane, N, True)

    @pl.when(half == 1)
    def _():
        own_mask()

    cross_bytes = [trade(0, 0, cross_send.at[0], cross_recv.at[k]) for k in range(2)]

    kind_set = half + low - 2 * half * low
    other = 4 + 2 * kind_set
    for pair in range(2):
        for sender in range(2):
            from_both = jnp.logical_and(half == 1, sender == pair)
            from_one = jnp.logical_and(half == 0, low == sender)

            @pl.when(jnp.logical_or(from_both, from_one) if pair == 0 else from_both)
            def _():
                cross_bytes[sender].wait_recv()

        first_part = WITHIN_PARTS + 4 * pair
        transform_yz(
            [
                (first_part + 2 * n, (i, other, root_two), (i, other + 1, root_two))
                for n, i in enumerate((2 * pair, 2 * pair + 1))
            ],
            (0, 1),
        )
        send(first_part, 4, 0, 2, 1 + pair, at_half, (0, 1))
        if pair == 0:

            @pl.when(half == 1)
            def _():
                pass_list()
                neg_mask(core, 2 * core, 2)

    @pl.when(half == 0)
    def _():
        pass_list()
        own_mask()
        neg_mask(core, 2 * core, 2)

    own_row = pl.ds(pl.multiple_of(2 * owner, 2), 2)
    for part in range(PARTS):
        for plane in range(2):
            r_buf[part, plane, own_row, :] = y_buf[part, plane, own_row, :]

    @pl.when(core == 0)
    def _():
        neg_pass.wait_recv()

    neg_mask(1, 3 - 2 * core, 3)
    loads[6].wait()

    def arrived(first_part, parts, chunk):
        there = r_buf.at[pl.ds(first_part, parts), :, pl.ds(0, N - 2)]
        pltpu.make_async_copy(there, there, a2a_recv.at[chunk]).wait()

    def power(first_part, count, totals):
        blocks = [(q, k) for q in range(count) for k in range(2)]
        columns = [
            jnp.concatenate(
                [
                    r_buf[first_part + 2 * q + part, plane, pl.ds(k, N // 2, stride=2), :]
                    for part in range(2)
                    for plane in range(2)
                ],
                axis=0,
            )
            for q, k in blocks
        ]
        high_part, low_part = split(jnp.concatenate(columns, axis=1))
        along_x = jnp.dot(
            tx_v[...],
            jnp.concatenate([high_part, low_part, high_part], axis=0),
            preferred_element_type=F32,
        )
        for n, (q, k) in enumerate(blocks):
            real = along_x[:N, n * N : (n + 1) * N]
            imag = along_x[N:, n * N : (n + 1) * N]
            term = real * real + imag * imag
            totals[k] = term if totals[k] is None else totals[k] + term
        return totals

    cell_x = iota((N, N), 0)
    cell_z = iota((N, N), 1)
    wave_x = (TWO_PI / N) * fold(cell_x).astype(F32)
    wave_z = (TWO_PI / N) * fold(cell_z).astype(F32)
    sign_x = jnp.where(cell_x == N // 2, -1.0, 1.0).astype(F32)
    sign_z = jnp.where(cell_z == N // 2, -1.0, 1.0).astype(F32)
    cells = float(N) ** 3
    scale = 0.5 * 4.0 * math.pi / (cells * cells * BANDS)
    wave_xz = wave_x * wave_z
    signs_y = []
    for k in range(2):
        wave_y = y_waves[k][0]
        sign_y = jnp.where(2 * owner + k == N // 2, -1.0, 1.0).astype(F32)
        signs_y.append(sign_y)
        square = wave_x * wave_x + wave_y * wave_y + wave_z * wave_z
        nonzero = square > 0
        inverse = 1.0 / jnp.where(nonzero, square, 1.0)
        weight = jnp.where(nonzero, scale * inverse, 0.0)
        here = weight * masks[k]
        there = weight * masks[2 + k]
        here_two = 2.0 * here * inverse
        there_two = 2.0 * there * inverse
        both_two = here_two + there_two
        total = here + there
        coefs[k, 0] = here
        coefs[k, 1] = there
        coefs[k, 2] = both_two * (wave_x * wave_x) - total
        coefs[k, 3] = wave_y * wave_x * (here_two + there_two * (sign_x * sign_y))
        coefs[k, 4] = wave_xz * (here_two + there_two * (sign_x * sign_z))
        coefs[k, 5] = both_two * (wave_y * wave_y) - total
        coefs[k, 6] = wave_y * wave_z * (here_two + there_two * (sign_z * sign_y))
        coefs[k, 7] = both_two * (wave_z * wave_z) - total

    arrived(0, WITHIN_PARTS, 0)
    spectrum = power(0, 5, [None, None])
    arrived(WITHIN_PARTS, 4, 1)
    spectrum = power(WITHIN_PARTS, 2, spectrum)
    arrived(WITHIN_PARTS + 4, 4, 2)
    spectrum = power(WITHIN_PARTS + 4, 2, spectrum)

    rows_re, rows_im = [], []
    for k in range(2):
        here = spectrum[k] * coefs[k, 0]
        there = spectrum[k] * coefs[k, 1]
        rows_re += [here, there]
        rows_im += [here, there * sign_z]
    stress_terms = [
        spectrum[0] * coefs[0, 2 + n] + spectrum[1] * coefs[1, 2 + n] for n in range(6)
    ]
    lane = iota((1, N), 1)
    stress_row = jnp.zeros((1, N), F32)
    for term, lanes in zip(stress_terms, ((0,), (1, 3), (2, 6), (4,), (5, 7), (8,))):
        value = jnp.sum(jnp.sum(term, axis=0, keepdims=True), axis=1, keepdims=True)
        for at in lanes:
            stress_row = jnp.where(lane == at, value, stress_row)

    def projected(rows, table):
        high_part, low_part = split(jnp.concatenate(rows, axis=0))
        return jnp.dot(
            jnp.concatenate([high_part, low_part, high_part], axis=1),
            table[...],
            preferred_element_type=F32,
        )

    proj_re = projected(rows_re, zc_re)
    proj_im = projected(rows_im, zc_im)
    ex_re, ex_im = x_re[...], x_im[...]
    flip_im = jnp.where(iota((N, ATOMS), 0) == N // 2, -ex_im, ex_im)
    atoms = jnp.zeros((1, ATOMS), F32)
    for n in range(4):
        re_part = proj_re[n * N : (n + 1) * N]
        im_part = proj_im[n * N : (n + 1) * N]
        k = n // 2
        table_im = flip_im if n % 2 else ex_im
        sine = y_waves[k][2] * signs_y[k] if n % 2 else y_waves[k][2]
        real = jnp.sum(ex_re * re_part - table_im * im_part, axis=0, keepdims=True)
        imag = jnp.sum(ex_re * im_part + table_im * re_part, axis=0, keepdims=True)
        atoms = atoms + (real * y_waves[k][1] - imag * sine)
    for r in range(4):
        red_src[r : r + 1, :] = atoms[:, r * N : (r + 1) * N]
    red_src[4:5, :] = stress_row

    def summed(source, parts, moves, slot, stage):
        used = source.at[pl.ds(0, 5)]
        for to_band, to_slab in moves:
            pltpu.make_async_remote_copy(
                used,
                parts.at[slot, pl.ds(0, 5)],
                red_sem.at[2 * stage],
                red_sem.at[2 * stage + 1],
                **device(to_band, to_slab),
            ).start()
        parts[slot, 0:5, :] = source[0:5, :]
        count = len(moves)
        shared = parts.at[pl.ds(0, count), pl.ds(0, 5)]
        pltpu.make_async_copy(shared, shared, red_sem.at[2 * stage + 1]).wait()
        return jnp.sum(parts[:, 0:5, :], axis=0), shared

    moves_x = [
        (greet_bands[dx][dc], greet_slabs[dx][0] + at_z[0])
        for dx in (2, 1, 3, 0)
        for dc in (1, 0)
        if dx + dc
    ]
    moves_yz = [
        (band, lows[0][dy] + at_z[dz])
        for dy, dz in sorted(
            ((dy, dz) for dy in range(4) for dz in range(4) if dy + dz),
            key=lambda m: -sum(min(v, 4 - v) for v in m),
        )
    ]
    middle, sent_x = summed(red_src, red_x, moves_x, 2 * pos_x + core, 0)
    red_mid[0:5, :] = middle
    sums, sent_yz = summed(red_mid, red_yz, moves_yz, 4 * pos_z + pos_y, 1)
    out_atoms[...] = sums[0:4]
    for r in range(3):
        row = sums[4:5, :]
        out_stress[r : r + 1, :] = (row if r == 0 else pltpu.roll(row, N - 3 * r, 1))[:, :3]

    mate_trade.wait_send()

    @pl.when(gives)
    def _():
        for gift in gifts:
            gift.wait_send()

    @pl.when(neg_slab != slab)
    def _():
        neg_copy.wait_send()

    @pl.when(core == 1)
    def _():
        neg_pass.wait_send()

    sent = r_buf.at[:, :, pl.ds(0, N - 2)]
    pltpu.make_async_copy(sent, sent, a2a_send).wait()
    pltpu.make_async_copy(sent_x, sent_x, red_sem.at[0]).wait()
    pltpu.make_async_copy(sent_yz, sent_yz, red_sem.at[2]).wait()


def per_device(orbitals, occupation, g_list, positions, species, widths):
    right_table, left_table, x_table = table_parts()
    anywhere = pl.BlockSpec(memory_space=pltpu.HBM)
    vector = pl.BlockSpec(memory_space=pltpu.VMEM)
    dma = pltpu.SemaphoreType.DMA
    atoms, stress = pl.pallas_call(
        kernel,
        out_shape=(
            jax.ShapeDtypeStruct((4, N), F32),
            jax.ShapeDtypeStruct((3, 3), F32),
        ),
        in_specs=[anywhere] * 9,
        out_specs=(vector, vector),
        scratch_shapes=[
            pltpu.SMEM((2,), F32),
            pltpu.SMEM((4,), F32),
            pltpu.VMEM((2, 4, N, N), F32),
            pltpu.VMEM((N, N), jnp.int32),
            pltpu.VMEM((2, N, N), jnp.int32),
            pltpu.VMEM((3, ATOMS), F32),
            pltpu.VMEM((1, ATOMS), jnp.int32),
            pltpu.VMEM((6 * N, 2 * N), BF16),
            pltpu.VMEM((2 * N, 6 * N), BF16),
            pltpu.VMEM((2 * N, 6 * N), BF16),
            pltpu.VMEM((BANDS, 2, N, N), F32),
            pltpu.VMEM((PARTS, 2, N, N), F32),
            pltpu.VMEM((PARTS, 2, N, N), F32),
            pltpu.VMEM((N, ATOMS), F32),
            pltpu.VMEM((N, ATOMS), F32),
            pltpu.VMEM((3 * N, ATOMS), BF16),
            pltpu.VMEM((3 * N, ATOMS), BF16),
            pltpu.VMEM((N, ATOMS), F32),
            pltpu.VMEM((N, ATOMS), F32),
            pltpu.VMEM((N, N), F32),
            pltpu.VMEM((N, N), F32),
            pltpu.VMEM((4, N, N), F32),
            pltpu.VMEM((2, 8, N, N), F32),
            pltpu.VMEM((8, N), F32),
            pltpu.VMEM((8, 8, N), F32),
            pltpu.VMEM((8, N), F32),
            pltpu.VMEM((16, 8, N), F32),
            dma((9,)),
            dma((2,)),
            dma((2,)),
            dma((2,)),
            dma((2,)),
            dma((2,)),
            dma,
            dma((3,)),
            dma((4,)),
        ],
        compiler_params=pltpu.CompilerParams(
            collective_id=0, has_side_effects=True, vmem_limit_bytes=48 << 20
        ),
    )(
        *(
            pltpu.with_memory_space_constraint(operand, pltpu.HBM)
            for operand in (
                orbitals,
                occupation,
                g_list.reshape(N, N),
                positions,
                species.reshape(1, ATOMS),
                widths,
                jnp.asarray(right_table),
                jnp.asarray(left_table),
                jnp.asarray(x_table),
            )
        )
    )
    return stress, atoms.reshape(ATOMS)


def solution(mesh):
    return jax.shard_map(
        per_device,
        mesh=mesh,
        in_specs=(P("band", "grid", None, None), P("band"), P("grid"), P(), P(), P()),
        out_specs=(P(), P()),
        check_vma=False,
    )
```

```python
import functools
import math

import jax
import jax.numpy as jnp
import numpy as np
from jax import lax
from jax.experimental import pallas as pl
from jax.experimental.pallas import tpu as pltpu
from jax.sharding import PartitionSpec as P

MESH = pl.DeviceIdType.MESH
N = 128
ATOMS = 512
BANDS = 8
TWO_PI = 2.0 * math.pi
F32 = jnp.float32
BF16 = jnp.bfloat16

MIXED = (((0, 1), (2, 3)), ((0, 2), (1, 3)), ((0, 3), (1, 2)))
WITHIN_PARTS = 10
PARTS = 18


def far_first(moves):
    order = np.random.RandomState(1).permutation(len(moves))
    return sorted((moves[o] for o in order), key=lambda m: -sum(min(v, 4 - v) for v in m[:3]))


MOVES = far_first(
    [(x, y, z, c) for x in range(2) for y in range(4) for z in range(4) for c in range(2) if x + y + z + c]
)
GREETED = far_first(
    [
        (x, y, z, c)
        for x in range(4)
        for y in range(4)
        for z in range(4)
        for c in range(2)
        if x + y + z + c and (x != 2 or y + z == 0)
    ]
)


def table_parts():
    index = np.arange(N)
    angle = 2.0 * np.pi / N * ((index[:, None] * index[None, :]) % N)
    cos, sin = np.cos(angle), np.sin(angle)
    right = np.block([[cos, -sin], [sin, cos]])
    high = np.asarray(right, dtype=jnp.bfloat16)
    low = np.asarray(right - high.astype(np.float64), dtype=jnp.bfloat16)
    right_cat = np.concatenate([high, high, low], axis=0)
    left_cat = np.concatenate([high.T, high.T, low.T], axis=1)
    order = np.concatenate([index[0::2], index[1::2]])
    order = np.concatenate([order, N + order])
    high_x, low_x = high.T[:, order], low.T[:, order]
    cross_cat = np.concatenate([high_x, high_x, low_x], axis=1)
    return right_cat, left_cat, cross_cat


def split(value):
    high = value.astype(BF16)
    low = (value - high.astype(F32)).astype(BF16)
    return high, low


def iota(shape, dim):
    return lax.broadcasted_iota(jnp.int32, shape, dim)


def fold(cell):
    return jnp.where(cell < N // 2, cell, cell - N)


def turns(value):
    return value - jnp.floor(value + 0.5)


def kernel(
    orbitals, occupation_at, g_list, positions, species, widths_at, right_table, left_table, x_table,
    out_atoms, out_stress,
    occupation, widths, orb_v, list_v, neg_v, pos_v, spec_v, right_v, left_v, tx_v,
    psi, y_buf, r_buf, z_re, z_im, zc_re, zc_im, x_re, x_im, x_flip, col_x, col_z, masks, coefs,
    red_src, red_x, red_mid, red_yz,
    load_sem, mate_sem, cross_send, cross_recv, neg_sem, pass_sem, a2a_send, a2a_recv, red_sem,
):
    band = lax.axis_index("band")
    slab = lax.axis_index("grid")
    half = band // 2
    core = lax.rem(band, 2)
    low = lax.rem(slab // 4, 2)
    pos_x = 2 * half + low
    pos_y = lax.rem(slab, 4)
    pos_z = slab // 8
    owner = 2 * slab + core
    mate = band + 1 - 2 * core

    def device(to_band, to_slab):
        return dict(device_id={"band": to_band, "grid": to_slab}, device_id_type=MESH)

    at_x = [lax.rem(pos_x + move, 4) for move in range(4)]
    at_y = [lax.rem(pos_y + move, 4) for move in range(4)]
    at_z = [8 * lax.rem(pos_z + move, 4) for move in range(4)]
    at_core = [core, 1 - core]
    at_half = [half, 1 - half]
    lows = [[4 * at + y for y in at_y] for at in (low, 1 - low)]

    barrier = pltpu.get_barrier_semaphore()
    loads = [
        pltpu.make_async_copy(src, dst, load_sem.at[k])
        for k, (src, dst) in enumerate(
            (
                (positions, pos_v),
                (species, spec_v),
                (orbitals, orb_v),
                (g_list, list_v),
                (right_table, right_v),
                (left_table, left_v),
                (x_table, tx_v),
                (occupation_at, occupation),
                (widths_at, widths),
            )
        )
    ]
    for k in (7, 2, 4, 5):
        loads[k].start()
    greet_bands = [[2 * (x // 2) + c for c in at_core] for x in at_x]
    greet_slabs = [[4 * lax.rem(x, 2) + y for y in at_y] for x in at_x]
    for dx, dy, dz, dc in GREETED:
        pl.semaphore_signal(
            barrier, 1, **device(greet_bands[dx][dc], greet_slabs[dx][dy] + at_z[dz])
        )

    for k in (3, 0, 1, 8, 6):
        loads[k].start()

    loads[7].wait()
    loads[2].wait()
    for i in range(2):
        root = jnp.sqrt(jnp.full((N, N), occupation[i], F32))
        for plane in range(4):
            orb_v[i, plane] = orb_v[i, plane] * root
        for plane in range(2):
            psi[2 * band + i, plane] = orb_v[i, 2 * core + plane]

    def transform_yz(transforms, planes):
        blocks = [(transform, plane) for plane in planes for transform in transforms]
        rows = []
        for (_, *pairs), plane in blocks:
            parts = []
            for i, j, scale in pairs:
                rho = psi[i, plane] * psi[j, plane]
                parts.append(rho if scale is None else rho * scale)
            rows.append(jnp.concatenate(parts, axis=1))
        high_part, low_part = split(jnp.concatenate(rows, axis=0))
        along_z = jnp.dot(
            jnp.concatenate([high_part, low_part, high_part], axis=1),
            right_v[...],
            preferred_element_type=F32,
        )
        columns = []
        for n in range(len(blocks)):
            block = along_z[n * N : (n + 1) * N]
            columns.append(jnp.concatenate([block[:, :N], block[:, N:]], axis=0))
        high_part, low_part = split(jnp.concatenate(columns, axis=1))
        along_y = jnp.dot(
            left_v[...],
            jnp.concatenate([high_part, low_part, high_part], axis=0),
            preferred_element_type=F32,
        )
        for n, ((part, *_), plane) in enumerate(blocks):
            y_buf[part, plane] = along_y[:N, n * N : (n + 1) * N]
            y_buf[part + 1, plane] = along_y[N:, n * N : (n + 1) * N]

    def send(first_part, parts, first_plane, planes, chunk, halves, columns):
        for dx, dy, dz, dc in MOVES:
            if dx not in columns:
                continue
            to_slab = lows[dx][dy] + at_z[dz]
            to_core = at_core[dc]
            to_row = pl.multiple_of(4 * to_slab + 2 * to_core, 2)
            my_row = pl.multiple_of(2 * owner, 2)
            where = (pl.ds(first_part, parts), pl.ds(first_plane, planes))
            pltpu.make_async_remote_copy(
                y_buf.at[(*where, pl.ds(to_row, 2))],
                r_buf.at[(*where, pl.ds(my_row, 2))],
                a2a_send,
                a2a_recv.at[chunk],
                **device(2 * halves[dx] + to_core, to_slab),
            ).start()

    loads[4].wait()
    loads[5].wait()
    root_two = math.sqrt(2.0)
    first = 4 * half
    same_half = [half, half]

    def within(part, band_at):
        return (part, (band_at, band_at, None), (band_at + 1, band_at + 1, None))

    transform_yz([within(8 * core, 2 * band)], (0, 1))

    pl.semaphore_wait(barrier, len(GREETED))

    def trade(to_band, to_core, send_sem, recv_sem):
        return pltpu.make_async_remote_copy(
            orb_v.at[:, pl.ds(2 * to_core, 2)],
            psi.at[pl.ds(2 * band, 2)],
            send_sem,
            recv_sem,
            **device(to_band, slab),
        )

    mate_trade = trade(mate, 1 - core, mate_sem.at[0], mate_sem.at[1])
    mate_trade.start()

    loads[3].wait()
    neg_slab = jnp.where(core == 0, lax.rem(32 - slab, 32), 31 - slab)
    neg_copy = pltpu.make_async_remote_copy(
        list_v, neg_v.at[core], neg_sem.at[0], neg_sem.at[1], **device(band, neg_slab)
    )
    neg_pass = pltpu.make_async_remote_copy(
        neg_v.at[1], neg_v.at[1], pass_sem.at[0], pass_sem.at[1], **device(mate, slab)
    )

    @pl.when(neg_slab != slab)
    def _():
        neg_copy.start()

    @pl.when(neg_slab == slab)
    def _():
        neg_v[core] = list_v[...]

    gives = jnp.logical_or(half == 0, core == low)
    gives_late = jnp.logical_and(half == 0, core == 1)
    gifts = [
        trade(2 * (1 - half) + to_core, to_core, cross_send.at[to_core], cross_recv.at[core])
        for to_core in range(2)
    ]

    @pl.when(jnp.logical_and(gives, jnp.logical_not(gives_late)))
    def _():
        for gift in gifts:
            gift.start()

    send(8 * core, 2, 0, 2, 0, same_half, (0,))

    mate_trade.wait_recv()
    rest = [within(8 - 8 * core, 2 * mate)]
    for n, ((i, j), (k, m)) in enumerate(MIXED):
        rest.append(
            (2 + 2 * n, (first + i, first + j, root_two), (first + k, first + m, root_two))
        )
    for plane in range(2):
        transform_yz(rest, (plane,))
        send(2 - 2 * core, 8, plane, 1, 0, same_half, (0,))

    @pl.when(gives_late)
    def _():
        for gift in gifts:
            gift.start()

    send(8 * core, 2, 0, 2, 0, same_half, (1,))
    for plane in range(2):
        send(2 - 2 * core, 8, plane, 1, 0, same_half, (1,))

    loads[0].wait()
    loads[1].wait()
    loads[8].wait()
    kind = spec_v[...]
    width = jnp.zeros((1, ATOMS), F32)
    for s in range(4):
        width = jnp.where(kind == s, widths[s], width)
    spread = -0.5 * width * width
    low_row = iota((8, ATOMS), 0).astype(F32)
    high_row = iota((16, ATOMS), 0)
    high_row = jnp.where(high_row < 8, high_row, high_row - 16).astype(F32)
    for dim, re_ref, im_ref in ((0, x_re, x_im), (2, z_re, z_im)):
        where_at = pos_v[dim : dim + 1, :]
        low_turn = TWO_PI * turns(low_row * where_at)
        high_turn = TWO_PI * turns(high_row * turns(8.0 * where_at))
        low_cos, low_sin = jnp.cos(low_turn), jnp.sin(low_turn)
        high_cos, high_sin = jnp.cos(high_turn), jnp.sin(high_turn)
        for a in range(16):
            wave = (TWO_PI / N) * (low_row + float(8 * (a if a < 8 else a - 16)))
            form = jnp.exp(spread * (wave * wave))
            hc, hs = high_cos[a : a + 1, :], high_sin[a : a + 1, :]
            re_ref[8 * a : 8 * a + 8, :] = (hc * low_cos - hs * low_sin) * form
            im_ref[8 * a : 8 * a + 8, :] = (hc * low_sin + hs * low_cos) * form
    for table, cat in ((z_re, zc_re), (z_im, zc_im)):
        high_part, low_part = split(table[...])
        cat[0:N, :] = high_part
        cat[N : 2 * N, :] = high_part
        cat[2 * N : 3 * N, :] = low_part
    y_waves = []
    at_turn = pos_v[1:2, :]
    for k in range(2):
        freq_y = fold(2 * owner + k)
        high_y = freq_y // 8
        low_y = freq_y - 8 * high_y
        turn_y = TWO_PI * turns(
            low_y.astype(F32) * at_turn + high_y.astype(F32) * turns(8.0 * at_turn)
        )
        wave_y = (TWO_PI / N) * freq_y.astype(F32)
        form_y = jnp.exp(spread * (wave_y * wave_y))
        y_waves.append((wave_y, jnp.cos(turn_y) * form_y, jnp.sin(turn_y) * form_y))

    def mask_of(cells, chosen, columns, negated):
        cell_x = lax.shift_right_logical(cells, 9)
        cell_z = cells & (columns - 1)
        if negated:
            cell_x = (N - cell_x) & (N - 1)
            cell_z = (N - cell_z) & (N - 1)
        col_x[...] = jnp.where(chosen, cell_x, -1).astype(F32)
        col_z[...] = cell_z.astype(F32)
        x_index = iota((N, N), 0).astype(F32).astype(BF16)
        z_index = iota((columns, N), 0).astype(F32).astype(BF16)
        one, zero = jnp.ones((), BF16), jnp.zeros((), BF16)

        def hot(index, block):
            found = []
            for r in range(8):
                row = jnp.broadcast_to(block[r : r + 1, :], (16, N)).astype(BF16)
                rows = jnp.concatenate([row] * (index.shape[0] // 16), axis=0)
                found.append(jnp.where(index == rows, one, zero))
            return found

        def block(step, total):
            first = pl.multiple_of(step * 8, 8)
            hot_x = hot(x_index, col_x[pl.ds(first, 8), :])
            hot_z = hot(z_index, col_z[pl.ds(first, 8), :])
            return total + lax.dot_general(
                jnp.concatenate(hot_x, axis=1),
                jnp.concatenate(hot_z, axis=1),
                (((1,), (1,)), ((), ())),
                preferred_element_type=F32,
            )

        return lax.fori_loop(0, N // 8, block, jnp.zeros((N, columns), F32))

    def own_mask():
        own_cells = list_v[...]
        own_pair = (lax.shift_right_logical(own_cells, 8) & 1) == core
        own_masks = mask_of(own_cells, own_pair, 2 * N, False)
        masks[0] = own_masks[:, :N]
        masks[1] = own_masks[:, N:]

    def pass_list():
        @pl.when(neg_slab != slab)
        def _():
            neg_copy.wait_recv()

        @pl.when(core == 1)
        def _():
            neg_pass.start()

    def neg_mask(slot, plane, at):
        cells = neg_v[slot]
        masks[at] = mask_of(cells, (lax.shift_right_logical(cells, 7) & 3) == plane, N, True)

    @pl.when(half == 1)
    def _():
        own_mask()

    cross_bytes = [trade(0, 0, cross_send.at[0], cross_recv.at[k]) for k in range(2)]

    kind_set = half + low - 2 * half * low
    other = 4 + 2 * kind_set
    for pair in range(2):
        for sender in range(2):
            from_both = jnp.logical_and(half == 1, sender == pair)
            from_one = jnp.logical_and(half == 0, low == sender)

            @pl.when(jnp.logical_or(from_both, from_one) if pair == 0 else from_both)
            def _():
                cross_bytes[sender].wait_recv()

        first_part = WITHIN_PARTS + 4 * pair
        transform_yz(
            [
                (first_part + 2 * n, (i, other, root_two), (i, other + 1, root_two))
                for n, i in enumerate((2 * pair, 2 * pair + 1))
            ],
            (0, 1),
        )
        send(first_part, 4, 0, 2, 1 + pair, at_half, (0, 1))
        if pair == 0:

            @pl.when(half == 1)
            def _():
                pass_list()
                neg_mask(core, 2 * core, 2)

    @pl.when(half == 0)
    def _():
        pass_list()
        own_mask()
        neg_mask(core, 2 * core, 2)

    own_row = pl.ds(pl.multiple_of(2 * owner, 2), 2)
    for part in range(PARTS):
        for plane in range(2):
            r_buf[part, plane, own_row, :] = y_buf[part, plane, own_row, :]

    @pl.when(core == 0)
    def _():
        neg_pass.wait_recv()

    neg_mask(1, 3 - 2 * core, 3)
    loads[6].wait()

    def arrived(first_part, parts, chunk):
        there = r_buf.at[pl.ds(first_part, parts), :, pl.ds(0, N - 2)]
        pltpu.make_async_copy(there, there, a2a_recv.at[chunk]).wait()

    def power(first_part, count, totals):
        blocks = [(q, k) for q in range(count) for k in range(2)]
        columns = [
            jnp.concatenate(
                [
                    r_buf[first_part + 2 * q + part, plane, pl.ds(k, N // 2, stride=2), :]
                    for part in range(2)
                    for plane in range(2)
                ],
                axis=0,
            )
            for q, k in blocks
        ]
        high_part, low_part = split(jnp.concatenate(columns, axis=1))
        along_x = jnp.dot(
            tx_v[...],
            jnp.concatenate([high_part, low_part, high_part], axis=0),
            preferred_element_type=F32,
        )
        for n, (q, k) in enumerate(blocks):
            real = along_x[:N, n * N : (n + 1) * N]
            imag = along_x[N:, n * N : (n + 1) * N]
            term = real * real + imag * imag
            totals[k] = term if totals[k] is None else totals[k] + term
        return totals

    x_flip[...] = jnp.where(iota((N, ATOMS), 0) == N // 2, -x_im[...], x_im[...])

    cell_x = iota((N, N), 0)
    cell_z = iota((N, N), 1)
    wave_x = (TWO_PI / N) * fold(cell_x).astype(F32)
    wave_z = (TWO_PI / N) * fold(cell_z).astype(F32)
    sign_x = jnp.where(cell_x == N // 2, -1.0, 1.0).astype(F32)
    sign_z = jnp.where(cell_z == N // 2, -1.0, 1.0).astype(F32)
    cells = float(N) ** 3
    scale = 0.5 * 4.0 * math.pi / (cells * cells * BANDS)
    wave_xz = wave_x * wave_z
    signs_y = []
    for k in range(2):
        wave_y = y_waves[k][0]
        sign_y = jnp.where(2 * owner + k == N // 2, -1.0, 1.0).astype(F32)
        signs_y.append(sign_y)
        square = wave_x * wave_x + wave_y * wave_y + wave_z * wave_z
        nonzero = square > 0
        inverse = 1.0 / jnp.where(nonzero, square, 1.0)
        weight = jnp.where(nonzero, scale * inverse, 0.0)
        here = weight * masks[k]
        there = weight * masks[2 + k]
        here_two = 2.0 * here * inverse
        there_two = 2.0 * there * inverse
        both_two = here_two + there_two
        total = here + there
        coefs[k, 0] = here
        coefs[k, 1] = there
        coefs[k, 2] = both_two * (wave_x * wave_x) - total
        coefs[k, 3] = wave_y * wave_x * (here_two + there_two * (sign_x * sign_y))
        coefs[k, 4] = wave_xz * (here_two + there_two * (sign_x * sign_z))
        coefs[k, 5] = both_two * (wave_y * wave_y) - total
        coefs[k, 6] = wave_y * wave_z * (here_two + there_two * (sign_z * sign_y))
        coefs[k, 7] = both_two * (wave_z * wave_z) - total

    arrived(0, WITHIN_PARTS, 0)
    spectrum = power(0, 5, [None, None])
    arrived(WITHIN_PARTS, 4, 1)
    spectrum = power(WITHIN_PARTS, 2, spectrum)
    arrived(WITHIN_PARTS + 4, 4, 2)
    spectrum = power(WITHIN_PARTS + 4, 2, spectrum)

    rows_re, rows_im = [], []
    for k in range(2):
        here = spectrum[k] * coefs[k, 0]
        there = spectrum[k] * coefs[k, 1]
        rows_re += [here, there]
        rows_im += [here, there * sign_z]
    stress_terms = [
        spectrum[0] * coefs[0, 2 + n] + spectrum[1] * coefs[1, 2 + n] for n in range(6)
    ]
    lane = iota((1, N), 1)
    stress_row = jnp.zeros((1, N), F32)
    for term, lanes in zip(stress_terms, ((0,), (1, 3), (2, 6), (4,), (5, 7), (8,))):
        value = jnp.sum(jnp.sum(term, axis=0, keepdims=True), axis=1, keepdims=True)
        for at in lanes:
            stress_row = jnp.where(lane == at, value, stress_row)

    def projected(rows, table):
        high_part, low_part = split(jnp.concatenate(rows, axis=0))
        return jnp.dot(
            jnp.concatenate([high_part, low_part, high_part], axis=1),
            table[...],
            preferred_element_type=F32,
        )

    proj_re = projected(rows_re, zc_re)
    proj_im = projected(rows_im, zc_im)
    ex_re, ex_im, flip_im = x_re[...], x_im[...], x_flip[...]
    atoms = jnp.zeros((1, ATOMS), F32)
    for n in range(4):
        re_part = proj_re[n * N : (n + 1) * N]
        im_part = proj_im[n * N : (n + 1) * N]
        k = n // 2
        table_im = flip_im if n % 2 else ex_im
        sine = y_waves[k][2] * signs_y[k] if n % 2 else y_waves[k][2]
        real = jnp.sum(ex_re * re_part - table_im * im_part, axis=0, keepdims=True)
        imag = jnp.sum(ex_re * im_part + table_im * re_part, axis=0, keepdims=True)
        atoms = atoms + (real * y_waves[k][1] - imag * sine)
    for r in range(4):
        red_src[r : r + 1, :] = atoms[:, r * N : (r + 1) * N]
    red_src[4:5, :] = stress_row

    def summed(source, parts, moves, slot, stage):
        used = source.at[pl.ds(0, 5)]
        for to_band, to_slab in moves:
            pltpu.make_async_remote_copy(
                used,
                parts.at[slot, pl.ds(0, 5)],
                red_sem.at[2 * stage],
                red_sem.at[2 * stage + 1],
                **device(to_band, to_slab),
            ).start()
        parts[slot, 0:5, :] = source[0:5, :]
        count = len(moves)
        shared = parts.at[pl.ds(0, count), pl.ds(0, 5)]
        pltpu.make_async_copy(shared, shared, red_sem.at[2 * stage + 1]).wait()
        return jnp.sum(parts[:, 0:5, :], axis=0), shared

    moves_x = [
        (greet_bands[dx][dc], greet_slabs[dx][0] + at_z[0])
        for dx in (2, 1, 3, 0)
        for dc in (1, 0)
        if dx + dc
    ]
    moves_yz = [
        (band, lows[0][dy] + at_z[dz])
        for dy, dz in sorted(
            ((dy, dz) for dy in range(4) for dz in range(4) if dy + dz),
            key=lambda m: -sum(min(v, 4 - v) for v in m),
        )
    ]
    middle, sent_x = summed(red_src, red_x, moves_x, 2 * pos_x + core, 0)
    red_mid[0:5, :] = middle
    sums, sent_yz = summed(red_mid, red_yz, moves_yz, 4 * pos_z + pos_y, 1)
    out_atoms[...] = sums[0:4]
    for r in range(3):
        row = sums[4:5, :]
        out_stress[r : r + 1, :] = (row if r == 0 else pltpu.roll(row, N - 3 * r, 1))[:, :3]

    mate_trade.wait_send()

    @pl.when(gives)
    def _():
        for gift in gifts:
            gift.wait_send()

    @pl.when(neg_slab != slab)
    def _():
        neg_copy.wait_send()

    @pl.when(core == 1)
    def _():
        neg_pass.wait_send()

    sent = r_buf.at[:, :, pl.ds(0, N - 2)]
    pltpu.make_async_copy(sent, sent, a2a_send).wait()
    pltpu.make_async_copy(sent_x, sent_x, red_sem.at[0]).wait()
    pltpu.make_async_copy(sent_yz, sent_yz, red_sem.at[2]).wait()


def per_device(orbitals, occupation, g_list, positions, species, widths):
    right_table, left_table, x_table = table_parts()
    anywhere = pl.BlockSpec(memory_space=pltpu.HBM)
    vector = pl.BlockSpec(memory_space=pltpu.VMEM)
    dma = pltpu.SemaphoreType.DMA
    atoms, stress = pl.pallas_call(
        kernel,
        out_shape=(
            jax.ShapeDtypeStruct((4, N), F32),
            jax.ShapeDtypeStruct((3, 3), F32),
        ),
        in_specs=[anywhere] * 9,
        out_specs=(vector, vector),
        scratch_shapes=[
            pltpu.SMEM((2,), F32),
            pltpu.SMEM((4,), F32),
            pltpu.VMEM((2, 4, N, N), F32),
            pltpu.VMEM((N, N), jnp.int32),
            pltpu.VMEM((2, N, N), jnp.int32),
            pltpu.VMEM((3, ATOMS), F32),
            pltpu.VMEM((1, ATOMS), jnp.int32),
            pltpu.VMEM((6 * N, 2 * N), BF16),
            pltpu.VMEM((2 * N, 6 * N), BF16),
            pltpu.VMEM((2 * N, 6 * N), BF16),
            pltpu.VMEM((BANDS, 2, N, N), F32),
            pltpu.VMEM((PARTS, 2, N, N), F32),
            pltpu.VMEM((PARTS, 2, N, N), F32),
            pltpu.VMEM((N, ATOMS), F32),
            pltpu.VMEM((N, ATOMS), F32),
            pltpu.VMEM((3 * N, ATOMS), BF16),
            pltpu.VMEM((3 * N, ATOMS), BF16),
            pltpu.VMEM((N, ATOMS), F32),
            pltpu.VMEM((N, ATOMS), F32),
            pltpu.VMEM((N, ATOMS), F32),
            pltpu.VMEM((N, N), F32),
            pltpu.VMEM((N, N), F32),
            pltpu.VMEM((4, N, N), F32),
            pltpu.VMEM((2, 8, N, N), F32),
            pltpu.VMEM((8, N), F32),
            pltpu.VMEM((8, 8, N), F32),
            pltpu.VMEM((8, N), F32),
            pltpu.VMEM((16, 8, N), F32),
            dma((9,)),
            dma((2,)),
            dma((2,)),
            dma((2,)),
            dma((2,)),
            dma((2,)),
            dma,
            dma((3,)),
            dma((4,)),
        ],
        compiler_params=pltpu.CompilerParams(
            collective_id=0, has_side_effects=True, vmem_limit_bytes=48 << 20
        ),
    )(
        *(
            pltpu.with_memory_space_constraint(operand, pltpu.HBM)
            for operand in (
                orbitals,
                occupation,
                g_list.reshape(N, N),
                positions,
                species.reshape(1, ATOMS),
                widths,
                jnp.asarray(right_table),
                jnp.asarray(left_table),
                jnp.asarray(x_table),
            )
        )
    )
    return stress, atoms.reshape(ATOMS)


def solution(mesh):
    return jax.shard_map(
        per_device,
        mesh=mesh,
        in_specs=(P("band", "grid", None, None), P("band"), P("grid"), P(), P(), P()),
        out_specs=(P(), P()),
        check_vma=False,
    )
```

```python
import functools
import math

import jax
import jax.numpy as jnp
import numpy as np
from jax import lax
from jax.experimental import pallas as pl
from jax.experimental.pallas import tpu as pltpu
from jax.sharding import PartitionSpec as P

MESH = pl.DeviceIdType.MESH
N = 128
ATOMS = 512
BANDS = 8
TWO_PI = 2.0 * math.pi
F32 = jnp.float32
BF16 = jnp.bfloat16

MIXED = (((0, 1), (2, 3)), ((0, 2), (1, 3)), ((0, 3), (1, 2)))
WITHIN_PARTS = 10
PARTS = 18


def far_first(moves):
    order = np.random.RandomState(1).permutation(len(moves))
    return sorted((moves[o] for o in order), key=lambda m: -sum(min(v, 4 - v) for v in m[:3]))


MOVES = far_first(
    [(x, y, z, c) for x in range(2) for y in range(4) for z in range(4) for c in range(2) if x + y + z + c]
)
GREETED = far_first(
    [
        (x, y, z, c)
        for x in range(4)
        for y in range(4)
        for z in range(4)
        for c in range(2)
        if x + y + z + c and (x != 2 or y + z == 0)
    ]
)


def table_parts():
    index = np.arange(N)
    angle = 2.0 * np.pi / N * ((index[:, None] * index[None, :]) % N)
    cos, sin = np.cos(angle), np.sin(angle)
    right = np.block([[cos, -sin], [sin, cos]])
    high = np.asarray(right, dtype=jnp.bfloat16)
    low = np.asarray(right - high.astype(np.float64), dtype=jnp.bfloat16)
    right_cat = np.concatenate([high, high, low], axis=0)
    left_cat = np.concatenate([high.T, high.T, low.T], axis=1)
    order = np.concatenate([index[0::2], index[1::2]])
    order = np.concatenate([order, N + order])
    high_x, low_x = high.T[:, order], low.T[:, order]
    cross_cat = np.concatenate([high_x, high_x, low_x], axis=1)
    return right_cat, left_cat, cross_cat


def split(value):
    high = value.astype(BF16)
    low = (value - high.astype(F32)).astype(BF16)
    return high, low


def iota(shape, dim):
    return lax.broadcasted_iota(jnp.int32, shape, dim)


def fold(cell):
    return jnp.where(cell < N // 2, cell, cell - N)


def turns(value):
    return value - jnp.floor(value + 0.5)


def kernel(
    orbitals, occupation_at, g_list, positions, species, widths_at, right_table, left_table, x_table,
    out_atoms, out_stress,
    occupation, widths, orb_v, list_v, neg_v, pos_v, spec_v, right_v, left_v, tx_v,
    psi, y_buf, r_buf, z_re, z_im, zc_re, zc_im, x_re, x_im, x_flip, col_x, col_z, masks, coefs,
    red_src, red_x, red_mid, red_yz,
    load_sem, mate_sem, cross_send, cross_recv, neg_sem, pass_sem, a2a_send, a2a_recv, red_sem,
):
    band = lax.axis_index("band")
    slab = lax.axis_index("grid")
    half = band // 2
    core = lax.rem(band, 2)
    low = lax.rem(slab // 4, 2)
    pos_x = 2 * half + low
    pos_y = lax.rem(slab, 4)
    pos_z = slab // 8
    owner = 2 * slab + core
    mate = band + 1 - 2 * core

    def device(to_band, to_slab):
        return dict(device_id={"band": to_band, "grid": to_slab}, device_id_type=MESH)

    at_x = [lax.rem(pos_x + move, 4) for move in range(4)]
    at_y = [lax.rem(pos_y + move, 4) for move in range(4)]
    at_z = [8 * lax.rem(pos_z + move, 4) for move in range(4)]
    at_core = [core, 1 - core]
    at_half = [half, 1 - half]
    lows = [[4 * at + y for y in at_y] for at in (low, 1 - low)]

    barrier = pltpu.get_barrier_semaphore()
    loads = [
        pltpu.make_async_copy(src, dst, load_sem.at[k])
        for k, (src, dst) in enumerate(
            (
                (positions, pos_v),
                (species, spec_v),
                (orbitals, orb_v),
                (g_list, list_v),
                (right_table, right_v),
                (left_table, left_v),
                (x_table, tx_v),
                (occupation_at, occupation),
                (widths_at, widths),
            )
        )
    ]
    greet_bands = [[2 * (x // 2) + c for c in at_core] for x in at_x]
    greet_slabs = [[4 * lax.rem(x, 2) + y for y in at_y] for x in at_x]
    for dx, dy, dz, dc in GREETED:
        pl.semaphore_signal(
            barrier, 1, **device(greet_bands[dx][dc], greet_slabs[dx][dy] + at_z[dz])
        )

    for k in (7, 2, 4, 5, 3, 0, 1, 8, 6):
        loads[k].start()

    loads[7].wait()
    loads[2].wait()
    for i in range(2):
        root = jnp.sqrt(jnp.full((N, N), occupation[i], F32))
        for plane in range(4):
            orb_v[i, plane] = orb_v[i, plane] * root
        for plane in range(2):
            psi[2 * band + i, plane] = orb_v[i, 2 * core + plane]

    def transform_yz(transforms, planes):
        blocks = [(transform, plane) for plane in planes for transform in transforms]
        rows = []
        for (_, *pairs), plane in blocks:
            parts = []
            for i, j, scale in pairs:
                rho = psi[i, plane] * psi[j, plane]
                parts.append(rho if scale is None else rho * scale)
            rows.append(jnp.concatenate(parts, axis=1))
        high_part, low_part = split(jnp.concatenate(rows, axis=0))
        along_z = jnp.dot(
            jnp.concatenate([high_part, low_part, high_part], axis=1),
            right_v[...],
            preferred_element_type=F32,
        )
        columns = []
        for n in range(len(blocks)):
            block = along_z[n * N : (n + 1) * N]
            columns.append(jnp.concatenate([block[:, :N], block[:, N:]], axis=0))
        high_part, low_part = split(jnp.concatenate(columns, axis=1))
        along_y = jnp.dot(
            left_v[...],
            jnp.concatenate([high_part, low_part, high_part], axis=0),
            preferred_element_type=F32,
        )
        for n, ((part, *_), plane) in enumerate(blocks):
            y_buf[part, plane] = along_y[:N, n * N : (n + 1) * N]
            y_buf[part + 1, plane] = along_y[N:, n * N : (n + 1) * N]

    def send(first_part, parts, first_plane, planes, chunk, halves, columns):
        for dx, dy, dz, dc in MOVES:
            if dx not in columns:
                continue
            to_slab = lows[dx][dy] + at_z[dz]
            to_core = at_core[dc]
            to_row = pl.multiple_of(4 * to_slab + 2 * to_core, 2)
            my_row = pl.multiple_of(2 * owner, 2)
            where = (pl.ds(first_part, parts), pl.ds(first_plane, planes))
            pltpu.make_async_remote_copy(
                y_buf.at[(*where, pl.ds(to_row, 2))],
                r_buf.at[(*where, pl.ds(my_row, 2))],
                a2a_send,
                a2a_recv.at[chunk],
                **device(2 * halves[dx] + to_core, to_slab),
            ).start()

    loads[4].wait()
    loads[5].wait()
    root_two = math.sqrt(2.0)
    first = 4 * half
    same_half = [half, half]

    def within(part, band_at):
        return (part, (band_at, band_at, None), (band_at + 1, band_at + 1, None))

    transform_yz([within(8 * core, 2 * band)], (0, 1))

    pl.semaphore_wait(barrier, len(GREETED))

    def trade(to_band, to_core, send_sem, recv_sem):
        return pltpu.make_async_remote_copy(
            orb_v.at[:, pl.ds(2 * to_core, 2)],
            psi.at[pl.ds(2 * band, 2)],
            send_sem,
            recv_sem,
            **device(to_band, slab),
        )

    mate_trade = trade(mate, 1 - core, mate_sem.at[0], mate_sem.at[1])
    mate_trade.start()

    loads[3].wait()
    neg_slab = jnp.where(core == 0, lax.rem(32 - slab, 32), 31 - slab)
    neg_copy = pltpu.make_async_remote_copy(
        list_v, neg_v.at[core], neg_sem.at[0], neg_sem.at[1], **device(band, neg_slab)
    )
    neg_pass = pltpu.make_async_remote_copy(
        neg_v.at[1], neg_v.at[1], pass_sem.at[0], pass_sem.at[1], **device(mate, slab)
    )

    @pl.when(neg_slab != slab)
    def _():
        neg_copy.start()

    @pl.when(neg_slab == slab)
    def _():
        neg_v[core] = list_v[...]

    gives = jnp.logical_or(half == 0, core == low)
    gives_late = jnp.logical_and(half == 0, core == 1)
    gifts = [
        trade(2 * (1 - half) + to_core, to_core, cross_send.at[to_core], cross_recv.at[core])
        for to_core in range(2)
    ]

    @pl.when(jnp.logical_and(gives, jnp.logical_not(gives_late)))
    def _():
        for gift in gifts:
            gift.start()

    send(8 * core, 2, 0, 2, 0, same_half, (0,))

    mate_trade.wait_recv()
    rest = [within(8 - 8 * core, 2 * mate)]
    for n, ((i, j), (k, m)) in enumerate(MIXED):
        rest.append(
            (2 + 2 * n, (first + i, first + j, root_two), (first + k, first + m, root_two))
        )
    for plane in range(2):
        transform_yz(rest, (plane,))
        send(2 - 2 * core, 8, plane, 1, 0, same_half, (0,))

    @pl.when(gives_late)
    def _():
        for gift in gifts:
            gift.start()

    send(8 * core, 2, 0, 2, 0, same_half, (1,))
    for plane in range(2):
        send(2 - 2 * core, 8, plane, 1, 0, same_half, (1,))

    loads[0].wait()
    loads[1].wait()
    loads[8].wait()
    kind = spec_v[...]
    width = jnp.zeros((1, ATOMS), F32)
    for s in range(4):
        width = jnp.where(kind == s, widths[s], width)
    spread = -0.5 * width * width
    low_row = iota((8, ATOMS), 0).astype(F32)
    high_row = iota((16, ATOMS), 0)
    high_row = jnp.where(high_row < 8, high_row, high_row - 16).astype(F32)
    for dim, re_ref, im_ref in ((0, x_re, x_im), (2, z_re, z_im)):
        where_at = pos_v[dim : dim + 1, :]
        low_turn = TWO_PI * turns(low_row * where_at)
        high_turn = TWO_PI * turns(high_row * turns(8.0 * where_at))
        low_cos, low_sin = jnp.cos(low_turn), jnp.sin(low_turn)
        high_cos, high_sin = jnp.cos(high_turn), jnp.sin(high_turn)
        for a in range(16):
            wave = (TWO_PI / N) * (low_row + float(8 * (a if a < 8 else a - 16)))
            form = jnp.exp(spread * (wave * wave))
            hc, hs = high_cos[a : a + 1, :], high_sin[a : a + 1, :]
            re_ref[8 * a : 8 * a + 8, :] = (hc * low_cos - hs * low_sin) * form
            im_ref[8 * a : 8 * a + 8, :] = (hc * low_sin + hs * low_cos) * form
    for table, cat in ((z_re, zc_re), (z_im, zc_im)):
        high_part, low_part = split(table[...])
        cat[0:N, :] = high_part
        cat[N : 2 * N, :] = high_part
        cat[2 * N : 3 * N, :] = low_part
    y_waves = []
    at_turn = pos_v[1:2, :]
    for k in range(2):
        freq_y = fold(2 * owner + k)
        high_y = freq_y // 8
        low_y = freq_y - 8 * high_y
        turn_y = TWO_PI * turns(
            low_y.astype(F32) * at_turn + high_y.astype(F32) * turns(8.0 * at_turn)
        )
        wave_y = (TWO_PI / N) * freq_y.astype(F32)
        form_y = jnp.exp(spread * (wave_y * wave_y))
        y_waves.append((wave_y, jnp.cos(turn_y) * form_y, jnp.sin(turn_y) * form_y))

    def mask_of(cells, chosen, columns, negated):
        cell_x = lax.shift_right_logical(cells, 9)
        cell_z = cells & (columns - 1)
        if negated:
            cell_x = (N - cell_x) & (N - 1)
            cell_z = (N - cell_z) & (N - 1)
        col_x[...] = jnp.where(chosen, cell_x, -1).astype(F32)
        col_z[...] = cell_z.astype(F32)
        x_index = iota((N, N), 0).astype(F32).astype(BF16)
        z_index = iota((columns, N), 0).astype(F32).astype(BF16)
        one, zero = jnp.ones((), BF16), jnp.zeros((), BF16)

        def hot(index, block):
            found = []
            for r in range(8):
                row = jnp.broadcast_to(block[r : r + 1, :], (16, N)).astype(BF16)
                rows = jnp.concatenate([row] * (index.shape[0] // 16), axis=0)
                found.append(jnp.where(index == rows, one, zero))
            return found

        def block(step, total):
            first = pl.multiple_of(step * 8, 8)
            hot_x = hot(x_index, col_x[pl.ds(first, 8), :])
            hot_z = hot(z_index, col_z[pl.ds(first, 8), :])
            return total + lax.dot_general(
                jnp.concatenate(hot_x, axis=1),
                jnp.concatenate(hot_z, axis=1),
                (((1,), (1,)), ((), ())),
                preferred_element_type=F32,
            )

        return lax.fori_loop(0, N // 8, block, jnp.zeros((N, columns), F32))

    def own_mask():
        own_cells = list_v[...]
        own_pair = (lax.shift_right_logical(own_cells, 8) & 1) == core
        own_masks = mask_of(own_cells, own_pair, 2 * N, False)
        masks[0] = own_masks[:, :N]
        masks[1] = own_masks[:, N:]

    def pass_list():
        @pl.when(neg_slab != slab)
        def _():
            neg_copy.wait_recv()

        @pl.when(core == 1)
        def _():
            neg_pass.start()

    def neg_mask(slot, plane, at):
        cells = neg_v[slot]
        masks[at] = mask_of(cells, (lax.shift_right_logical(cells, 7) & 3) == plane, N, True)

    @pl.when(half == 1)
    def _():
        own_mask()

    cross_bytes = [trade(0, 0, cross_send.at[0], cross_recv.at[k]) for k in range(2)]

    kind_set = half + low - 2 * half * low
    other = 4 + 2 * kind_set
    for pair in range(2):
        for sender in range(2):
            from_both = jnp.logical_and(half == 1, sender == pair)
            from_one = jnp.logical_and(half == 0, low == sender)

            @pl.when(jnp.logical_or(from_both, from_one) if pair == 0 else from_both)
            def _():
                cross_bytes[sender].wait_recv()

        first_part = WITHIN_PARTS + 4 * pair
        transform_yz(
            [
                (first_part + 2 * n, (i, other, root_two), (i, other + 1, root_two))
                for n, i in enumerate((2 * pair, 2 * pair + 1))
            ],
            (0, 1),
        )
        send(first_part, 4, 0, 2, 1 + pair, at_half, (0, 1))
        if pair == 0:

            @pl.when(half == 1)
            def _():
                pass_list()
                neg_mask(core, 2 * core, 2)

    @pl.when(half == 0)
    def _():
        pass_list()
        own_mask()
        neg_mask(core, 2 * core, 2)

    own_row = pl.ds(pl.multiple_of(2 * owner, 2), 2)
    for part in range(PARTS):
        for plane in range(2):
            r_buf[part, plane, own_row, :] = y_buf[part, plane, own_row, :]

    @pl.when(core == 0)
    def _():
        neg_pass.wait_recv()

    neg_mask(1, 3 - 2 * core, 3)
    loads[6].wait()

    def arrived(first_part, parts, chunk):
        there = r_buf.at[pl.ds(first_part, parts), :, pl.ds(0, N - 2)]
        pltpu.make_async_copy(there, there, a2a_recv.at[chunk]).wait()

    def power(first_part, count, totals):
        blocks = [(q, k) for q in range(count) for k in range(2)]
        columns = [
            jnp.concatenate(
                [
                    r_buf[first_part + 2 * q + part, plane, pl.ds(k, N // 2, stride=2), :]
                    for part in range(2)
                    for plane in range(2)
                ],
                axis=0,
            )
            for q, k in blocks
        ]
        high_part, low_part = split(jnp.concatenate(columns, axis=1))
        along_x = jnp.dot(
            tx_v[...],
            jnp.concatenate([high_part, low_part, high_part], axis=0),
            preferred_element_type=F32,
        )
        for n, (q, k) in enumerate(blocks):
            real = along_x[:N, n * N : (n + 1) * N]
            imag = along_x[N:, n * N : (n + 1) * N]
            term = real * real + imag * imag
            totals[k] = term if totals[k] is None else totals[k] + term
        return totals

    x_flip[...] = jnp.where(iota((N, ATOMS), 0) == N // 2, -x_im[...], x_im[...])

    cell_x = iota((N, N), 0)
    cell_z = iota((N, N), 1)
    wave_x = (TWO_PI / N) * fold(cell_x).astype(F32)
    wave_z = (TWO_PI / N) * fold(cell_z).astype(F32)
    sign_x = jnp.where(cell_x == N // 2, -1.0, 1.0).astype(F32)
    sign_z = jnp.where(cell_z == N // 2, -1.0, 1.0).astype(F32)
    cells = float(N) ** 3
    scale = 0.5 * 4.0 * math.pi / (cells * cells * BANDS)
    wave_xz = wave_x * wave_z
    signs_y = []
    for k in range(2):
        wave_y = y_waves[k][0]
        sign_y = jnp.where(2 * owner + k == N // 2, -1.0, 1.0).astype(F32)
        signs_y.append(sign_y)
        square = wave_x * wave_x + wave_y * wave_y + wave_z * wave_z
        nonzero = square > 0
        inverse = 1.0 / jnp.where(nonzero, square, 1.0)
        weight = jnp.where(nonzero, scale * inverse, 0.0)
        here = weight * masks[k]
        there = weight * masks[2 + k]
        here_two = 2.0 * here * inverse
        there_two = 2.0 * there * inverse
        both_two = here_two + there_two
        total = here + there
        coefs[k, 0] = here
        coefs[k, 1] = there
        coefs[k, 2] = both_two * (wave_x * wave_x) - total
        coefs[k, 3] = wave_y * wave_x * (here_two + there_two * (sign_x * sign_y))
        coefs[k, 4] = wave_xz * (here_two + there_two * (sign_x * sign_z))
        coefs[k, 5] = both_two * (wave_y * wave_y) - total
        coefs[k, 6] = wave_y * wave_z * (here_two + there_two * (sign_z * sign_y))
        coefs[k, 7] = both_two * (wave_z * wave_z) - total

    arrived(0, WITHIN_PARTS, 0)
    spectrum = power(0, 5, [None, None])
    arrived(WITHIN_PARTS, 4, 1)
    spectrum = power(WITHIN_PARTS, 2, spectrum)
    arrived(WITHIN_PARTS + 4, 4, 2)
    spectrum = power(WITHIN_PARTS + 4, 2, spectrum)

    rows_re, rows_im = [], []
    for k in range(2):
        here = spectrum[k] * coefs[k, 0]
        there = spectrum[k] * coefs[k, 1]
        rows_re += [here, there]
        rows_im += [here, there * sign_z]
    stress_terms = [
        spectrum[0] * coefs[0, 2 + n] + spectrum[1] * coefs[1, 2 + n] for n in range(6)
    ]
    lane = iota((1, N), 1)
    stress_row = jnp.zeros((1, N), F32)
    for term, lanes in zip(stress_terms, ((0,), (1, 3), (2, 6), (4,), (5, 7), (8,))):
        value = jnp.sum(jnp.sum(term, axis=0, keepdims=True), axis=1, keepdims=True)
        for at in lanes:
            stress_row = jnp.where(lane == at, value, stress_row)

    def projected(rows, table):
        high_part, low_part = split(jnp.concatenate(rows, axis=0))
        return jnp.dot(
            jnp.concatenate([high_part, low_part, high_part], axis=1),
            table[...],
            preferred_element_type=F32,
        )

    proj_re = projected(rows_re, zc_re)
    proj_im = projected(rows_im, zc_im)
    ex_re, ex_im, flip_im = x_re[...], x_im[...], x_flip[...]
    atoms = jnp.zeros((1, ATOMS), F32)
    for n in range(4):
        re_part = proj_re[n * N : (n + 1) * N]
        im_part = proj_im[n * N : (n + 1) * N]
        k = n // 2
        table_im = flip_im if n % 2 else ex_im
        sine = y_waves[k][2] * signs_y[k] if n % 2 else y_waves[k][2]
        real = jnp.sum(ex_re * re_part - table_im * im_part, axis=0, keepdims=True)
        imag = jnp.sum(ex_re * im_part + table_im * re_part, axis=0, keepdims=True)
        atoms = atoms + (real * y_waves[k][1] - imag * sine)
    for r in range(4):
        red_src[r : r + 1, :] = atoms[:, r * N : (r + 1) * N]
    red_src[4:5, :] = stress_row

    def summed(source, parts, moves, slot, stage):
        used = source.at[pl.ds(0, 5)]
        for to_band, to_slab in moves:
            pltpu.make_async_remote_copy(
                used,
                parts.at[slot, pl.ds(0, 5)],
                red_sem.at[2 * stage],
                red_sem.at[2 * stage + 1],
                **device(to_band, to_slab),
            ).start()
        parts[slot, 0:5, :] = source[0:5, :]
        count = len(moves)
        shared = parts.at[pl.ds(0, count), pl.ds(0, 5)]
        pltpu.make_async_copy(shared, shared, red_sem.at[2 * stage + 1]).wait()
        return jnp.sum(parts[:, 0:5, :], axis=0), shared

    moves_x = [
        (greet_bands[dx][dc], greet_slabs[dx][0] + at_z[0])
        for dx in (2, 1, 3, 0)
        for dc in (1, 0)
        if dx + dc
    ]
    moves_yz = [
        (band, lows[0][dy] + at_z[dz])
        for dy, dz in sorted(
            ((dy, dz) for dy in range(4) for dz in range(4) if dy + dz),
            key=lambda m: -sum(min(v, 4 - v) for v in m),
        )
    ]
    middle, sent_x = summed(red_src, red_x, moves_x, 2 * pos_x + core, 0)
    red_mid[0:5, :] = middle
    sums, sent_yz = summed(red_mid, red_yz, moves_yz, 4 * pos_z + pos_y, 1)
    out_atoms[...] = sums[0:4]
    for r in range(3):
        row = sums[4:5, :]
        out_stress[r : r + 1, :] = (row if r == 0 else pltpu.roll(row, N - 3 * r, 1))[:, :3]

    mate_trade.wait_send()

    @pl.when(gives)
    def _():
        for gift in gifts:
            gift.wait_send()

    @pl.when(neg_slab != slab)
    def _():
        neg_copy.wait_send()

    @pl.when(core == 1)
    def _():
        neg_pass.wait_send()

    sent = r_buf.at[:, :, pl.ds(0, N - 2)]
    pltpu.make_async_copy(sent, sent, a2a_send).wait()
    pltpu.make_async_copy(sent_x, sent_x, red_sem.at[0]).wait()
    pltpu.make_async_copy(sent_yz, sent_yz, red_sem.at[2]).wait()


def per_device(orbitals, occupation, g_list, positions, species, widths):
    right_table, left_table, x_table = table_parts()
    anywhere = pl.BlockSpec(memory_space=pltpu.HBM)
    vector = pl.BlockSpec(memory_space=pltpu.VMEM)
    dma = pltpu.SemaphoreType.DMA
    atoms, stress = pl.pallas_call(
        kernel,
        out_shape=(
            jax.ShapeDtypeStruct((4, N), F32),
            jax.ShapeDtypeStruct((3, 3), F32),
        ),
        in_specs=[anywhere] * 9,
        out_specs=(vector, vector),
        scratch_shapes=[
            pltpu.SMEM((2,), F32),
            pltpu.SMEM((4,), F32),
            pltpu.VMEM((2, 4, N, N), F32),
            pltpu.VMEM((N, N), jnp.int32),
            pltpu.VMEM((2, N, N), jnp.int32),
            pltpu.VMEM((3, ATOMS), F32),
            pltpu.VMEM((1, ATOMS), jnp.int32),
            pltpu.VMEM((6 * N, 2 * N), BF16),
            pltpu.VMEM((2 * N, 6 * N), BF16),
            pltpu.VMEM((2 * N, 6 * N), BF16),
            pltpu.VMEM((BANDS, 2, N, N), F32),
            pltpu.VMEM((PARTS, 2, N, N), F32),
            pltpu.VMEM((PARTS, 2, N, N), F32),
            pltpu.VMEM((N, ATOMS), F32),
            pltpu.VMEM((N, ATOMS), F32),
            pltpu.VMEM((3 * N, ATOMS), BF16),
            pltpu.VMEM((3 * N, ATOMS), BF16),
            pltpu.VMEM((N, ATOMS), F32),
            pltpu.VMEM((N, ATOMS), F32),
            pltpu.VMEM((N, ATOMS), F32),
            pltpu.VMEM((N, N), F32),
            pltpu.VMEM((N, N), F32),
            pltpu.VMEM((4, N, N), F32),
            pltpu.VMEM((2, 8, N, N), F32),
            pltpu.VMEM((8, N), F32),
            pltpu.VMEM((8, 8, N), F32),
            pltpu.VMEM((8, N), F32),
            pltpu.VMEM((16, 8, N), F32),
            dma((9,)),
            dma((2,)),
            dma((2,)),
            dma((2,)),
            dma((2,)),
            dma((2,)),
            dma,
            dma((3,)),
            dma((4,)),
        ],
        compiler_params=pltpu.CompilerParams(
            collective_id=0, has_side_effects=True, vmem_limit_bytes=48 << 20
        ),
    )(
        *(
            pltpu.with_memory_space_constraint(operand, pltpu.HBM)
            for operand in (
                orbitals,
                occupation,
                g_list.reshape(N, N),
                positions,
                species.reshape(1, ATOMS),
                widths,
                jnp.asarray(right_table),
                jnp.asarray(left_table),
                jnp.asarray(x_table),
            )
        )
    )
    return stress, atoms.reshape(ATOMS)


def solution(mesh):
    return jax.shard_map(
        per_device,
        mesh=mesh,
        in_specs=(P("band", "grid", None, None), P("band"), P("grid"), P(), P(), P()),
        out_specs=(P(), P()),
        check_vma=False,
    )
```
